256 devices in a mesh: rep: 2 (over z), blk: 128 (over x, y, core).
Axes of the slice: x: 8, y: 8, z: 2, core: 2. Of those that a mesh axis runs over, the one named last changes fastest.
The devices are a block of a 8x8x16 slice.
Arguments:
- hidden: bfloat16 [32, 4096], P('rep', 'blk'), parts along dimension 0, may hold values from -4 to 4
- queries: bfloat16 [32, 4096], P('rep'), parts along dimension 0, may hold values from -180 to 180
- cache_kv: bfloat16 [2, 32, 4096, 1024], P(None, 'rep', 'blk'), parts along dimension 1, may hold values from -6 to 6
- cache_len: int32 [32], P('rep'), parts along dimension 0, may hold values from 1 to 4096
- inserted_key_value: bfloat16 [2, 16, 4096, 1024], P(None, 'rep', 'blk'), parts along dimension 1, may hold values from -6 to 6
- insert_slot: int32 [16], P('rep'), parts along dimension 0, may hold values from 0 to 15, as said below
- prefix_len: int32 [16], P('rep'), parts along dimension 0, may hold values from 1 to 4096, as said below
- out_weight: bfloat16 [4096, 4096], P(None, 'blk'), may hold values from -0.09375 to 0.09375
- norm_gain: bfloat16 [4096], replicated, may hold values from 0.25 to 1.75
- router_weight: bfloat16 [4096, 4], replicated, may hold values from -0.09375 to 0.09375
- expert_ids: int32 [32, 2], P('rep'), parts along dimension 0, may hold values from 0 to 3, all different within a row
- gate_up: bfloat16 [2, 4096, 28672], P(None, None, 'blk'), may hold values from -0.09375 to 0.09375
- down_proj: bfloat16 [28672, 4096], P('blk'), may hold values from -0.0625 to 0.0625
Outputs:
- layer_out: bfloat16 [32, 4096], P('rep', 'blk'), parts along dimension 0
The draws below stay inside these ranges and needn't reach their ends.
There are 2 independent parts, one for each index of `rep`. The reference program is written for one: setup_inputs(seed, part) draws one part's arguments, and reference() takes and returns one part's arrays. A program takes and returns all parts, laid end to end along the dimension named above; an argument that names none is the same for every part. Nothing has to cross between parts.
Inputs may be any that keep to these rules, and one draw needn't show every extreme that they name: `insert_slot`: 8 different slot numbers. `prefix_len`: some inserted request has all 4096 positions.
All inputs are finite; a program needn't handle non-finite values.
Results may differ from the reference program's by a relative error of at most 0.012.
Values may be sent and summed in bfloat16 or wider, within the bound.
No kernel may reach another device: no remote copies, remote signals or barrier semaphores. Data moves between devices by JAX's collectives and lax.ppermute only.
A program may use at most 128 MiB of HBM per device.

```python
import math
import jax
import jax.numpy as jnp
from jax import lax

D = 4096
QUERY_HEADS = 32
KEY_VALUE_HEADS = 8
HEAD_SIZE = 128
EXPERTS = 4
FF = 7168
SLOTS = 16
INSERTED_SLOTS = 8
CACHE_POSITIONS = 4096


def slot_order(key):
    return jax.random.permutation(jax.random.fold_in(key, 11), SLOTS).astype(jnp.int32)


def cache_lengths(key):
    return jax.random.randint(jax.random.fold_in(key, 12), (SLOTS,), 1, CACHE_POSITIONS + 1).astype(jnp.int32)


def rows_per_slot(key, slot_entry):
    cache_rows = jax.random.normal(jax.random.fold_in(jax.random.fold_in(key, 13), slot_entry), (2, CACHE_POSITIONS, KEY_VALUE_HEADS * HEAD_SIZE), jnp.float32)
    return jnp.clip(cache_rows, -6.0, 6.0)


def inserted_rows(key):
    drawn = jax.random.normal(jax.random.fold_in(key, 41), (2, INSERTED_SLOTS, CACHE_POSITIONS, KEY_VALUE_HEADS * HEAD_SIZE), jnp.float32)
    return jnp.clip(drawn, -6.0, 6.0)


def longest_request(key):
    return jax.random.randint(jax.random.fold_in(key, 32), (), 0, INSERTED_SLOTS).astype(jnp.int32)


def draw_insert_slot(key, part):
    return slot_order(key)[:INSERTED_SLOTS]


def draw_prefix_len(key, part):
    drawn = jax.random.randint(jax.random.fold_in(key, 31), (INSERTED_SLOTS,), 1, CACHE_POSITIONS + 1).astype(jnp.int32)
    longest = longest_request(key)
    return jnp.where(jnp.arange(INSERTED_SLOTS, dtype=jnp.int32) == longest, CACHE_POSITIONS, drawn).astype(jnp.int32)


def draw_cache_len(key, part):
    return cache_lengths(key)


def draw_inserted_key_value(key, part):
    return inserted_rows(key).astype(jnp.bfloat16)


def draw_cache_kv(key, part):
    every_entry = jax.vmap(lambda slot_entry: rows_per_slot(key, slot_entry))(jnp.arange(SLOTS, dtype=jnp.int32))
    return jnp.transpose(every_entry, (1, 0, 2, 3)).astype(jnp.bfloat16)


def draw_queries(key, part):
    base = jnp.clip(1.5 * jax.random.normal(jax.random.fold_in(key, 21), (SLOTS, QUERY_HEADS * HEAD_SIZE), jnp.float32), -9.0, 9.0)
    longest = longest_request(key)
    target_slot = slot_order(key)[longest]
    final_keys = inserted_rows(key)[0, longest, CACHE_POSITIONS // 2 - 1].astype(jnp.bfloat16).astype(jnp.float32).reshape(KEY_VALUE_HEADS, 1, HEAD_SIZE)
    final_query = jnp.broadcast_to(4.0 * final_keys, (KEY_VALUE_HEADS, QUERY_HEADS // KEY_VALUE_HEADS, HEAD_SIZE)).reshape(QUERY_HEADS * HEAD_SIZE)
    base = base.at[target_slot].set(final_query)
    return base.astype(jnp.bfloat16)


def levels(stream_key, extent, cuts, low, largest):
    def one(axis_at, shards_of):
        draws = jax.random.uniform(jax.random.fold_in(jax.random.fold_in(stream_key, 6), axis_at), (shards_of,), jnp.float32, low / len(cuts), largest / len(cuts))
        return jnp.repeat(jnp.exp(draws), extent[axis_at] // shards_of).reshape((-1,) + (1,) * (len(extent) - axis_at - 1))

    level = one(*cuts[0])
    for cut in cuts[1:]:
        level = level * one(*cut)
    return level


def choose_distinct(stream_key, rows, count, top, lift):
    sequence = jax.random.permutation(jax.random.fold_in(stream_key, 1), count)
    boost = sequence
    for power in range(3):
        boost = boost * boost // count
    boost = boost * lift // count
    tickets = jax.random.randint(jax.random.fold_in(stream_key, 2), (rows, count), 0, 4096) + boost
    sure = jax.random.permutation(jax.random.fold_in(stream_key, 3), rows)[jnp.arange(count) % rows]
    tickets = jnp.where(jnp.arange(rows)[:, None] == sure[None, :], 1 << 14, tickets)
    priority = tickets * count + jnp.arange(count)
    return lax.top_k(priority.astype(jnp.int32), top)[1].astype(jnp.int32)


def bell_draw(stream_key, shape, deviation, reach, split=(), held_as=jnp.bfloat16):
    factor_of = levels(stream_key, shape, split, -0.22, 0.18) if split else 1.0
    result = jax.random.normal(stream_key, shape, jnp.float32) * deviation * factor_of
    return jnp.minimum(jnp.maximum(result, -reach), reach).astype(held_as)


def setup_inputs(seed: int = 0, part: int = 0) -> dict:
    splits = jax.random.split(jax.random.key(seed), 14)
    part_splits = jax.random.split(jax.random.fold_in(splits[13], part), 14)
    return {
        "hidden": bell_draw(part_splits[0], (SLOTS, D), 0.3, 4.0, ((1, 128),)),
        "queries": draw_queries(jax.random.fold_in(jax.random.fold_in(splits[13], part), 71), part),
        "cache_kv": draw_cache_kv(jax.random.fold_in(jax.random.fold_in(splits[13], part), 71), part),
        "cache_len": draw_cache_len(jax.random.fold_in(jax.random.fold_in(splits[13], part), 71), part),
        "inserted_key_value": draw_inserted_key_value(jax.random.fold_in(jax.random.fold_in(splits[13], part), 71), part),
        "insert_slot": draw_insert_slot(jax.random.fold_in(jax.random.fold_in(splits[13], part), 71), part),
        "prefix_len": draw_prefix_len(jax.random.fold_in(jax.random.fold_in(splits[13], part), 71), part),
        "out_weight": bell_draw(splits[7], (QUERY_HEADS * HEAD_SIZE, D), (QUERY_HEADS * HEAD_SIZE) ** -0.5, 0.09375, ((1, 128),)),
        "norm_gain": jnp.clip(1.0 + 0.15 * jax.random.normal(splits[8], (D,), jnp.float32), 0.25, 1.75).astype(jnp.bfloat16),
        "router_weight": bell_draw(splits[9], (D, EXPERTS), D ** -0.5, 0.09375),
        "expert_ids": choose_distinct(part_splits[10], SLOTS, EXPERTS, 2, 8192),
        "gate_up": bell_draw(splits[11], (2, D, EXPERTS * FF), D ** -0.5, 0.09375, ((2, 128),)),
        "down_proj": bell_draw(splits[12], (EXPERTS * FF, D), FF ** -0.5, 0.0625, ((0, 128),)),
    }


def attend(queries, key_rows, value_rows, slot_lengths):
    slot_list = queries.shape[0]
    query_groups = QUERY_HEADS // KEY_VALUE_HEADS
    heads_of_queries = queries.astype(jnp.float32).reshape(slot_list, KEY_VALUE_HEADS, query_groups, HEAD_SIZE)
    heads_of_keys = key_rows.astype(jnp.float32).reshape(slot_list, -1, KEY_VALUE_HEADS, HEAD_SIZE)
    heads_of_values = value_rows.astype(jnp.float32).reshape(slot_list, -1, KEY_VALUE_HEADS, HEAD_SIZE)
    scores = jnp.einsum('skgd,sckd->skgc', heads_of_queries, heads_of_keys) / math.sqrt(HEAD_SIZE)
    positions = jnp.arange(heads_of_keys.shape[1], dtype=jnp.int32)
    masked = (positions[None, :] < slot_lengths[:, None])[:, None, None, :]
    scores = jnp.where(masked, scores, -1e+30)
    peak = lax.optimization_barrier(jnp.max(scores, axis=-1, keepdims=True))
    weights = jnp.where(masked, jnp.exp(scores - peak), 0.0)
    totals = lax.optimization_barrier(jnp.sum(weights, axis=-1))
    mixed_values = jnp.einsum('skgc,sckd->skgd', weights, heads_of_values)
    return (mixed_values / totals[..., None]).reshape(slot_list, QUERY_HEADS * HEAD_SIZE)

def route_shares(normed, router_weight, expert_ids):
    logits = jnp.dot(normed, router_weight, preferred_element_type=jnp.float32)
    chosen = (expert_ids[:, :, None] == jnp.arange(EXPERTS, dtype=jnp.int32)[None, None, :]).astype(jnp.float32)
    picked = lax.optimization_barrier(jnp.sum(chosen * logits[:, None, :], axis=-1))
    gates = jax.nn.sigmoid(picked - picked[:, ::-1])
    return lax.optimization_barrier(jnp.sum(gates[:, :, None] * chosen, axis=1))

def reference(hidden, queries, cache_kv, cache_len, inserted_key_value, insert_slot, prefix_len, out_weight, norm_gain, router_weight, expert_ids, gate_up, down_proj):
    placed = jnp.roll(inserted_key_value, CACHE_POSITIONS // 2, axis=2)
    cache = cache_kv.at[:, insert_slot].set(placed)
    slot_lengths = cache_len.at[insert_slot].set(prefix_len)
    attn = attend(queries, cache[0], cache[1], slot_lengths).astype(jnp.bfloat16)
    mixed = (hidden.astype(jnp.float32) + jnp.dot(attn, out_weight, preferred_element_type=jnp.float32)).astype(jnp.bfloat16)
    mixed_f = mixed.astype(jnp.float32)
    scale = jax.lax.rsqrt(lax.optimization_barrier(jnp.mean(mixed_f * mixed_f, axis=-1, keepdims=True)) + 1e-05)
    normed = (mixed_f * scale * norm_gain.astype(jnp.float32)).astype(jnp.bfloat16)
    shares = route_shares(normed, router_weight, expert_ids)
    moe = jnp.zeros(mixed_f.shape, jnp.float32)
    for expert in range(EXPERTS):
        gate_part = gate_up[0][:, expert * FF:(expert + 1) * FF]
        up_part = gate_up[1][:, expert * FF:(expert + 1) * FF]
        act = (jax.nn.silu(jnp.dot(normed, gate_part, preferred_element_type=jnp.float32)) * jnp.dot(normed, up_part, preferred_element_type=jnp.float32)).astype(jnp.bfloat16)
        moe = moe + shares[:, expert:expert + 1] * jnp.dot(act, down_proj[expert * FF:(expert + 1) * FF], preferred_element_type=jnp.float32)
    return (mixed_f + moe).astype(jnp.bfloat16)
```

```python
import math

import jax
import jax.numpy as jnp
from jax import lax
from jax.sharding import Mesh
from jax.sharding import PartitionSpec as P

QUERY_HEADS = 32
KEY_VALUE_HEADS = 8
HEAD_SIZE = 128
EXPERTS = 4
FF = 7168
BLK = ("blk_0", "blk_1", "blk_2")


def exchanged(pieces):
    return lax.all_to_all(pieces, BLK, 0, 0, tiled=True)


def gathered(shard):
    return exchanged(jnp.broadcast_to(shard[None], (lax.axis_size(BLK), *shard.shape)))


def block_attention(queries, key_rows, value_rows, valid):
    slot_list = queries.shape[0]
    query_groups = QUERY_HEADS // KEY_VALUE_HEADS
    heads_of_queries = queries.reshape(slot_list, KEY_VALUE_HEADS, query_groups, HEAD_SIZE)
    heads_of_keys = key_rows.reshape(slot_list, -1, KEY_VALUE_HEADS, HEAD_SIZE)
    heads_of_values = value_rows.reshape(slot_list, -1, KEY_VALUE_HEADS, HEAD_SIZE)
    scores = jnp.einsum(
        "skgd,sckd->skgc", heads_of_queries, heads_of_keys, preferred_element_type=jnp.float32
    ) / math.sqrt(HEAD_SIZE)
    masked = valid[:, None, None, :]
    peak = jnp.max(jnp.where(masked, scores, -1e30), axis=-1, keepdims=True)
    peak = lax.reduce_precision(peak, 8, 7)
    weights = jnp.where(masked, jnp.exp(jnp.where(masked, scores, peak) - peak), 0.0)
    totals = jnp.sum(weights, axis=-1, keepdims=True)
    partial_value = jnp.einsum(
        "skgc,sckd->skgd",
        weights.astype(jnp.bfloat16),
        heads_of_values,
        preferred_element_type=jnp.float32,
    )
    partial_value = partial_value / jnp.where(totals > 0, totals, 1.0)
    lanes = lax.broadcasted_iota(jnp.int32, partial_value.shape, 3)
    stats = jnp.where(lanes < HEAD_SIZE // 2, peak, totals)
    both = jnp.concatenate([partial_value, stats], axis=2).astype(jnp.bfloat16)
    return both.reshape(slot_list * KEY_VALUE_HEADS, 2 * query_groups, HEAD_SIZE)


def merged(pieces):
    rows = pieces.shape[1] // 2
    pieces = pieces.astype(jnp.float32)
    values, stats = pieces[:, :rows], pieces[:, rows:]
    peaks, totals = stats[:, :, :1], stats[:, :, HEAD_SIZE // 2 : HEAD_SIZE // 2 + 1]
    scales = jnp.exp(peaks - jnp.max(peaks, axis=0, keepdims=True)) * totals
    return (jnp.sum(values * scales, axis=0) / jnp.sum(scales, axis=0)).astype(jnp.bfloat16)


def route_shares(normed, router_weight, expert_ids):
    logits = jnp.dot(normed, router_weight, preferred_element_type=jnp.float32)
    chosen = (expert_ids[:, :, None] == jnp.arange(EXPERTS, dtype=jnp.int32)[None, None, :]).astype(
        jnp.float32
    )
    picked = jnp.sum(chosen * logits[:, None, :], axis=-1)
    gates = jax.nn.sigmoid(picked - picked[:, ::-1])
    return jnp.sum(gates[:, :, None] * chosen, axis=1)


def on_device(
    hidden,
    queries,
    cache_kv,
    cache_len,
    inserted_key_value,
    insert_slot,
    prefix_len,
    out_weight,
    norm_gain,
    router_weight,
    expert_ids,
    gate_up,
    down_proj,
):
    cycle_size = lax.axis_size(BLK)
    dev_index = lax.axis_index(BLK)
    ctx_rows = cache_kv.shape[2]
    slots, features = hidden.shape
    positions_in_all = cycle_size * ctx_rows
    cache = cache_kv.at[:, insert_slot].set(inserted_key_value)
    slot_lengths = cache_len.at[insert_slot].set(prefix_len)
    first = jnp.full_like(cache_len, dev_index * ctx_rows)
    first = first.at[insert_slot].set(
        (dev_index * ctx_rows + positions_in_all // 2) % positions_in_all
    )
    positions = first[:, None] + jnp.arange(ctx_rows, dtype=jnp.int32)[None, :]
    valid = positions < slot_lengths[:, None]
    partials = block_attention(queries, cache[0], cache[1], valid)
    attn = gathered(merged(exchanged(partials))).reshape(slots, QUERY_HEADS * HEAD_SIZE)
    local_mixed = (
        hidden.astype(jnp.float32) + jnp.dot(attn, out_weight, preferred_element_type=jnp.float32)
    ).astype(jnp.bfloat16)
    mixed = gathered(local_mixed.reshape(-1, 128)).reshape(cycle_size, slots, features)
    mixed = jnp.transpose(mixed, (1, 0, 2)).reshape(slots, cycle_size * features)
    mixed_f = mixed.astype(jnp.float32)
    scale = lax.rsqrt(jnp.mean(mixed_f * mixed_f, axis=-1, keepdims=True) + 1e-05)
    normed = (mixed_f * scale * norm_gain.astype(jnp.float32)).astype(jnp.bfloat16)
    shares = route_shares(normed, router_weight, expert_ids)
    unit_count = gate_up.shape[2]
    expert_now = dev_index * unit_count // FF
    picker = (jnp.arange(EXPERTS, dtype=jnp.int32) == expert_now).astype(jnp.float32)
    expert_share = jnp.sum(shares * picker[None, :], axis=1)
    act = (
        jax.nn.silu(jnp.dot(normed, gate_up[0], preferred_element_type=jnp.float32))
        * jnp.dot(normed, gate_up[1], preferred_element_type=jnp.float32)
    ).astype(jnp.bfloat16)
    term = expert_share[:, None] * jnp.dot(act, down_proj, preferred_element_type=jnp.float32)
    term = term.astype(jnp.bfloat16).reshape(slots, cycle_size, features)
    term = jnp.transpose(term, (1, 0, 2)).reshape(cycle_size, -1, 128)
    moe = jnp.sum(exchanged(term).astype(jnp.float32), axis=0).reshape(slots, features)
    return (local_mixed.astype(jnp.float32) + moe).astype(jnp.bfloat16)


def solution(mesh):
    split = Mesh(
        mesh.devices.reshape(mesh.shape["rep"], 8, 8, 2), ("rep", "blk_0", "blk_1", "blk_2")
    )
    return jax.shard_map(
        on_device,
        mesh=split,
        in_specs=(
            P("rep", BLK),
            P("rep", None),
            P(None, "rep", BLK, None),
            P("rep"),
            P(None, "rep", BLK, None),
            P("rep"),
            P("rep"),
            P(None, BLK),
            P(),
            P(),
            P("rep", None),
            P(None, None, BLK),
            P(BLK, None),
        ),
        out_specs=P("rep", BLK),
        check_vma=False,
    )
```

```python
import functools
import math

import jax
import jax.numpy as jnp
from jax import lax
from jax.experimental import pallas as pl
from jax.experimental.pallas import tpu as pltpu
from jax.sharding import Mesh
from jax.sharding import PartitionSpec as P

QUERY_HEADS = 32
KEY_VALUE_HEADS = 8
HEAD_SIZE = 128
EXPERTS = 4
FF = 7168
BLK = ("blk_0", "blk_1", "blk_2")
GROUP = QUERY_HEADS // KEY_VALUE_HEADS
LANES = 128
IN_VMEM = pl.BlockSpec(memory_space=pltpu.VMEM)
IN_SMEM = pl.BlockSpec(memory_space=pltpu.SMEM)
ANYWHERE = pl.BlockSpec(memory_space=pl.ANY)
MIB = 1 << 20


def exchanged(pieces):
    return lax.all_to_all(pieces, BLK, 0, 0, tiled=True)


def params(mib):
    return pltpu.CompilerParams(vmem_limit_bytes=mib * MIB)


def attention_kernel(
    first, lengths, insert_slot, prefix_len, queries, cache, inserted, out, spread, rows, sems
):
    slots, prefixes, count = lengths.shape[0], insert_slot.shape[0], rows.shape[2]
    wide = 2 * QUERY_HEADS
    valid = []
    for s in range(slots):
        length, found, at = lengths[s], jnp.int32(0), jnp.int32(0)
        for j in range(prefixes):
            here = insert_slot[j] == s
            length = jnp.where(here, prefix_len[j], length)
            at = jnp.where(here, j, at)
            found = jnp.where(here, 1, found)
        valid.append(length - jnp.where(found == 1, first[1], first[0]))

        @pl.when(found == 1)
        def _():
            pltpu.make_async_copy(inserted.at[:, at], rows.at[s], sems.at[s]).start()

        @pl.when(found == 0)
        def _():
            pltpu.make_async_copy(cache.at[:, s], rows.at[s], sems.at[s]).start()

    for g in range(KEY_VALUE_HEADS):
        for h in range(GROUP):
            at = (g * GROUP + h) * HEAD_SIZE
            one = queries[:, at : at + HEAD_SIZE].astype(jnp.float32)
            for twin in range(2):
                spread[pl.ds(g * 2 * GROUP + twin * GROUP + h, slots, stride=wide), :] = one
    shape = (wide, KEY_VALUE_HEADS * HEAD_SIZE)
    own = (
        lax.broadcasted_iota(jnp.int32, shape, 0) // (2 * GROUP)
        == lax.broadcasted_iota(jnp.int32, shape, 1) // HEAD_SIZE
    )
    is_value = lax.broadcasted_iota(jnp.int32, (wide, HEAD_SIZE), 0) % (2 * GROUP) < GROUP
    is_peak = lax.broadcasted_iota(jnp.int32, (wide, HEAD_SIZE), 1) < HEAD_SIZE // 2
    place = lax.broadcasted_iota(jnp.int32, (wide, count), 1)
    for s in range(slots):
        one = spread[s * wide : (s + 1) * wide, :]
        tiled = jnp.concatenate([one] * KEY_VALUE_HEADS, axis=1)
        blocks = jnp.where(own, tiled, 0.0).astype(jnp.bfloat16)
        pltpu.make_async_copy(cache.at[:, s], rows.at[s], sems.at[s]).wait()
        scores = lax.dot_general(
            blocks, rows[s, 0], (((1,), (1,)), ((), ())), preferred_element_type=jnp.float32
        ) * (1.0 / math.sqrt(HEAD_SIZE))
        inside = place < valid[s]
        scores = jnp.where(inside, scores, -1e30)
        peak = jnp.max(scores, axis=1, keepdims=True).astype(jnp.bfloat16).astype(jnp.float32)
        weights = jnp.where(inside, jnp.exp(scores - peak), 0.0)
        total = jnp.sum(weights, axis=1, keepdims=True)
        every = jnp.dot(
            weights.astype(jnp.bfloat16), rows[s, 1], preferred_element_type=jnp.float32
        )
        value = jnp.concatenate(
            [
                every[g * 2 * GROUP : (g + 1) * 2 * GROUP, g * HEAD_SIZE : (g + 1) * HEAD_SIZE]
                for g in range(KEY_VALUE_HEADS)
            ],
            axis=0,
        )
        value = value / jnp.where(total > 0.0, total, 1.0)
        result = jnp.where(is_value, value, jnp.where(is_peak, peak, total))
        out[s] = result.astype(jnp.bfloat16)


def combine_kernel(pieces, out):
    shape = pieces.shape[1:]
    left = lax.broadcasted_iota(jnp.int32, shape, 1) < HEAD_SIZE // 2
    half = HEAD_SIZE // 2
    found = pieces[...].astype(jnp.float32)
    highest = jnp.max(found, axis=0, keepdims=True)
    scale = jnp.exp(found - highest) * pltpu.roll(found, half, axis=2)
    scale = jnp.where(left[None], scale, pltpu.roll(scale, half, axis=2))
    scale = pltpu.roll(scale, GROUP, axis=1)
    value = jnp.sum(found * scale, axis=0) / jnp.sum(scale, axis=0)
    out[...] = jnp.broadcast_to(value[None, :GROUP].astype(jnp.bfloat16), out.shape)


def project_kernel(attn, weight, hidden, mixed, packed, spread):
    slots, columns = hidden.shape
    spread[...] = attn[...].astype(jnp.float32)
    blocks = [spread[pl.ds(k, slots, stride=QUERY_HEADS), :] for k in range(QUERY_HEADS)]
    whole = jnp.concatenate(blocks, axis=1).astype(jnp.bfloat16)
    total = hidden[...].astype(jnp.float32) + jnp.dot(
        whole, weight[...], preferred_element_type=jnp.float32
    )
    mixed[...] = total.astype(jnp.bfloat16)
    share = LANES // columns
    deep = slots // share
    line = jnp.concatenate([total[b * deep : (b + 1) * deep] for b in range(share)], axis=1)
    packed[...] = jnp.broadcast_to(line[None].astype(jnp.bfloat16), packed.shape)


def swapped(tiles, share):
    slots = tiles.shape[1]
    deep, width = slots // share, LANES // share
    row = lax.broadcasted_iota(jnp.int32, tiles.shape, 1) // deep
    lane = lax.broadcasted_iota(jnp.int32, tiles.shape, 2) // width
    turn = (lane - row + share) % share
    result = tiles
    for j in range(1, share):
        moved = pltpu.roll(pltpu.roll(tiles, j * width, axis=2), slots - j * deep, axis=1)
        result = jnp.where(turn == j, moved, result)
    return result


def experts_kernel(share, expert, gathered, gain, router, chosen, gate_up, down, out):
    blocks, slots = gathered.shape[0], gathered.shape[1]
    mixed = swapped(gathered[...].astype(jnp.float32), share)
    squares = jnp.sum(jnp.sum(mixed * mixed, axis=0), axis=1, keepdims=True)
    scale = lax.rsqrt(squares / (blocks * LANES) + 1e-05)
    normed = (mixed * scale[None] * gain[...].astype(jnp.float32)).astype(jnp.bfloat16)
    plain = normed.astype(jnp.float32)
    logits = [
        jnp.sum(
            jnp.sum(plain * router[e].astype(jnp.float32), axis=0), axis=1, keepdims=True
        )
        for e in range(EXPERTS)
    ]
    ids = [chosen[:, i : i + 1] for i in range(2)]
    picked = [sum(jnp.where(k == e, logits[e], 0.0) for e in range(EXPERTS)) for k in ids]
    gates = [jax.nn.sigmoid(picked[i] - picked[1 - i]) for i in range(2)]
    part = sum(jnp.where(ids[i] == expert[0], gates[i], 0.0) for i in range(2))
    line = jnp.concatenate([normed[k] for k in range(blocks)], axis=1)
    gate = jnp.dot(line, gate_up[0], preferred_element_type=jnp.float32)
    up = jnp.dot(line, gate_up[1], preferred_element_type=jnp.float32)
    act = (gate * jax.nn.sigmoid(gate) * up).astype(jnp.bfloat16)
    term = part * jnp.dot(act, down[...], preferred_element_type=jnp.float32)
    tiles = [term[None, :, k * LANES : (k + 1) * LANES] for k in range(blocks)]
    out[...] = swapped(jnp.concatenate(tiles, axis=0), share).astype(jnp.bfloat16)


def final_kernel(pieces, mixed, out):
    slots, columns = mixed.shape
    share = LANES // columns
    total = jnp.sum(pieces[...].astype(jnp.float32), axis=0)
    moe = jnp.concatenate(
        [total[:, b * columns : (b + 1) * columns] for b in range(share)], axis=0
    )
    out[...] = (mixed[...].astype(jnp.float32) + moe).astype(jnp.bfloat16)


def on_device(
    hidden,
    queries,
    cache_kv,
    cache_len,
    inserted_key_value,
    insert_slot,
    prefix_len,
    out_weight,
    norm_gain,
    router_weight,
    expert_ids,
    gate_up,
    down_proj,
):
    devices = lax.axis_size(BLK)
    dev_index = lax.axis_index(BLK)
    slots, columns = hidden.shape
    ctx_rows, kv_width = cache_kv.shape[2:]
    share = LANES // columns
    width = devices * columns
    blocks = width // LANES
    bf16 = jnp.bfloat16

    positions = devices * ctx_rows
    here = dev_index * ctx_rows
    first = jnp.stack([here, (here + positions // 2) % positions]).astype(jnp.int32)
    partials = pl.pallas_call(
        attention_kernel,
        out_shape=jax.ShapeDtypeStruct((slots, 2 * QUERY_HEADS, HEAD_SIZE), bf16),
        in_specs=[IN_SMEM] * 4 + [IN_VMEM, ANYWHERE, ANYWHERE],
        out_specs=IN_VMEM,
        scratch_shapes=[
            pltpu.VMEM((slots * 2 * QUERY_HEADS, HEAD_SIZE), jnp.float32),
            pltpu.VMEM((slots, 2, ctx_rows, kv_width), bf16),
            pltpu.SemaphoreType.DMA((slots,)),
        ],
        compiler_params=params(12),
        name="attention",
    )(first, cache_len, insert_slot, prefix_len, queries, cache_kv, inserted_key_value)
    pieces = exchanged(partials.reshape(slots * KEY_VALUE_HEADS, 2 * GROUP, HEAD_SIZE))

    own = pl.pallas_call(
        combine_kernel,
        out_shape=jax.ShapeDtypeStruct((devices, GROUP, HEAD_SIZE), bf16),
        in_specs=[IN_VMEM],
        out_specs=IN_VMEM,
        compiler_params=params(8),
        name="combine",
    )(pieces)
    attn = exchanged(own).reshape(slots * QUERY_HEADS, HEAD_SIZE)

    local_mixed, packed = pl.pallas_call(
        project_kernel,
        out_shape=(
            jax.ShapeDtypeStruct((slots, columns), bf16),
            jax.ShapeDtypeStruct((devices, slots // share, LANES), bf16),
        ),
        in_specs=[IN_VMEM] * 3,
        out_specs=(IN_VMEM, IN_VMEM),
        scratch_shapes=[pltpu.VMEM((slots * QUERY_HEADS, HEAD_SIZE), jnp.float32)],
        compiler_params=params(8),
        name="project",
    )(attn, out_weight, hidden)
    gathered = exchanged(packed).reshape(blocks, slots, LANES)

    expert = (dev_index * gate_up.shape[2] // FF).astype(jnp.int32).reshape(1)
    terms = pl.pallas_call(
        functools.partial(experts_kernel, share),
        out_shape=jax.ShapeDtypeStruct((blocks, slots, LANES), bf16),
        in_specs=[IN_SMEM] + [IN_VMEM] * 6,
        out_specs=IN_VMEM,
        compiler_params=params(16),
        name="experts",
    )(
        expert,
        gathered,
        norm_gain.reshape(blocks, 1, LANES),
        router_weight.T.reshape(EXPERTS, blocks, 1, LANES),
        expert_ids,
        gate_up,
        down_proj,
    )
    moe = exchanged(terms.reshape(devices, slots // share, LANES))
    return pl.pallas_call(
        final_kernel,
        out_shape=jax.ShapeDtypeStruct((slots, columns), bf16),
        in_specs=[IN_VMEM] * 2,
        out_specs=IN_VMEM,
        compiler_params=params(4),
        name="final",
    )(moe, local_mixed)


def solution(mesh):
    split = Mesh(
        mesh.devices.reshape(mesh.shape["rep"], 8, 8, 2), ("rep", "blk_0", "blk_1", "blk_2")
    )
    return jax.shard_map(
        on_device,
        mesh=split,
        in_specs=(
            P("rep", BLK),
            P("rep", None),
            P(None, "rep", BLK, None),
            P("rep"),
            P(None, "rep", BLK, None),
            P("rep"),
            P("rep"),
            P(None, BLK),
            P(),
            P(),
            P("rep", None),
            P(None, None, BLK),
            P(BLK, None),
        ),
        out_specs=P("rep", BLK),
        check_vma=False,
    )
```

```python
import functools
import math

import jax
import jax.numpy as jnp
from jax import lax
from jax.experimental import pallas as pl
from jax.experimental.pallas import tpu as pltpu
from jax.sharding import Mesh
from jax.sharding import PartitionSpec as P

QUERY_HEADS = 32
KEY_VALUE_HEADS = 8
HEAD_SIZE = 128
EXPERTS = 4
FF = 7168
BLK = ("blk_0", "blk_1", "blk_2")
GROUP = QUERY_HEADS // KEY_VALUE_HEADS
LANES = 128
IN_VMEM = pl.BlockSpec(memory_space=pltpu.VMEM)
IN_SMEM = pl.BlockSpec(memory_space=pltpu.SMEM)
IN_HBM = pl.BlockSpec(memory_space=pltpu.HBM)
BATCH = 4
MIB = 1 << 20
COVER = pl.CostEstimate(flops=8*10**8, bytes_accessed=8 << 20, transcendentals=0)
ALL_VMEM = 67043328


def exchanged(pieces):
    return lax.all_to_all(pieces, BLK, 0, 0, tiled=True)


def params(mib):
    return pltpu.CompilerParams(vmem_limit_bytes=mib * MIB)


def attention_kernel(
    positions,
    first,
    lengths_in,
    insert_slot_in,
    prefix_len_in,
    queries_in,
    cache,
    inserted,
    out,
    lengths,
    insert_slot,
    prefix_len,
    queries,
    spread,
    rows,
    score_of,
    sems,
):
    slots, prefixes, count = lengths.shape[0], insert_slot.shape[0], rows.shape[2]
    wide = 2 * QUERY_HEADS
    copies = [
        pltpu.make_async_copy(lengths_in, lengths, sems.at[0]),
        pltpu.make_async_copy(insert_slot_in, insert_slot, sems.at[1]),
        pltpu.make_async_copy(prefix_len_in, prefix_len, sems.at[2]),
        pltpu.make_async_copy(queries_in, queries, sems.at[3]),
    ]
    copies += [
        pltpu.make_async_copy(cache.at[k, s], rows.at[s, k], sems.at[4 + 2 * s + k])
        for s in range(slots)
        for k in range(2)
    ]
    copies += [
        pltpu.make_async_copy(
            inserted.at[k, j], rows.at[slots + j, k], sems.at[4 + 2 * (slots + j) + k]
        )
        for j in range(prefixes)
        for k in range(2)
    ]
    for copy in copies:
        copy.start()
    for copy in copies[:4]:
        copy.wait()
    for g in range(KEY_VALUE_HEADS):
        for h in range(GROUP):
            at = (g * GROUP + h) * HEAD_SIZE
            one = queries[:, at : at + HEAD_SIZE].astype(jnp.float32)
            for twin in range(2):
                spread[pl.ds(g * 2 * GROUP + twin * GROUP + h, slots, stride=wide), :] = one
    here = first[0]
    half = positions // 2
    there = jnp.where(here < half, here + half, here - half)
    valid, source = [], []
    for s in range(slots):
        length, at, start = lengths[s], jnp.int32(s), here
        for j in range(prefixes):
            mine = insert_slot[j] == s
            length = jnp.where(mine, prefix_len[j], length)
            at = jnp.where(mine, slots + j, at)
            start = jnp.where(mine, there, start)
        valid.append(length - start)
        source.append(at)
    for copy in copies[4:]:
        copy.wait()
    shape = (wide, KEY_VALUE_HEADS * HEAD_SIZE)
    own = (
        lax.broadcasted_iota(jnp.int32, shape, 0) // (2 * GROUP)
        == lax.broadcasted_iota(jnp.int32, shape, 1) // HEAD_SIZE
    )
    is_value = lax.broadcasted_iota(jnp.int32, (wide, HEAD_SIZE), 0) % (2 * GROUP) < GROUP
    is_peak = lax.broadcasted_iota(jnp.int32, (wide, HEAD_SIZE), 1) < HEAD_SIZE // 2
    place = lax.broadcasted_iota(jnp.int32, (wide, count), 1)
    for s in range(slots):
        one = spread[s * wide : (s + 1) * wide, :]
        tiled = jnp.concatenate([one] * KEY_VALUE_HEADS, axis=1)
        blocks = jnp.where(own, tiled, 0.0).astype(jnp.bfloat16)
        score_of[s] = lax.dot_general(
            blocks,
            rows[source[s], 0],
            (((1,), (1,)), ((), ())),
            preferred_element_type=jnp.float32,
        ) * (1.0 / math.sqrt(HEAD_SIZE))
    for batch in range(0, slots, BATCH):
        several = range(batch, batch + BATCH)
        inside = [place < valid[s] for s in several]
        scores = [jnp.where(i, score_of[s], -1e30) for i, s in zip(inside, several)]
        peaks = [jnp.max(x, axis=1, keepdims=True) for x in scores]
        peaks = [x.astype(jnp.bfloat16).astype(jnp.float32) for x in peaks]
        weights = [
            jnp.where(i, jnp.exp(x - p), 0.0) for i, x, p in zip(inside, scores, peaks)
        ]
        totals = [jnp.sum(x, axis=1, keepdims=True) for x in weights]
        every = [
            jnp.dot(
                x.astype(jnp.bfloat16), rows[source[s], 1], preferred_element_type=jnp.float32
            )
            for x, s in zip(weights, several)
        ]
        for s, full, peak, total in zip(several, every, peaks, totals):
            value = jnp.concatenate(
                [
                    full[g * 2 * GROUP : (g + 1) * 2 * GROUP, g * HEAD_SIZE : (g + 1) * HEAD_SIZE]
                    for g in range(KEY_VALUE_HEADS)
                ],
                axis=0,
            )
            value = value / jnp.where(total > 0.0, total, 1.0)
            result = jnp.where(is_value, value, jnp.where(is_peak, peak, total))
            out[s] = result.astype(jnp.bfloat16)


def combine_kernel(pieces, out):
    shape = pieces.shape[1:]
    left = lax.broadcasted_iota(jnp.int32, shape, 1) < HEAD_SIZE // 2
    half = HEAD_SIZE // 2
    found = pieces[...].astype(jnp.float32)
    highest = jnp.max(found, axis=0, keepdims=True)
    scale = jnp.exp(found - highest) * pltpu.roll(found, half, axis=2)
    scale = jnp.where(left[None], scale, pltpu.roll(scale, half, axis=2))
    scale = pltpu.roll(scale, GROUP, axis=1)
    value = jnp.sum(found * scale, axis=0) / jnp.sum(scale, axis=0)
    out[...] = jnp.broadcast_to(value[None, :GROUP].astype(jnp.bfloat16), out.shape)


def project_kernel(attn, weight, hidden, mixed, packed, spread):
    slots, columns = hidden.shape
    spread[...] = attn[...].astype(jnp.float32)
    blocks = [spread[pl.ds(k, slots, stride=QUERY_HEADS), :] for k in range(QUERY_HEADS)]
    whole = jnp.concatenate(blocks, axis=1).astype(jnp.bfloat16)
    total = hidden[...].astype(jnp.float32) + lax.dot_general(
        whole, weight[...], (((1,), (1,)), ((), ())), preferred_element_type=jnp.float32
    )
    mixed[...] = total.astype(jnp.bfloat16)
    share = LANES // columns
    deep = slots // share
    line = jnp.concatenate([total[b * deep : (b + 1) * deep] for b in range(share)], axis=1)
    packed[...] = jnp.broadcast_to(line[None].astype(jnp.bfloat16), packed.shape)


def swapped(tiles, share):
    slots = tiles.shape[1]
    deep, width = slots // share, LANES // share
    row = lax.broadcasted_iota(jnp.int32, tiles.shape, 1) // deep
    lane = lax.broadcasted_iota(jnp.int32, tiles.shape, 2) // width
    turn = (lane - row + share) % share
    result = tiles
    for j in range(1, share):
        moved = pltpu.roll(pltpu.roll(tiles, j * width, axis=2), slots - j * deep, axis=1)
        result = jnp.where(turn == j, moved, result)
    return result


def experts_kernel(share, expert, gathered, gain, router, chosen, gate_up, down, out):
    blocks, slots = gathered.shape[0], gathered.shape[1]
    tiles = swapped(gathered[...].astype(jnp.float32), share)
    mixed = jnp.concatenate([tiles[k] for k in range(blocks)], axis=1)
    scale = lax.rsqrt(jnp.sum(mixed * mixed, axis=1, keepdims=True) / (blocks * LANES) + 1e-05)
    normed = (mixed * scale * gain[...].astype(jnp.float32).reshape(1, blocks * LANES)).astype(jnp.bfloat16)
    plain = normed.astype(jnp.float32)
    weights = router[...].astype(jnp.float32)
    logits = [
        jnp.sum(plain * weights[e : e + 1], axis=1, keepdims=True) for e in range(EXPERTS)
    ]
    upright = lax.broadcasted_iota(jnp.int32, (slots, slots), 0) == lax.broadcasted_iota(
        jnp.int32, (slots, slots), 1
    )
    ids = [
        jnp.sum(
            jnp.where(upright, chosen[i : i + 1, :].astype(jnp.float32), 0.0),
            axis=1,
            keepdims=True,
        )
        for i in range(2)
    ]
    picked = [sum(jnp.where(k == e, logits[e], 0.0) for e in range(EXPERTS)) for k in ids]
    gates = [jax.nn.sigmoid(picked[i] - picked[1 - i]) for i in range(2)]
    mine = expert[0].astype(jnp.float32)
    part = sum(jnp.where(ids[i] == mine, gates[i], 0.0) for i in range(2))
    gate, up = [
        lax.dot_general(
            normed, gate_up[i], (((1,), (1,)), ((), ())), preferred_element_type=jnp.float32
        )
        for i in range(2)
    ]
    act = (gate * jax.nn.sigmoid(gate) * up).astype(jnp.bfloat16)
    term = part * jnp.dot(act, down[...], preferred_element_type=jnp.float32)
    tiles = [term[None, :, k * LANES : (k + 1) * LANES] for k in range(blocks)]
    out[...] = swapped(jnp.concatenate(tiles, axis=0), share).astype(jnp.bfloat16)


def final_kernel(pieces, mixed, out):
    slots, columns = mixed.shape
    share = LANES // columns
    total = jnp.sum(pieces[...].astype(jnp.float32), axis=0)
    moe = jnp.concatenate(
        [total[:, b * columns : (b + 1) * columns] for b in range(share)], axis=0
    )
    out[...] = (mixed[...].astype(jnp.float32) + moe).astype(jnp.bfloat16)


def on_device(
    hidden,
    queries,
    cache_kv,
    cache_len,
    inserted_key_value,
    insert_slot,
    prefix_len,
    out_weight,
    norm_gain,
    router_weight,
    expert_ids,
    gate_up,
    down_proj,
):
    devices = lax.axis_size(BLK)
    dev_index = lax.axis_index(BLK)
    slots, columns = hidden.shape
    ctx_rows, kv_width = cache_kv.shape[2:]
    prefixes = insert_slot.shape[0]
    share = LANES // columns
    width = devices * columns
    blocks = width // LANES
    bf16 = jnp.bfloat16

    first = (dev_index * ctx_rows).astype(jnp.int32).reshape(1)
    partials = pl.pallas_call(
        functools.partial(attention_kernel, devices * ctx_rows),
        out_shape=jax.ShapeDtypeStruct((slots, 2 * QUERY_HEADS, HEAD_SIZE), bf16),
        in_specs=[IN_SMEM] + [IN_HBM] * 6,
        out_specs=IN_VMEM,
        scratch_shapes=[
            pltpu.SMEM((slots,), jnp.int32),
            pltpu.SMEM((prefixes,), jnp.int32),
            pltpu.SMEM((prefixes,), jnp.int32),
            pltpu.VMEM(queries.shape, bf16),
            pltpu.VMEM((slots * 2 * QUERY_HEADS, HEAD_SIZE), jnp.float32),
            pltpu.VMEM((slots + prefixes, 2, ctx_rows, kv_width), bf16),
            pltpu.VMEM((slots, 2 * QUERY_HEADS, ctx_rows), jnp.float32),
            pltpu.SemaphoreType.DMA((4 + 2 * (slots + prefixes),)),
        ],
        compiler_params=pltpu.CompilerParams(vmem_limit_bytes=ALL_VMEM),
        name="attention",
    )(first, cache_len, insert_slot, prefix_len, queries, cache_kv, inserted_key_value)
    pieces = exchanged(partials.reshape(slots * KEY_VALUE_HEADS, 2 * GROUP, HEAD_SIZE))

    own = pl.pallas_call(
        combine_kernel,
        out_shape=jax.ShapeDtypeStruct((devices, GROUP, HEAD_SIZE), bf16),
        in_specs=[IN_VMEM],
        out_specs=IN_VMEM,
        compiler_params=params(8),
        cost_estimate=COVER,
        name="combine",
    )(pieces)
    attn = exchanged(own).reshape(slots * QUERY_HEADS, HEAD_SIZE)

    local_mixed, packed = pl.pallas_call(
        project_kernel,
        out_shape=(
            jax.ShapeDtypeStruct((slots, columns), bf16),
            jax.ShapeDtypeStruct((devices, slots // share, LANES), bf16),
        ),
        in_specs=[IN_VMEM] * 3,
        out_specs=(IN_VMEM, IN_VMEM),
        scratch_shapes=[pltpu.VMEM((slots * QUERY_HEADS, HEAD_SIZE), jnp.float32)],
        compiler_params=params(8),
        cost_estimate=COVER,
        name="project",
    )(attn, out_weight.T, hidden)
    gathered = exchanged(packed).reshape(blocks, slots, LANES)

    expert = (dev_index * gate_up.shape[2] // FF).astype(jnp.int32).reshape(1)
    terms = pl.pallas_call(
        functools.partial(experts_kernel, share),
        out_shape=jax.ShapeDtypeStruct((blocks, slots, LANES), bf16),
        in_specs=[IN_SMEM] + [IN_VMEM] * 6,
        out_specs=IN_VMEM,
        compiler_params=params(16),
        name="experts",
    )(
        expert,
        gathered,
        norm_gain,
        router_weight.T,
        expert_ids.T,
        jnp.swapaxes(gate_up, 1, 2),
        down_proj,
    )
    moe = exchanged(terms.reshape(devices, slots // share, LANES))
    return pl.pallas_call(
        final_kernel,
        out_shape=jax.ShapeDtypeStruct((slots, columns), bf16),
        in_specs=[IN_VMEM] * 2,
        out_specs=IN_VMEM,
        compiler_params=params(4),
        name="final",
    )(moe, local_mixed)


def solution(mesh):
    split = Mesh(
        mesh.devices.reshape(mesh.shape["rep"], 8, 8, 2), ("rep", "blk_0", "blk_1", "blk_2")
    )
    return jax.shard_map(
        on_device,
        mesh=split,
        in_specs=(
            P("rep", BLK),
            P("rep", None),
            P(None, "rep", BLK, None),
            P("rep"),
            P(None, "rep", BLK, None),
            P("rep"),
            P("rep"),
            P(None, BLK),
            P(),
            P(),
            P("rep", None),
            P(None, None, BLK),
            P(BLK, None),
        ),
        out_specs=P("rep", BLK),
        check_vma=False,
    )
```

```python
import functools
import math

import jax
import jax.numpy as jnp
from jax import lax
from jax.experimental import pallas as pl
from jax.experimental.pallas import tpu as pltpu
from jax.sharding import Mesh
from jax.sharding import PartitionSpec as P

QUERY_HEADS = 32
KEY_VALUE_HEADS = 8
HEAD_SIZE = 128
EXPERTS = 4
FF = 7168
BLK = ("blk_0", "blk_1", "blk_2")
GROUP = QUERY_HEADS // KEY_VALUE_HEADS
LANES = 128
SPAN = LANES // GROUP
IN_VMEM = pl.BlockSpec(memory_space=pltpu.VMEM)
IN_SMEM = pl.BlockSpec(memory_space=pltpu.SMEM)
IN_HBM = pl.BlockSpec(memory_space=pltpu.HBM)
BATCH = 4
MIB = 1 << 20
COVER = pl.CostEstimate(flops=8*10**8, bytes_accessed=8 << 20, transcendentals=0)
ALL_VMEM = 67043328


def exchanged(pieces, axis=BLK):
    return lax.all_to_all(pieces, axis, 0, 0, tiled=True)


def merging(kernel, shape, *pieces):
    return pl.pallas_call(
        kernel,
        out_shape=jax.ShapeDtypeStruct(shape, jnp.bfloat16),
        in_specs=[IN_VMEM] * len(pieces),
        out_specs=IN_VMEM,
        compiler_params=params(8),
        cost_estimate=COVER,
        name=kernel.__name__,
    )(*pieces)


def params(mib):
    return pltpu.CompilerParams(vmem_limit_bytes=mib * MIB)


def attention_kernel(
    positions,
    first,
    lengths_in,
    insert_slot_in,
    prefix_len_in,
    queries_in,
    cache,
    inserted,
    out,
    lengths,
    insert_slot,
    prefix_len,
    queries,
    spread,
    rows,
    score_of,
    values,
    stats,
    sems,
):
    slots, prefixes, count = lengths.shape[0], insert_slot.shape[0], rows.shape[2]
    wide = QUERY_HEADS
    copies = [
        pltpu.make_async_copy(lengths_in, lengths, sems.at[0]),
        pltpu.make_async_copy(insert_slot_in, insert_slot, sems.at[1]),
        pltpu.make_async_copy(prefix_len_in, prefix_len, sems.at[2]),
        pltpu.make_async_copy(queries_in, queries, sems.at[3]),
    ]
    copies += [
        pltpu.make_async_copy(cache.at[k, s], rows.at[s, k], sems.at[4 + 2 * s + k])
        for s in range(slots)
        for k in range(2)
    ]
    copies += [
        pltpu.make_async_copy(
            inserted.at[k, j], rows.at[slots + j, k], sems.at[4 + 2 * (slots + j) + k]
        )
        for j in range(prefixes)
        for k in range(2)
    ]
    for copy in copies:
        copy.start()
    for copy in copies[:4]:
        copy.wait()
    for g in range(KEY_VALUE_HEADS):
        for h in range(GROUP):
            at = (g * GROUP + h) * HEAD_SIZE
            one = queries[:, at : at + HEAD_SIZE].astype(jnp.float32)
            spread[pl.ds(g * GROUP + h, slots, stride=wide), :] = one
    here = first[0]
    half = positions // 2
    there = jnp.where(here < half, here + half, here - half)
    valid, source = [], []
    for s in range(slots):
        length, at, start = lengths[s], jnp.int32(s), here
        for j in range(prefixes):
            mine = insert_slot[j] == s
            length = jnp.where(mine, prefix_len[j], length)
            at = jnp.where(mine, slots + j, at)
            start = jnp.where(mine, there, start)
        valid.append(length - start)
        source.append(at)
    for copy in copies[4:]:
        copy.wait()
    shape = (wide, KEY_VALUE_HEADS * HEAD_SIZE)
    own = (
        lax.broadcasted_iota(jnp.int32, shape, 0) // GROUP
        == lax.broadcasted_iota(jnp.int32, shape, 1) // HEAD_SIZE
    )
    row = lax.broadcasted_iota(jnp.int32, (wide, HEAD_SIZE), 0)
    lane = lax.broadcasted_iota(jnp.int32, (wide, HEAD_SIZE), 1)
    counted = lane // SPAN == row % GROUP
    early = lax.broadcasted_iota(jnp.int32, (2 * GROUP, HEAD_SIZE), 0) < GROUP
    place = lax.broadcasted_iota(jnp.int32, (wide, count), 1)
    for s in range(slots):
        one = spread[s * wide : (s + 1) * wide, :]
        tiled = jnp.concatenate([one] * KEY_VALUE_HEADS, axis=1)
        blocks = jnp.where(own, tiled, 0.0).astype(jnp.bfloat16)
        score_of[s] = lax.dot_general(
            blocks,
            rows[source[s], 0],
            (((1,), (1,)), ((), ())),
            preferred_element_type=jnp.float32,
        ) * (1.0 / math.sqrt(HEAD_SIZE))
    for batch in range(0, slots, BATCH):
        several = range(batch, batch + BATCH)
        inside = [place < valid[s] for s in several]
        scores = [jnp.where(i, score_of[s], -1e30) for i, s in zip(inside, several)]
        peaks = [jnp.max(x, axis=1, keepdims=True) for x in scores]
        peaks = [x.astype(jnp.bfloat16).astype(jnp.float32) for x in peaks]
        weights = [
            jnp.where(i, jnp.exp(x - p), 0.0) for i, x, p in zip(inside, scores, peaks)
        ]
        totals = [jnp.sum(x, axis=1, keepdims=True) for x in weights]
        every = [
            jnp.dot(
                x.astype(jnp.bfloat16), rows[source[s], 1], preferred_element_type=jnp.float32
            )
            for x, s in zip(weights, several)
        ]
        for s, full, peak, total in zip(several, every, peaks, totals):
            value = jnp.concatenate(
                [
                    jnp.where(
                        early,
                        full[g * GROUP : (g + 2) * GROUP, g * HEAD_SIZE : (g + 1) * HEAD_SIZE],
                        full[
                            g * GROUP : (g + 2) * GROUP, (g + 1) * HEAD_SIZE : (g + 2) * HEAD_SIZE
                        ],
                    )
                    for g in range(0, KEY_VALUE_HEADS, 2)
                ],
                axis=0,
            )
            values[pl.ds(s, wide, stride=slots), :] = value / jnp.where(total > 0.0, total, 1.0)
            stats[pl.ds(s, wide, stride=slots), :] = jnp.where(
                counted, packed_stats(lane, peak, total), 0.0
            )
    deep = GROUP * slots
    for g in range(KEY_VALUE_HEADS):
        out[g, :deep, :] = values[g * deep : (g + 1) * deep, :].astype(jnp.bfloat16)
        one = [stats[g * deep + h * slots : g * deep + (h + 1) * slots, :] for h in range(GROUP)]
        out[g, deep:, :] = sum(one).astype(jnp.bfloat16)


def packed_stats(lane, peak, total):
    rounded = total.astype(jnp.bfloat16).astype(jnp.float32)
    at = lane % SPAN
    return jnp.where(
        at < SPAN // 2, peak, jnp.where(at < SPAN * 3 // 4, rounded, total - rounded)
    )


def merge(pieces):
    slots = pieces[0].shape[0] // (GROUP + 1)
    found = [x[GROUP * slots :].astype(jnp.float32) for x in pieces]
    highest = functools.reduce(jnp.maximum, found)
    scales = [
        jnp.exp(x - highest)
        * (
            pltpu.roll(x, LANES - SPAN // 2, axis=1)
            + pltpu.roll(x, LANES - SPAN * 3 // 4, axis=1)
        )
        for x in found
    ]
    total = sum(scales)
    safe = jnp.where(total > 0.0, total, 1.0)
    values = []
    for h in range(GROUP):
        column = slice(h * SPAN, h * SPAN + 1)
        parts = [
            x[h * slots : (h + 1) * slots].astype(jnp.float32) * y[:, column]
            for x, y in zip(pieces, scales)
        ]
        values.append(sum(parts) / safe[:, column])
    return values, highest, total


def whole_part(pieces):
    values, highest, total = merge(pieces)
    lane = lax.broadcasted_iota(jnp.int32, highest.shape, 1)
    total = pltpu.roll(total, SPAN // 2, axis=1)
    rounded = total.astype(jnp.bfloat16).astype(jnp.float32)
    rest = pltpu.roll(total - rounded, SPAN // 4, axis=1)
    at = lane % SPAN
    stats = jnp.where(at < SPAN // 2, highest, jnp.where(at < SPAN * 3 // 4, rounded, rest))
    return jnp.concatenate(values + [stats], axis=0).astype(jnp.bfloat16)


def spread_kernel(pieces, out):
    part = whole_part([pieces[i] for i in range(pieces.shape[0])])
    for i in range(out.shape[0]):
        out[i] = part


def part_kernel(pieces, out):
    out[...] = whole_part([pieces[i] for i in range(pieces.shape[0])])


def pair_kernel(mine, other, out):
    values, _, _ = merge([mine[...], other[...]])
    part = jnp.concatenate(values, axis=0).astype(jnp.bfloat16)
    for i in range(out.shape[0]):
        out[i] = part


def project_kernel(attn, weight, hidden, mixed, packed):
    slots, columns = hidden.shape
    blocks = [
        attn[g, h * slots : (h + 1) * slots, :]
        for g in range(KEY_VALUE_HEADS)
        for h in range(GROUP)
    ]
    whole = jnp.concatenate(blocks, axis=1)
    total = hidden[...].astype(jnp.float32) + lax.dot_general(
        whole, weight[...], (((1,), (1,)), ((), ())), preferred_element_type=jnp.float32
    )
    mixed[...] = total.astype(jnp.bfloat16)
    share = LANES // columns
    deep = slots // share
    line = jnp.concatenate([total[b * deep : (b + 1) * deep] for b in range(share)], axis=1)
    packed[...] = jnp.broadcast_to(line[None].astype(jnp.bfloat16), packed.shape)


def swapped(tiles, share):
    slots = tiles.shape[1]
    deep, width = slots // share, LANES // share
    row = lax.broadcasted_iota(jnp.int32, tiles.shape, 1) // deep
    lane = lax.broadcasted_iota(jnp.int32, tiles.shape, 2) // width
    turn = (lane - row + share) % share
    result = tiles
    for j in range(1, share):
        moved = pltpu.roll(pltpu.roll(tiles, j * width, axis=2), slots - j * deep, axis=1)
        result = jnp.where(turn == j, moved, result)
    return result


def experts_kernel(share, expert, gathered, gain, router, chosen, gate_up, down, out):
    blocks, slots = gathered.shape[0], gathered.shape[1]
    tiles = swapped(gathered[...].astype(jnp.float32), share)
    mixed = jnp.concatenate([tiles[k] for k in range(blocks)], axis=1)
    scale = lax.rsqrt(jnp.sum(mixed * mixed, axis=1, keepdims=True) / (blocks * LANES) + 1e-05)
    normed = (mixed * scale * gain[...].astype(jnp.float32).reshape(1, blocks * LANES)).astype(jnp.bfloat16)
    plain = normed.astype(jnp.float32)
    weights = router[...].astype(jnp.float32)
    logits = [
        jnp.sum(plain * weights[e : e + 1], axis=1, keepdims=True) for e in range(EXPERTS)
    ]
    upright = lax.broadcasted_iota(jnp.int32, (slots, slots), 0) == lax.broadcasted_iota(
        jnp.int32, (slots, slots), 1
    )
    ids = [
        jnp.sum(
            jnp.where(upright, chosen[i : i + 1, :].astype(jnp.float32), 0.0),
            axis=1,
            keepdims=True,
        )
        for i in range(2)
    ]
    picked = [sum(jnp.where(k == e, logits[e], 0.0) for e in range(EXPERTS)) for k in ids]
    gates = [jax.nn.sigmoid(picked[i] - picked[1 - i]) for i in range(2)]
    mine = expert[0].astype(jnp.float32)
    part = sum(jnp.where(ids[i] == mine, gates[i], 0.0) for i in range(2))
    gate, up = [
        lax.dot_general(
            normed, gate_up[i], (((1,), (1,)), ((), ())), preferred_element_type=jnp.float32
        )
        for i in range(2)
    ]
    act = (gate * jax.nn.sigmoid(gate) * up).astype(jnp.bfloat16)
    term = part * jnp.dot(act, down[...], preferred_element_type=jnp.float32)
    tiles = [term[None, :, k * LANES : (k + 1) * LANES] for k in range(blocks)]
    out[...] = swapped(jnp.concatenate(tiles, axis=0), share).astype(jnp.bfloat16)


def final_kernel(pieces, mixed, out):
    slots, columns = mixed.shape
    share = LANES // columns
    total = jnp.sum(pieces[...].astype(jnp.float32), axis=0)
    moe = jnp.concatenate(
        [total[:, b * columns : (b + 1) * columns] for b in range(share)], axis=0
    )
    out[...] = (mixed[...].astype(jnp.float32) + moe).astype(jnp.bfloat16)


def on_device(
    hidden,
    queries,
    cache_kv,
    cache_len,
    inserted_key_value,
    insert_slot,
    prefix_len,
    out_weight,
    norm_gain,
    router_weight,
    expert_ids,
    gate_up,
    down_proj,
):
    devices = lax.axis_size(BLK)
    dev_index = lax.axis_index(BLK)
    slots, columns = hidden.shape
    ctx_rows, kv_width = cache_kv.shape[2:]
    prefixes = insert_slot.shape[0]
    share = LANES // columns
    deep = slots * (GROUP + 1)
    width = devices * columns
    blocks = width // LANES
    bf16 = jnp.bfloat16

    first = (dev_index * ctx_rows).astype(jnp.int32).reshape(1)
    partials = pl.pallas_call(
        functools.partial(attention_kernel, devices * ctx_rows),
        out_shape=jax.ShapeDtypeStruct((KEY_VALUE_HEADS, deep, HEAD_SIZE), bf16),
        in_specs=[IN_SMEM] + [IN_HBM] * 6,
        out_specs=IN_VMEM,
        scratch_shapes=[
            pltpu.SMEM((slots,), jnp.int32),
            pltpu.SMEM((prefixes,), jnp.int32),
            pltpu.SMEM((prefixes,), jnp.int32),
            pltpu.VMEM(queries.shape, bf16),
            pltpu.VMEM((slots * QUERY_HEADS, HEAD_SIZE), jnp.float32),
            pltpu.VMEM((slots + prefixes, 2, ctx_rows, kv_width), bf16),
            pltpu.VMEM((slots, QUERY_HEADS, ctx_rows), jnp.float32),
            pltpu.VMEM((slots * QUERY_HEADS, HEAD_SIZE), jnp.float32),
            pltpu.VMEM((slots * QUERY_HEADS, HEAD_SIZE), jnp.float32),
            pltpu.SemaphoreType.DMA((4 + 2 * (slots + prefixes),)),
        ],
        compiler_params=pltpu.CompilerParams(vmem_limit_bytes=ALL_VMEM),
        name="attention",
    )(first, cache_len, insert_slot, prefix_len, queries, cache_kv, inserted_key_value)
    along, across, pair = BLK
    copies = lax.axis_size(across)
    part = merging(spread_kernel, (copies, deep, HEAD_SIZE), exchanged(partials, along))
    part = merging(part_kernel, (deep, HEAD_SIZE), exchanged(part, across))
    other = lax.ppermute(part, pair, [(0, 1), (1, 0)])
    own = merging(pair_kernel, (KEY_VALUE_HEADS, slots * GROUP, HEAD_SIZE), part, other)
    attn = exchanged(own, along)

    local_mixed, packed = pl.pallas_call(
        project_kernel,
        out_shape=(
            jax.ShapeDtypeStruct((slots, columns), bf16),
            jax.ShapeDtypeStruct((devices, slots // share, LANES), bf16),
        ),
        in_specs=[IN_VMEM] * 3,
        out_specs=(IN_VMEM, IN_VMEM),
        compiler_params=params(8),
        cost_estimate=COVER,
        name="project",
    )(attn, out_weight.T, hidden)
    gathered = exchanged(packed).reshape(blocks, slots, LANES)

    expert = (dev_index * gate_up.shape[2] // FF).astype(jnp.int32).reshape(1)
    terms = pl.pallas_call(
        functools.partial(experts_kernel, share),
        out_shape=jax.ShapeDtypeStruct((blocks, slots, LANES), bf16),
        in_specs=[IN_SMEM] + [IN_VMEM] * 6,
        out_specs=IN_VMEM,
        compiler_params=params(16),
        name="experts",
    )(
        expert,
        gathered,
        norm_gain,
        router_weight.T,
        expert_ids.T,
        jnp.swapaxes(gate_up, 1, 2),
        down_proj,
    )
    moe = exchanged(terms.reshape(devices, slots // share, LANES))
    return pl.pallas_call(
        final_kernel,
        out_shape=jax.ShapeDtypeStruct((slots, columns), bf16),
        in_specs=[IN_VMEM] * 2,
        out_specs=IN_VMEM,
        compiler_params=params(4),
        name="final",
    )(moe, local_mixed)


def solution(mesh):
    split = Mesh(
        mesh.devices.reshape(mesh.shape["rep"], 8, 8, 2), ("rep", "blk_0", "blk_1", "blk_2")
    )
    return jax.shard_map(
        on_device,
        mesh=split,
        in_specs=(
            P("rep", BLK),
            P("rep", None),
            P(None, "rep", BLK, None),
            P("rep"),
            P(None, "rep", BLK, None),
            P("rep"),
            P("rep"),
            P(None, BLK),
            P(),
            P(),
            P("rep", None),
            P(None, None, BLK),
            P(BLK, None),
        ),
        out_specs=P("rep", BLK),
        check_vma=False,
    )
```

```python
import functools
import math

import jax
import jax.numpy as jnp
from jax import lax
from jax.experimental import pallas as pl
from jax.experimental.pallas import tpu as pltpu
from jax.sharding import Mesh
from jax.sharding import PartitionSpec as P

QUERY_HEADS = 32
KEY_VALUE_HEADS = 8
HEAD_SIZE = 128
EXPERTS = 4
FF = 7168
BLK = ("blk_0", "blk_1", "blk_2")
GROUP = QUERY_HEADS // KEY_VALUE_HEADS
LANES = 128
SPAN = LANES // GROUP
IN_VMEM = pl.BlockSpec(memory_space=pltpu.VMEM)
IN_SMEM = pl.BlockSpec(memory_space=pltpu.SMEM)
IN_HBM = pl.BlockSpec(memory_space=pltpu.HBM)
BATCH = 4
CHUNKS = 4
MIB = 1 << 20
COVER = pl.CostEstimate(flops=8*10**8, bytes_accessed=8 << 20, transcendentals=0)
ALL_VMEM = 67043328


def exchanged(pieces, axis=BLK):
    return lax.all_to_all(pieces, axis, 0, 0, tiled=True)


def merging(kernel, shape, *pieces):
    return pl.pallas_call(
        kernel,
        out_shape=jax.ShapeDtypeStruct(shape, jnp.bfloat16),
        in_specs=[IN_VMEM] * len(pieces),
        out_specs=IN_VMEM,
        compiler_params=params(8),
        cost_estimate=COVER,
        name=kernel.__name__,
    )(*pieces)


def params(mib):
    return pltpu.CompilerParams(vmem_limit_bytes=mib * MIB)


def attention_kernel(
    positions,
    first,
    lengths_in,
    insert_slot_in,
    prefix_len_in,
    queries_in,
    weight_in,
    cache,
    inserted,
    out,
    lengths,
    insert_slot,
    prefix_len,
    queries,
    weight,
    spread,
    rows,
    score_of,
    values,
    stats,
    sems,
):
    slots, prefixes, count = lengths.shape[0], insert_slot.shape[0], rows.shape[2]
    wide = QUERY_HEADS
    copies = [
        pltpu.make_async_copy(lengths_in, lengths, sems.at[0]),
        pltpu.make_async_copy(insert_slot_in, insert_slot, sems.at[1]),
        pltpu.make_async_copy(prefix_len_in, prefix_len, sems.at[2]),
        pltpu.make_async_copy(queries_in, queries, sems.at[3]),
        pltpu.make_async_copy(weight_in, weight, sems.at[4]),
    ]
    copies += [
        pltpu.make_async_copy(cache.at[k, s], rows.at[s, k], sems.at[5 + 2 * s + k])
        for s in range(slots)
        for k in range(2)
    ]
    copies += [
        pltpu.make_async_copy(
            inserted.at[k, j], rows.at[slots + j, k], sems.at[5 + 2 * (slots + j) + k]
        )
        for j in range(prefixes)
        for k in range(2)
    ]
    for copy in copies:
        copy.start()
    for copy in copies[:4]:
        copy.wait()
    for g in range(KEY_VALUE_HEADS):
        for h in range(GROUP):
            at = (g * GROUP + h) * HEAD_SIZE
            one = queries[:, at : at + HEAD_SIZE].astype(jnp.float32)
            spread[pl.ds(g * GROUP + h, slots, stride=wide), :] = one
    here = first[0]
    half = positions // 2
    there = jnp.where(here < half, here + half, here - half)
    valid, source = [], []
    for s in range(slots):
        length, at, start = lengths[s], jnp.int32(s), here
        for j in range(prefixes):
            mine = insert_slot[j] == s
            length = jnp.where(mine, prefix_len[j], length)
            at = jnp.where(mine, slots + j, at)
            start = jnp.where(mine, there, start)
        valid.append(length - start)
        source.append(at)
    for copy in copies[4:]:
        copy.wait()
    shape = (wide, KEY_VALUE_HEADS * HEAD_SIZE)
    own = (
        lax.broadcasted_iota(jnp.int32, shape, 0) // GROUP
        == lax.broadcasted_iota(jnp.int32, shape, 1) // HEAD_SIZE
    )
    row = lax.broadcasted_iota(jnp.int32, (wide, HEAD_SIZE), 0)
    lane = lax.broadcasted_iota(jnp.int32, (wide, HEAD_SIZE), 1)
    counted = lane // SPAN == row % GROUP
    early = lax.broadcasted_iota(jnp.int32, (2 * GROUP, HEAD_SIZE), 0) < GROUP
    place = lax.broadcasted_iota(jnp.int32, (wide, count), 1)
    for s in range(slots):
        one = spread[s * wide : (s + 1) * wide, :]
        tiled = jnp.concatenate([one] * KEY_VALUE_HEADS, axis=1)
        blocks = jnp.where(own, tiled, 0.0).astype(jnp.bfloat16)
        score_of[s] = lax.dot_general(
            blocks,
            rows[source[s], 0],
            (((1,), (1,)), ((), ())),
            preferred_element_type=jnp.float32,
        ) * (1.0 / math.sqrt(HEAD_SIZE))
    for batch in range(0, slots, BATCH):
        several = range(batch, batch + BATCH)
        inside = [place < valid[s] for s in several]
        scores = [jnp.where(i, score_of[s], -1e30) for i, s in zip(inside, several)]
        peaks = [jnp.max(x, axis=1, keepdims=True) for x in scores]
        peaks = [x.astype(jnp.bfloat16).astype(jnp.float32) for x in peaks]
        weights = [
            jnp.where(i, jnp.exp(x - p), 0.0) for i, x, p in zip(inside, scores, peaks)
        ]
        totals = [jnp.sum(x, axis=1, keepdims=True) for x in weights]
        every = [
            jnp.dot(
                x.astype(jnp.bfloat16), rows[source[s], 1], preferred_element_type=jnp.float32
            )
            for x, s in zip(weights, several)
        ]
        for s, full, peak, total in zip(several, every, peaks, totals):
            value = jnp.concatenate(
                [
                    jnp.where(
                        early,
                        full[g * GROUP : (g + 2) * GROUP, g * HEAD_SIZE : (g + 1) * HEAD_SIZE],
                        full[
                            g * GROUP : (g + 2) * GROUP, (g + 1) * HEAD_SIZE : (g + 2) * HEAD_SIZE
                        ],
                    )
                    for g in range(0, KEY_VALUE_HEADS, 2)
                ],
                axis=0,
            )
            values[pl.ds(s, wide, stride=slots), :] = value / jnp.where(total > 0.0, total, 1.0)
            stats[pl.ds(s, wide, stride=slots), :] = jnp.where(
                counted, packed_stats(lane, peak, total), 0.0
            )
    deep = GROUP * slots
    for g in range(KEY_VALUE_HEADS):
        out[g, :deep, :] = values[g * deep : (g + 1) * deep, :].astype(jnp.bfloat16)
        one = [stats[g * deep + h * slots : g * deep + (h + 1) * slots, :] for h in range(GROUP)]
        out[g, deep : deep + slots, :] = sum(one).astype(jnp.bfloat16)
        for h in range(GROUP):
            at = deep + slots + h * weight.shape[0]
            head = (g * GROUP + h) * HEAD_SIZE
            out[g, at : at + weight.shape[0], :] = weight[:, head : head + HEAD_SIZE]


def packed_stats(lane, peak, total):
    rounded = total.astype(jnp.bfloat16).astype(jnp.float32)
    at = lane % SPAN
    return jnp.where(
        at < SPAN // 2, peak, jnp.where(at < SPAN * 3 // 4, rounded, total - rounded)
    )


def merge(pieces):
    slots = pieces[0].shape[0] // (GROUP + 1)
    found = [x[GROUP * slots :].astype(jnp.float32) for x in pieces]
    highest = functools.reduce(jnp.maximum, found)
    scales = [
        jnp.exp(x - highest)
        * (
            pltpu.roll(x, LANES - SPAN // 2, axis=1)
            + pltpu.roll(x, LANES - SPAN * 3 // 4, axis=1)
        )
        for x in found
    ]
    total = sum(scales)
    safe = jnp.where(total > 0.0, total, 1.0)
    values = []
    for h in range(GROUP):
        column = slice(h * SPAN, h * SPAN + 1)
        parts = [
            x[h * slots : (h + 1) * slots].astype(jnp.float32) * y[:, column]
            for x, y in zip(pieces, scales)
        ]
        values.append(sum(parts) / safe[:, column])
    return values, highest, total


def whole_part(pieces):
    values, highest, total = merge(pieces)
    lane = lax.broadcasted_iota(jnp.int32, highest.shape, 1)
    total = pltpu.roll(total, SPAN // 2, axis=1)
    rounded = total.astype(jnp.bfloat16).astype(jnp.float32)
    rest = pltpu.roll(total - rounded, SPAN // 4, axis=1)
    at = lane % SPAN
    stats = jnp.where(at < SPAN // 2, highest, jnp.where(at < SPAN * 3 // 4, rounded, rest))
    return jnp.concatenate(values + [stats], axis=0).astype(jnp.bfloat16)


def spread_kernel(pieces, out):
    part = whole_part([pieces[i, : out.shape[1], :] for i in range(pieces.shape[0])])
    for i in range(out.shape[0]):
        out[i] = part


def part_kernel(pieces, out):
    out[...] = whole_part([pieces[i] for i in range(pieces.shape[0])])


def project_kernel(place, mine, other, landed, hidden, out):
    slots, columns = hidden.shape
    count, deep = landed.shape[0], mine.shape[0]
    values, _, _ = merge([mine[...], other[...]])
    attn = jnp.concatenate(values, axis=1).astype(jnp.bfloat16)
    heads = []
    for h in range(GROUP):
        at = deep + h * columns
        parts = [landed[i, at : at + columns, :] for i in range(count)]
        heads.append(jnp.concatenate(parts, axis=0))
    weight = jnp.concatenate(heads, axis=1)
    total = lax.dot_general(
        attn, weight, (((1,), (1,)), ((), ())), preferred_element_type=jnp.float32
    )
    tiled = jnp.concatenate([hidden[...].astype(jnp.float32)] * count, axis=1)
    owner = lax.broadcasted_iota(jnp.int32, tiled.shape, 1) // columns
    part = (total + jnp.where(owner == place[0], tiled, 0.0)).astype(jnp.bfloat16)
    for i in range(count):
        out[i] = part


def mixed_kernel(place, pieces, own, out):
    columns = own.shape[1]
    total = pieces[0].astype(jnp.float32)
    for i in range(1, pieces.shape[0]):
        total = total + pieces[i].astype(jnp.float32)
    mixed = total.astype(jnp.bfloat16)
    for i in range(out.shape[0]):
        out[i] = mixed
    mine = [total[:, i * columns : (i + 1) * columns] for i in range(pieces.shape[0])]
    own[...] = sum(jnp.where(place[0] == i, x, 0.0) for i, x in enumerate(mine)).astype(
        jnp.bfloat16
    )


def in_feature_order(gathered, share):
    count, slots, width = gathered.shape
    columns, rows, halves = LANES // share, count // share, width // LANES
    block = lax.broadcasted_iota(jnp.int32, (slots, LANES), 1) // columns
    tiles = {}
    for m in range(rows):
        for half in range(halves):
            found = [
                gathered[share * m + j, :, half * LANES : (half + 1) * LANES].astype(jnp.float32)
                for j in range(share)
            ]
            for b in range(share):
                tile = found[b]
                for j in range(share):
                    if j != b:
                        turned = pltpu.roll(found[j], (j - b) % share * columns, axis=1)
                        tile = jnp.where(block == j, turned, tile)
                tiles[(half * share + b) * rows + m] = tile
    return jnp.concatenate([tiles[k] for k in range(len(tiles))], axis=1)


def swapped(tiles, share):
    slots = tiles.shape[1]
    deep, width = slots // share, LANES // share
    row = lax.broadcasted_iota(jnp.int32, tiles.shape, 1) // deep
    lane = lax.broadcasted_iota(jnp.int32, tiles.shape, 2) // width
    turn = (lane - row + share) % share
    result = tiles
    for j in range(1, share):
        moved = pltpu.roll(pltpu.roll(tiles, j * width, axis=2), slots - j * deep, axis=1)
        result = jnp.where(turn == j, moved, result)
    return result


def experts_kernel(
    share, expert, gathered, gain, router, chosen, gate_up_in, down, out, gate_up, sems
):
    blocks, slots = out.shape[0], out.shape[1]
    step = blocks * LANES // CHUNKS
    copies = []
    for i in range(CHUNKS):
        lanes = pl.ds(i * step, step)
        copies.append(
            pltpu.make_async_copy(
                gate_up_in.at[:, :, lanes], gate_up.at[:, :, lanes], sems.at[i]
            )
        )
        copies[i].start()
    mixed = in_feature_order(gathered, share)
    scale = lax.rsqrt(jnp.sum(mixed * mixed, axis=1, keepdims=True) / (blocks * LANES) + 1e-05)
    normed = (mixed * scale * gain[...].astype(jnp.float32).reshape(1, blocks * LANES)).astype(jnp.bfloat16)
    plain = normed.astype(jnp.float32)
    weights = router[...].astype(jnp.float32)
    logits = [
        jnp.sum(plain * weights[e : e + 1], axis=1, keepdims=True) for e in range(EXPERTS)
    ]
    upright = lax.broadcasted_iota(jnp.int32, (slots, slots), 0) == lax.broadcasted_iota(
        jnp.int32, (slots, slots), 1
    )
    ids = [
        jnp.sum(
            jnp.where(upright, chosen[i : i + 1, :].astype(jnp.float32), 0.0),
            axis=1,
            keepdims=True,
        )
        for i in range(2)
    ]
    picked = [sum(jnp.where(k == e, logits[e], 0.0) for e in range(EXPERTS)) for k in ids]
    gates = [jax.nn.sigmoid(picked[i] - picked[1 - i]) for i in range(2)]
    mine = expert[0].astype(jnp.float32)
    part = sum(jnp.where(ids[i] == mine, gates[i], 0.0) for i in range(2))
    gate, up = 0.0, 0.0
    for i in range(CHUNKS):
        copies[i].wait()
        lanes = slice(i * step, (i + 1) * step)
        contract = functools.partial(
            lax.dot_general,
            normed[:, lanes],
            dimension_numbers=(((1,), (1,)), ((), ())),
            preferred_element_type=jnp.float32,
        )
        gate = gate + contract(gate_up[0, :, lanes])
        up = up + contract(gate_up[1, :, lanes])
    act = (gate * jax.nn.sigmoid(gate) * up).astype(jnp.bfloat16)
    term = part * jnp.dot(act, down[...], preferred_element_type=jnp.float32)
    tiles = [term[None, :, k * LANES : (k + 1) * LANES] for k in range(blocks)]
    out[...] = swapped(jnp.concatenate(tiles, axis=0), share).astype(jnp.bfloat16)


def final_kernel(pieces, mixed, out):
    slots, columns = mixed.shape
    share = LANES // columns
    total = jnp.sum(pieces[...].astype(jnp.float32), axis=0)
    moe = jnp.concatenate(
        [total[:, b * columns : (b + 1) * columns] for b in range(share)], axis=0
    )
    out[...] = (mixed[...].astype(jnp.float32) + moe).astype(jnp.bfloat16)


def on_device(
    hidden,
    queries,
    cache_kv,
    cache_len,
    inserted_key_value,
    insert_slot,
    prefix_len,
    out_weight,
    norm_gain,
    router_weight,
    expert_ids,
    gate_up,
    down_proj,
):
    devices = lax.axis_size(BLK)
    dev_index = lax.axis_index(BLK)
    slots, columns = hidden.shape
    ctx_rows, kv_width = cache_kv.shape[2:]
    prefixes = insert_slot.shape[0]
    share = LANES // columns
    deep = slots * (GROUP + 1)
    width = devices * columns
    blocks = width // LANES
    bf16 = jnp.bfloat16

    first = (dev_index * ctx_rows).astype(jnp.int32).reshape(1)
    partials = pl.pallas_call(
        functools.partial(attention_kernel, devices * ctx_rows),
        out_shape=jax.ShapeDtypeStruct((KEY_VALUE_HEADS, deep + GROUP * columns, HEAD_SIZE), bf16),
        in_specs=[IN_SMEM] + [IN_HBM] * 7,
        out_specs=IN_VMEM,
        scratch_shapes=[
            pltpu.SMEM((slots,), jnp.int32),
            pltpu.SMEM((prefixes,), jnp.int32),
            pltpu.SMEM((prefixes,), jnp.int32),
            pltpu.VMEM(queries.shape, bf16),
            pltpu.VMEM(out_weight.shape[::-1], bf16),
            pltpu.VMEM((slots * QUERY_HEADS, HEAD_SIZE), jnp.float32),
            pltpu.VMEM((slots + prefixes, 2, ctx_rows, kv_width), bf16),
            pltpu.VMEM((slots, QUERY_HEADS, ctx_rows), jnp.float32),
            pltpu.VMEM((slots * QUERY_HEADS, HEAD_SIZE), jnp.float32),
            pltpu.VMEM((slots * QUERY_HEADS, HEAD_SIZE), jnp.float32),
            pltpu.SemaphoreType.DMA((5 + 2 * (slots + prefixes),)),
        ],
        compiler_params=pltpu.CompilerParams(vmem_limit_bytes=ALL_VMEM),
        name="attention",
    )(first, cache_len, insert_slot, prefix_len, queries, out_weight.T, cache_kv, inserted_key_value)
    along, across, pair = BLK
    copies = lax.axis_size(across)
    landed = exchanged(partials, along)
    part = merging(spread_kernel, (copies, deep, HEAD_SIZE), landed)
    part = merging(part_kernel, (deep, HEAD_SIZE), exchanged(part, across))
    other = lax.ppermute(part, pair, [(0, 1), (1, 0)])
    count = lax.axis_size(along)
    place = lax.axis_index(along).astype(jnp.int32).reshape(1)
    parts = pl.pallas_call(
        project_kernel,
        out_shape=jax.ShapeDtypeStruct((count, slots, count * columns), bf16),
        in_specs=[IN_SMEM] + [IN_VMEM] * 4,
        out_specs=IN_VMEM,
        compiler_params=params(8),
        cost_estimate=COVER,
        name="project",
    )(place, part, other, landed, hidden)
    local_mixed, packed = pl.pallas_call(
        mixed_kernel,
        out_shape=(
            jax.ShapeDtypeStruct((slots, columns), bf16),
            jax.ShapeDtypeStruct((devices // count, slots, count * columns), bf16),
        ),
        in_specs=[IN_SMEM, IN_VMEM],
        out_specs=(IN_VMEM, IN_VMEM),
        compiler_params=params(8),
        cost_estimate=COVER,
        name="mixed",
    )(place, exchanged(parts, along))
    gathered = exchanged(packed, (across, pair))

    expert = (dev_index * gate_up.shape[2] // FF).astype(jnp.int32).reshape(1)
    terms = pl.pallas_call(
        functools.partial(experts_kernel, share),
        out_shape=jax.ShapeDtypeStruct((blocks, slots, LANES), bf16),
        in_specs=[IN_SMEM] + [IN_VMEM] * 4 + [IN_HBM, IN_VMEM],
        out_specs=IN_VMEM,
        scratch_shapes=[
            pltpu.VMEM((2, gate_up.shape[2], width), bf16),
            pltpu.SemaphoreType.DMA((CHUNKS,)),
        ],
        compiler_params=params(50),
        name="experts",
    )(
        expert,
        gathered,
        norm_gain,
        router_weight.T,
        expert_ids.T,
        jnp.swapaxes(gate_up, 1, 2),
        down_proj,
    )
    moe = exchanged(terms.reshape(devices, slots // share, LANES))
    return pl.pallas_call(
        final_kernel,
        out_shape=jax.ShapeDtypeStruct((slots, columns), bf16),
        in_specs=[IN_VMEM] * 2,
        out_specs=IN_VMEM,
        compiler_params=params(4),
        name="final",
    )(moe, local_mixed)


def solution(mesh):
    split = Mesh(
        mesh.devices.reshape(mesh.shape["rep"], 8, 8, 2), ("rep", "blk_0", "blk_1", "blk_2")
    )
    return jax.shard_map(
        on_device,
        mesh=split,
        in_specs=(
            P("rep", BLK),
            P("rep", None),
            P(None, "rep", BLK, None),
            P("rep"),
            P(None, "rep", BLK, None),
            P("rep"),
            P("rep"),
            P(None, BLK),
            P(),
            P(),
            P("rep", None),
            P(None, None, BLK),
            P(BLK, None),
        ),
        out_specs=P("rep", BLK),
        check_vma=False,
    )
```

```python
import functools
import math

import jax
import jax.numpy as jnp
from jax import lax
from jax.experimental import pallas as pl
from jax.experimental.pallas import tpu as pltpu
from jax.sharding import Mesh
from jax.sharding import PartitionSpec as P

QUERY_HEADS = 32
KEY_VALUE_HEADS = 8
HEAD_SIZE = 128
EXPERTS = 4
FF = 7168
BLK = ("blk_0", "blk_1", "blk_2")
GROUP = QUERY_HEADS // KEY_VALUE_HEADS
LANES = 128
SPAN = LANES // GROUP
IN_VMEM = pl.BlockSpec(memory_space=pltpu.VMEM)
IN_SMEM = pl.BlockSpec(memory_space=pltpu.SMEM)
IN_HBM = pl.BlockSpec(memory_space=pltpu.HBM)
BATCH = 4
CHUNKS = 4
MIB = 1 << 20
COVER = pl.CostEstimate(flops=8*10**8, bytes_accessed=8 << 20, transcendentals=0)
ALL_VMEM = 67043328


def exchanged(pieces, axis=BLK):
    return lax.all_to_all(pieces, axis, 0, 0, tiled=True)


def merging(kernel, shape, *pieces):
    return pl.pallas_call(
        kernel,
        out_shape=jax.ShapeDtypeStruct(shape, jnp.bfloat16),
        in_specs=[IN_VMEM] * len(pieces),
        out_specs=IN_VMEM,
        compiler_params=params(8),
        cost_estimate=COVER,
        name=kernel.__name__,
    )(*pieces)


def params(mib):
    return pltpu.CompilerParams(vmem_limit_bytes=mib * MIB)


def attention_kernel(
    positions,
    first,
    lengths_in,
    insert_slot_in,
    prefix_len_in,
    queries_in,
    weight_in,
    cache,
    inserted,
    out,
    lengths,
    insert_slot,
    prefix_len,
    queries,
    weight,
    spread,
    rows,
    score_of,
    values,
    stats,
    sems,
):
    slots, prefixes, count = lengths.shape[0], insert_slot.shape[0], rows.shape[2]
    wide = QUERY_HEADS
    copies = [
        pltpu.make_async_copy(lengths_in, lengths, sems.at[0]),
        pltpu.make_async_copy(insert_slot_in, insert_slot, sems.at[1]),
        pltpu.make_async_copy(prefix_len_in, prefix_len, sems.at[2]),
        pltpu.make_async_copy(queries_in, queries, sems.at[3]),
        pltpu.make_async_copy(weight_in, weight, sems.at[4]),
    ]
    key_copies, value_copies = [], []
    for k, group in enumerate((key_copies, value_copies)):
        for start in range(0, slots, BATCH):
            here = pl.ds(start, BATCH)
            group.append((cache.at[k, here], rows.at[k, here]))
        for start in range(0, prefixes, BATCH):
            group.append(
                (inserted.at[k, pl.ds(start, BATCH)], rows.at[k, pl.ds(slots + start, BATCH)])
            )
    for at, group in ((5, key_copies), (5 + len(key_copies), value_copies)):
        for i, (source_ref, target_ref) in enumerate(group):
            group[i] = pltpu.make_async_copy(source_ref, target_ref, sems.at[at + i])
    copies = copies[:4] + key_copies + value_copies + copies[4:]
    for copy in copies:
        copy.start()
    for copy in copies[:4]:
        copy.wait()
    for g in range(KEY_VALUE_HEADS):
        for h in range(GROUP):
            at = (g * GROUP + h) * HEAD_SIZE
            one = queries[:, at : at + HEAD_SIZE].astype(jnp.float32)
            spread[pl.ds(g * GROUP + h, slots, stride=wide), :] = one
    here = first[0]
    half = positions // 2
    there = jnp.where(here < half, here + half, here - half)
    valid, source = [], []
    for s in range(slots):
        length, at, start = lengths[s], jnp.int32(s), here
        for j in range(prefixes):
            mine = insert_slot[j] == s
            length = jnp.where(mine, prefix_len[j], length)
            at = jnp.where(mine, slots + j, at)
            start = jnp.where(mine, there, start)
        valid.append(length - start)
        source.append(at)
    for copy in key_copies:
        copy.wait()
    shape = (wide, KEY_VALUE_HEADS * HEAD_SIZE)
    own = (
        lax.broadcasted_iota(jnp.int32, shape, 0) // GROUP
        == lax.broadcasted_iota(jnp.int32, shape, 1) // HEAD_SIZE
    )
    row = lax.broadcasted_iota(jnp.int32, (wide, HEAD_SIZE), 0)
    lane = lax.broadcasted_iota(jnp.int32, (wide, HEAD_SIZE), 1)
    counted = lane // SPAN == row % GROUP
    early = lax.broadcasted_iota(jnp.int32, (2 * GROUP, HEAD_SIZE), 0) < GROUP
    place = lax.broadcasted_iota(jnp.int32, (wide, count), 1)
    for s in range(slots):
        one = spread[s * wide : (s + 1) * wide, :]
        tiled = jnp.concatenate([one] * KEY_VALUE_HEADS, axis=1)
        blocks = jnp.where(own, tiled, 0.0).astype(jnp.bfloat16)
        score_of[s] = lax.dot_general(
            blocks,
            rows[0, source[s]],
            (((1,), (1,)), ((), ())),
            preferred_element_type=jnp.float32,
        ) * (1.0 / math.sqrt(HEAD_SIZE))
    for copy in value_copies:
        copy.wait()
    for batch in range(0, slots, BATCH):
        several = range(batch, batch + BATCH)
        inside = [place < valid[s] for s in several]
        scores = [jnp.where(i, score_of[s], -1e30) for i, s in zip(inside, several)]
        peaks = [jnp.max(x, axis=1, keepdims=True) for x in scores]
        peaks = [x.astype(jnp.bfloat16).astype(jnp.float32) for x in peaks]
        weights = [
            jnp.where(i, jnp.exp(x - p), 0.0) for i, x, p in zip(inside, scores, peaks)
        ]
        totals = [jnp.sum(x, axis=1, keepdims=True) for x in weights]
        every = [
            jnp.dot(
                x.astype(jnp.bfloat16), rows[1, source[s]], preferred_element_type=jnp.float32
            )
            for x, s in zip(weights, several)
        ]
        for s, full, peak, total in zip(several, every, peaks, totals):
            value = jnp.concatenate(
                [
                    jnp.where(
                        early,
                        full[g * GROUP : (g + 2) * GROUP, g * HEAD_SIZE : (g + 1) * HEAD_SIZE],
                        full[
                            g * GROUP : (g + 2) * GROUP, (g + 1) * HEAD_SIZE : (g + 2) * HEAD_SIZE
                        ],
                    )
                    for g in range(0, KEY_VALUE_HEADS, 2)
                ],
                axis=0,
            )
            values[pl.ds(s, wide, stride=slots), :] = value / jnp.where(total > 0.0, total, 1.0)
            stats[pl.ds(s, wide, stride=slots), :] = jnp.where(
                counted, packed_stats(lane, peak, total), 0.0
            )
    deep = GROUP * slots
    copies[-1].wait()
    for g in range(KEY_VALUE_HEADS):
        out[g, :deep, :] = values[g * deep : (g + 1) * deep, :].astype(jnp.bfloat16)
        one = [stats[g * deep + h * slots : g * deep + (h + 1) * slots, :] for h in range(GROUP)]
        out[g, deep : deep + slots, :] = sum(one).astype(jnp.bfloat16)
        for h in range(GROUP):
            at = deep + slots + h * weight.shape[0]
            head = (g * GROUP + h) * HEAD_SIZE
            out[g, at : at + weight.shape[0], :] = weight[:, head : head + HEAD_SIZE]


def packed_stats(lane, peak, total):
    rounded = total.astype(jnp.bfloat16).astype(jnp.float32)
    at = lane % SPAN
    return jnp.where(
        at < SPAN // 2, peak, jnp.where(at < SPAN * 3 // 4, rounded, total - rounded)
    )


def merge(pieces):
    slots = pieces[0].shape[0] // (GROUP + 1)
    found = [x[GROUP * slots :].astype(jnp.float32) for x in pieces]
    highest = functools.reduce(jnp.maximum, found)
    scales = [
        jnp.exp(x - highest)
        * (
            pltpu.roll(x, LANES - SPAN // 2, axis=1)
            + pltpu.roll(x, LANES - SPAN * 3 // 4, axis=1)
        )
        for x in found
    ]
    total = sum(scales)
    safe = jnp.where(total > 0.0, total, 1.0)
    values = []
    for h in range(GROUP):
        column = slice(h * SPAN, h * SPAN + 1)
        parts = [
            x[h * slots : (h + 1) * slots].astype(jnp.float32) * y[:, column]
            for x, y in zip(pieces, scales)
        ]
        values.append(sum(parts) / safe[:, column])
    return values, highest, total


def whole_part(pieces):
    values, highest, total = merge(pieces)
    lane = lax.broadcasted_iota(jnp.int32, highest.shape, 1)
    total = pltpu.roll(total, SPAN // 2, axis=1)
    rounded = total.astype(jnp.bfloat16).astype(jnp.float32)
    rest = pltpu.roll(total - rounded, SPAN // 4, axis=1)
    at = lane % SPAN
    stats = jnp.where(at < SPAN // 2, highest, jnp.where(at < SPAN * 3 // 4, rounded, rest))
    return jnp.concatenate(values + [stats], axis=0).astype(jnp.bfloat16)


def spread_kernel(pieces, out):
    part = whole_part([pieces[i, : out.shape[1], :] for i in range(pieces.shape[0])])
    for i in range(out.shape[0]):
        out[i] = part


def part_kernel(pieces, out):
    out[...] = whole_part([pieces[i] for i in range(pieces.shape[0])])


def project_kernel(place, mine, other, landed, hidden, out):
    slots, columns = hidden.shape
    count, deep = landed.shape[0], mine.shape[0]
    values, _, _ = merge([mine[...], other[...]])
    attn = jnp.concatenate(values, axis=1).astype(jnp.bfloat16)
    heads = []
    for h in range(GROUP):
        at = deep + h * columns
        parts = [landed[i, at : at + columns, :] for i in range(count)]
        heads.append(jnp.concatenate(parts, axis=0))
    weight = jnp.concatenate(heads, axis=1)
    total = lax.dot_general(
        attn, weight, (((1,), (1,)), ((), ())), preferred_element_type=jnp.float32
    )
    tiled = jnp.concatenate([hidden[...].astype(jnp.float32)] * count, axis=1)
    owner = lax.broadcasted_iota(jnp.int32, tiled.shape, 1) // columns
    part = (total + jnp.where(owner == place[0], tiled, 0.0)).astype(jnp.bfloat16)
    for i in range(count):
        out[i] = part


def mixed_kernel(place, pieces, own, out):
    columns = own.shape[1]
    total = pieces[0].astype(jnp.float32)
    for i in range(1, pieces.shape[0]):
        total = total + pieces[i].astype(jnp.float32)
    mixed = total.astype(jnp.bfloat16)
    for i in range(out.shape[0]):
        out[i] = mixed
    mine = [total[:, i * columns : (i + 1) * columns] for i in range(pieces.shape[0])]
    own[...] = sum(jnp.where(place[0] == i, x, 0.0) for i, x in enumerate(mine)).astype(
        jnp.bfloat16
    )


def in_feature_order(gathered, share):
    count, slots, width = gathered.shape
    columns, rows, halves = LANES // share, count // share, width // LANES
    block = lax.broadcasted_iota(jnp.int32, (slots, LANES), 1) // columns
    tiles = {}
    for m in range(rows):
        for half in range(halves):
            found = [
                gathered[share * m + j, :, half * LANES : (half + 1) * LANES].astype(jnp.float32)
                for j in range(share)
            ]
            for b in range(share):
                tile = found[b]
                for j in range(share):
                    if j != b:
                        turned = pltpu.roll(found[j], (j - b) % share * columns, axis=1)
                        tile = jnp.where(block == j, turned, tile)
                tiles[(half * share + b) * rows + m] = tile
    return jnp.concatenate([tiles[k] for k in range(len(tiles))], axis=1)


def swapped(tiles, share):
    slots = tiles.shape[1]
    deep, width = slots // share, LANES // share
    row = lax.broadcasted_iota(jnp.int32, tiles.shape, 1) // deep
    lane = lax.broadcasted_iota(jnp.int32, tiles.shape, 2) // width
    turn = (lane - row + share) % share
    result = tiles
    for j in range(1, share):
        moved = pltpu.roll(pltpu.roll(tiles, j * width, axis=2), slots - j * deep, axis=1)
        result = jnp.where(turn == j, moved, result)
    return result


def experts_kernel(
    share, expert, gathered, gain, router, chosen, gate_up_in, down, out, gate_up, sems
):
    blocks, slots = out.shape[0], out.shape[1]
    step = blocks * LANES // CHUNKS
    copies = []
    for i in range(CHUNKS):
        lanes = pl.ds(i * step, step)
        copies.append(
            pltpu.make_async_copy(
                gate_up_in.at[:, :, lanes], gate_up.at[:, :, lanes], sems.at[i]
            )
        )
        copies[i].start()
    mixed = in_feature_order(gathered, share)
    scale = lax.rsqrt(jnp.sum(mixed * mixed, axis=1, keepdims=True) / (blocks * LANES) + 1e-05)
    normed = (mixed * scale * gain[...].astype(jnp.float32).reshape(1, blocks * LANES)).astype(jnp.bfloat16)
    plain = normed.astype(jnp.float32)
    weights = router[...].astype(jnp.float32)
    logits = [
        jnp.sum(plain * weights[e : e + 1], axis=1, keepdims=True) for e in range(EXPERTS)
    ]
    upright = lax.broadcasted_iota(jnp.int32, (slots, slots), 0) == lax.broadcasted_iota(
        jnp.int32, (slots, slots), 1
    )
    ids = [
        jnp.sum(
            jnp.where(upright, chosen[i : i + 1, :].astype(jnp.float32), 0.0),
            axis=1,
            keepdims=True,
        )
        for i in range(2)
    ]
    picked = [sum(jnp.where(k == e, logits[e], 0.0) for e in range(EXPERTS)) for k in ids]
    gates = [jax.nn.sigmoid(picked[i] - picked[1 - i]) for i in range(2)]
    mine = expert[0].astype(jnp.float32)
    part = sum(jnp.where(ids[i] == mine, gates[i], 0.0) for i in range(2))
    gate, up = 0.0, 0.0
    for i in range(CHUNKS):
        copies[i].wait()
        lanes = slice(i * step, (i + 1) * step)
        contract = functools.partial(
            lax.dot_general,
            normed[:, lanes],
            dimension_numbers=(((1,), (1,)), ((), ())),
            preferred_element_type=jnp.float32,
        )
        gate = gate + contract(gate_up[0, :, lanes])
        up = up + contract(gate_up[1, :, lanes])
    act = (gate * jax.nn.sigmoid(gate) * up).astype(jnp.bfloat16)
    term = part * jnp.dot(act, down[...], preferred_element_type=jnp.float32)
    tiles = [term[None, :, k * LANES : (k + 1) * LANES] for k in range(blocks)]
    out[...] = swapped(jnp.concatenate(tiles, axis=0), share).astype(jnp.bfloat16)


def final_kernel(pieces, mixed, out):
    slots, columns = mixed.shape
    share = LANES // columns
    total = jnp.sum(pieces[...].astype(jnp.float32), axis=0)
    moe = jnp.concatenate(
        [total[:, b * columns : (b + 1) * columns] for b in range(share)], axis=0
    )
    out[...] = (mixed[...].astype(jnp.float32) + moe).astype(jnp.bfloat16)


def on_device(
    hidden,
    queries,
    cache_kv,
    cache_len,
    inserted_key_value,
    insert_slot,
    prefix_len,
    out_weight,
    norm_gain,
    router_weight,
    expert_ids,
    gate_up,
    down_proj,
):
    devices = lax.axis_size(BLK)
    dev_index = lax.axis_index(BLK)
    slots, columns = hidden.shape
    ctx_rows, kv_width = cache_kv.shape[2:]
    prefixes = insert_slot.shape[0]
    share = LANES // columns
    deep = slots * (GROUP + 1)
    width = devices * columns
    blocks = width // LANES
    bf16 = jnp.bfloat16

    first = (dev_index * ctx_rows).astype(jnp.int32).reshape(1)
    place = lax.axis_index(BLK[0]).astype(jnp.int32).reshape(1)
    expert = (dev_index * gate_up.shape[2] // FF).astype(jnp.int32).reshape(1)
    first, place, expert = lax.optimization_barrier((first, place, expert))
    partials = pl.pallas_call(
        functools.partial(attention_kernel, devices * ctx_rows),
        out_shape=jax.ShapeDtypeStruct((KEY_VALUE_HEADS, deep + GROUP * columns, HEAD_SIZE), bf16),
        in_specs=[IN_SMEM] + [IN_HBM] * 7,
        out_specs=IN_VMEM,
        scratch_shapes=[
            pltpu.SMEM((slots,), jnp.int32),
            pltpu.SMEM((prefixes,), jnp.int32),
            pltpu.SMEM((prefixes,), jnp.int32),
            pltpu.VMEM(queries.shape, bf16),
            pltpu.VMEM(out_weight.shape[::-1], bf16),
            pltpu.VMEM((slots * QUERY_HEADS, HEAD_SIZE), jnp.float32),
            pltpu.VMEM((2, slots + prefixes, ctx_rows, kv_width), bf16),
            pltpu.VMEM((slots, QUERY_HEADS, ctx_rows), jnp.float32),
            pltpu.VMEM((slots * QUERY_HEADS, HEAD_SIZE), jnp.float32),
            pltpu.VMEM((slots * QUERY_HEADS, HEAD_SIZE), jnp.float32),
            pltpu.SemaphoreType.DMA((5 + 2 * (slots + prefixes) // BATCH,)),
        ],
        compiler_params=pltpu.CompilerParams(vmem_limit_bytes=ALL_VMEM),
        name="attention",
    )(first, cache_len, insert_slot, prefix_len, queries, out_weight.T, cache_kv, inserted_key_value)
    along, across, pair = BLK
    copies = lax.axis_size(across)
    landed = exchanged(partials, along)
    part = merging(spread_kernel, (copies, deep, HEAD_SIZE), landed)
    part = merging(part_kernel, (deep, HEAD_SIZE), exchanged(part, across))
    other = lax.ppermute(part, pair, [(0, 1), (1, 0)])
    count = lax.axis_size(along)
    parts = pl.pallas_call(
        project_kernel,
        out_shape=jax.ShapeDtypeStruct((count, slots, count * columns), bf16),
        in_specs=[IN_SMEM] + [IN_VMEM] * 4,
        out_specs=IN_VMEM,
        compiler_params=params(8),
        cost_estimate=COVER,
        name="project",
    )(place, part, other, landed, hidden)
    local_mixed, packed = pl.pallas_call(
        mixed_kernel,
        out_shape=(
            jax.ShapeDtypeStruct((slots, columns), bf16),
            jax.ShapeDtypeStruct((devices // count, slots, count * columns), bf16),
        ),
        in_specs=[IN_SMEM, IN_VMEM],
        out_specs=(IN_VMEM, IN_VMEM),
        compiler_params=params(8),
        cost_estimate=COVER,
        name="mixed",
    )(place, exchanged(parts, along))
    gathered = exchanged(packed, (across, pair))

    terms = pl.pallas_call(
        functools.partial(experts_kernel, share),
        out_shape=jax.ShapeDtypeStruct((blocks, slots, LANES), bf16),
        in_specs=[IN_SMEM] + [IN_VMEM] * 4 + [IN_HBM, IN_VMEM],
        out_specs=IN_VMEM,
        scratch_shapes=[
            pltpu.VMEM((2, gate_up.shape[2], width), bf16),
            pltpu.SemaphoreType.DMA((CHUNKS,)),
        ],
        compiler_params=params(50),
        name="experts",
    )(
        expert,
        gathered,
        norm_gain,
        router_weight.T,
        expert_ids.T,
        jnp.swapaxes(gate_up, 1, 2),
        down_proj,
    )
    moe = exchanged(terms.reshape(devices, slots // share, LANES))
    return pl.pallas_call(
        final_kernel,
        out_shape=jax.ShapeDtypeStruct((slots, columns), bf16),
        in_specs=[IN_VMEM] * 2,
        out_specs=IN_VMEM,
        compiler_params=params(4),
        name="final",
    )(moe, local_mixed)


def solution(mesh):
    split = Mesh(
        mesh.devices.reshape(mesh.shape["rep"], 8, 8, 2), ("rep", "blk_0", "blk_1", "blk_2")
    )
    return jax.shard_map(
        on_device,
        mesh=split,
        in_specs=(
            P("rep", BLK),
            P("rep", None),
            P(None, "rep", BLK, None),
            P("rep"),
            P(None, "rep", BLK, None),
            P("rep"),
            P("rep"),
            P(None, BLK),
            P(),
            P(),
            P("rep", None),
            P(None, None, BLK),
            P(BLK, None),
        ),
        out_specs=P("rep", BLK),
        check_vma=False,
    )
```

```python
import functools
import math

import jax
import jax.numpy as jnp
from jax import lax
from jax.experimental import pallas as pl
from jax.experimental.pallas import tpu as pltpu
from jax.sharding import Mesh
from jax.sharding import PartitionSpec as P

QUERY_HEADS = 32
KEY_VALUE_HEADS = 8
HEAD_SIZE = 128
EXPERTS = 4
FF = 7168
BLK = ("blk_0", "blk_1", "blk_2")
GROUP = QUERY_HEADS // KEY_VALUE_HEADS
LANES = 128
SPAN = LANES // GROUP
IN_VMEM = pl.BlockSpec(memory_space=pltpu.VMEM)
IN_SMEM = pl.BlockSpec(memory_space=pltpu.SMEM)
IN_HBM = pl.BlockSpec(memory_space=pltpu.HBM)
BATCH = 4
CHUNKS = 8
MIB = 1 << 20
COVER = pl.CostEstimate(flops=8*10**8, bytes_accessed=8 << 20, transcendentals=0)
ALL_VMEM = 67043328


def exchanged(pieces, axis=BLK):
    return lax.all_to_all(pieces, axis, 0, 0, tiled=True)


def merging(kernel, shape, *pieces):
    return pl.pallas_call(
        kernel,
        out_shape=jax.ShapeDtypeStruct(shape, jnp.bfloat16),
        in_specs=[IN_VMEM] * len(pieces),
        out_specs=IN_VMEM,
        compiler_params=params(8),
        cost_estimate=COVER,
        name=kernel.__name__,
    )(*pieces)


def params(mib):
    return pltpu.CompilerParams(vmem_limit_bytes=mib * MIB)


def attention_kernel(
    positions,
    first,
    lengths_in,
    insert_slot_in,
    prefix_len_in,
    queries_in,
    weight_in,
    cache,
    inserted,
    out,
    lengths,
    insert_slot,
    prefix_len,
    queries,
    weight,
    spread,
    rows,
    score_of,
    values,
    stats,
    sems,
):
    slots, prefixes, count = lengths.shape[0], insert_slot.shape[0], rows.shape[2]
    wide = QUERY_HEADS
    copies = [
        pltpu.make_async_copy(lengths_in, lengths, sems.at[0]),
        pltpu.make_async_copy(insert_slot_in, insert_slot, sems.at[1]),
        pltpu.make_async_copy(prefix_len_in, prefix_len, sems.at[2]),
        pltpu.make_async_copy(queries_in, queries, sems.at[3]),
        pltpu.make_async_copy(weight_in, weight, sems.at[4]),
    ]
    key_copies, value_copies = [], []
    for k, group in enumerate((key_copies, value_copies)):
        for start in range(0, slots, BATCH):
            here = pl.ds(start, BATCH)
            group.append((cache.at[k, here], rows.at[k, here]))
        for start in range(0, prefixes, BATCH):
            group.append(
                (inserted.at[k, pl.ds(start, BATCH)], rows.at[k, pl.ds(slots + start, BATCH)])
            )
    for at, group in ((5, key_copies), (5 + len(key_copies), value_copies)):
        for i, (source_ref, target_ref) in enumerate(group):
            group[i] = pltpu.make_async_copy(source_ref, target_ref, sems.at[at + i])
    copies = copies[:4] + key_copies + value_copies + copies[4:]
    for copy in copies:
        copy.start()
    for copy in copies[:4]:
        copy.wait()
    for g in range(KEY_VALUE_HEADS):
        for h in range(GROUP):
            at = (g * GROUP + h) * HEAD_SIZE
            one = queries[:, at : at + HEAD_SIZE].astype(jnp.float32)
            spread[pl.ds(g * GROUP + h, slots, stride=wide), :] = one
    here = first[0]
    half = positions // 2
    there = jnp.where(here < half, here + half, here - half)
    valid, source = [], []
    for s in range(slots):
        length, at, start = lengths[s], jnp.int32(s), here
        for j in range(prefixes):
            mine = insert_slot[j] == s
            length = jnp.where(mine, prefix_len[j], length)
            at = jnp.where(mine, slots + j, at)
            start = jnp.where(mine, there, start)
        valid.append(length - start)
        source.append(at)
    for copy in key_copies:
        copy.wait()
    shape = (wide, KEY_VALUE_HEADS * HEAD_SIZE)
    own = (
        lax.broadcasted_iota(jnp.int32, shape, 0) // GROUP
        == lax.broadcasted_iota(jnp.int32, shape, 1) // HEAD_SIZE
    )
    row = lax.broadcasted_iota(jnp.int32, (wide, HEAD_SIZE), 0)
    lane = lax.broadcasted_iota(jnp.int32, (wide, HEAD_SIZE), 1)
    counted = lane // SPAN == row % GROUP
    early = lax.broadcasted_iota(jnp.int32, (2 * GROUP, HEAD_SIZE), 0) < GROUP
    place = lax.broadcasted_iota(jnp.int32, (wide, count), 1)
    for s in range(slots):
        one = spread[s * wide : (s + 1) * wide, :]
        tiled = jnp.concatenate([one] * KEY_VALUE_HEADS, axis=1)
        blocks = jnp.where(own, tiled, 0.0).astype(jnp.bfloat16)
        score_of[s] = lax.dot_general(
            blocks,
            rows[0, source[s]],
            (((1,), (1,)), ((), ())),
            preferred_element_type=jnp.float32,
        ) * (1.0 / math.sqrt(HEAD_SIZE))
    for copy in value_copies:
        copy.wait()
    for batch in range(0, slots, BATCH):
        several = range(batch, batch + BATCH)
        inside = [place < valid[s] for s in several]
        scores = [jnp.where(i, score_of[s], -1e30) for i, s in zip(inside, several)]
        peaks = [jnp.max(x, axis=1, keepdims=True) for x in scores]
        peaks = [x.astype(jnp.bfloat16).astype(jnp.float32) for x in peaks]
        weights = [
            jnp.where(i, jnp.exp(x - p), 0.0) for i, x, p in zip(inside, scores, peaks)
        ]
        totals = [jnp.sum(x, axis=1, keepdims=True) for x in weights]
        every = [
            jnp.dot(
                x.astype(jnp.bfloat16), rows[1, source[s]], preferred_element_type=jnp.float32
            )
            for x, s in zip(weights, several)
        ]
        for s, full, peak, total in zip(several, every, peaks, totals):
            value = jnp.concatenate(
                [
                    jnp.where(
                        early,
                        full[g * GROUP : (g + 2) * GROUP, g * HEAD_SIZE : (g + 1) * HEAD_SIZE],
                        full[
                            g * GROUP : (g + 2) * GROUP, (g + 1) * HEAD_SIZE : (g + 2) * HEAD_SIZE
                        ],
                    )
                    for g in range(0, KEY_VALUE_HEADS, 2)
                ],
                axis=0,
            )
            values[pl.ds(s, wide, stride=slots), :] = value / jnp.where(total > 0.0, total, 1.0)
            stats[pl.ds(s, wide, stride=slots), :] = jnp.where(
                counted, packed_stats(lane, peak, total), 0.0
            )
    deep = GROUP * slots
    copies[-1].wait()
    for g in range(KEY_VALUE_HEADS):
        out[g, :deep, :] = values[g * deep : (g + 1) * deep, :].astype(jnp.bfloat16)
        one = [stats[g * deep + h * slots : g * deep + (h + 1) * slots, :] for h in range(GROUP)]
        out[g, deep : deep + slots, :] = sum(one).astype(jnp.bfloat16)
        for h in range(GROUP):
            at = deep + slots + h * weight.shape[0]
            head = (g * GROUP + h) * HEAD_SIZE
            out[g, at : at + weight.shape[0], :] = weight[:, head : head + HEAD_SIZE]


def packed_stats(lane, peak, total):
    rounded = total.astype(jnp.bfloat16).astype(jnp.float32)
    at = lane % SPAN
    return jnp.where(
        at < SPAN // 2, peak, jnp.where(at < SPAN * 3 // 4, rounded, total - rounded)
    )


def merge(pieces):
    slots = pieces[0].shape[0] // (GROUP + 1)
    found = [x[GROUP * slots :].astype(jnp.float32) for x in pieces]
    highest = functools.reduce(jnp.maximum, found)
    scales = [
        jnp.exp(x - highest)
        * (
            pltpu.roll(x, LANES - SPAN // 2, axis=1)
            + pltpu.roll(x, LANES - SPAN * 3 // 4, axis=1)
        )
        for x in found
    ]
    total = sum(scales)
    safe = jnp.where(total > 0.0, total, 1.0)
    values = []
    for h in range(GROUP):
        column = slice(h * SPAN, h * SPAN + 1)
        parts = [
            x[h * slots : (h + 1) * slots].astype(jnp.float32) * y[:, column]
            for x, y in zip(pieces, scales)
        ]
        values.append(sum(parts) / safe[:, column])
    return values, highest, total


def whole_part(pieces):
    values, highest, total = merge(pieces)
    lane = lax.broadcasted_iota(jnp.int32, highest.shape, 1)
    total = pltpu.roll(total, SPAN // 2, axis=1)
    rounded = total.astype(jnp.bfloat16).astype(jnp.float32)
    rest = pltpu.roll(total - rounded, SPAN // 4, axis=1)
    at = lane % SPAN
    stats = jnp.where(at < SPAN // 2, highest, jnp.where(at < SPAN * 3 // 4, rounded, rest))
    return jnp.concatenate(values + [stats], axis=0).astype(jnp.bfloat16)


def spread_kernel(pieces, out):
    part = whole_part([pieces[i, : out.shape[1], :] for i in range(pieces.shape[0])])
    for i in range(out.shape[0]):
        out[i] = part


def part_kernel(pieces, out):
    out[...] = whole_part([pieces[i] for i in range(pieces.shape[0])])


def project_kernel(place, mine, other, landed, hidden, out):
    slots, columns = hidden.shape
    count, deep = landed.shape[0], mine.shape[0]
    values, _, _ = merge([mine[...], other[...]])
    attn = jnp.concatenate(values, axis=1).astype(jnp.bfloat16)
    heads = []
    for h in range(GROUP):
        at = deep + h * columns
        parts = [landed[i, at : at + columns, :] for i in range(count)]
        heads.append(jnp.concatenate(parts, axis=0))
    weight = jnp.concatenate(heads, axis=1)
    total = lax.dot_general(
        attn, weight, (((1,), (1,)), ((), ())), preferred_element_type=jnp.float32
    )
    tiled = jnp.concatenate([hidden[...].astype(jnp.float32)] * count, axis=1)
    owner = lax.broadcasted_iota(jnp.int32, tiled.shape, 1) // columns
    part = (total + jnp.where(owner == place[0], tiled, 0.0)).astype(jnp.bfloat16)
    for i in range(count):
        out[i] = part


def mixed_kernel(place, pieces, own, out):
    columns = own.shape[1]
    total = pieces[0].astype(jnp.float32)
    for i in range(1, pieces.shape[0]):
        total = total + pieces[i].astype(jnp.float32)
    mixed = total.astype(jnp.bfloat16)
    for i in range(out.shape[0]):
        out[i] = mixed
    mine = [total[:, i * columns : (i + 1) * columns] for i in range(pieces.shape[0])]
    own[...] = sum(jnp.where(place[0] == i, x, 0.0) for i, x in enumerate(mine)).astype(
        jnp.bfloat16
    )


def in_feature_order(gathered, share):
    count, slots, width = gathered.shape
    columns, rows, halves = LANES // share, count // share, width // LANES
    block = lax.broadcasted_iota(jnp.int32, (slots, LANES), 1) // columns
    tiles = {}
    for m in range(rows):
        for half in range(halves):
            found = [
                gathered[share * m + j, :, half * LANES : (half + 1) * LANES].astype(jnp.float32)
                for j in range(share)
            ]
            for b in range(share):
                tile = found[b]
                for j in range(share):
                    if j != b:
                        turned = pltpu.roll(found[j], (j - b) % share * columns, axis=1)
                        tile = jnp.where(block == j, turned, tile)
                tiles[(half * share + b) * rows + m] = tile
    return jnp.concatenate([tiles[k] for k in range(len(tiles))], axis=1)


def swapped(tiles, share):
    slots = tiles.shape[1]
    deep, width = slots // share, LANES // share
    row = lax.broadcasted_iota(jnp.int32, tiles.shape, 1) // deep
    lane = lax.broadcasted_iota(jnp.int32, tiles.shape, 2) // width
    turn = (lane - row + share) % share
    result = tiles
    for j in range(1, share):
        moved = pltpu.roll(pltpu.roll(tiles, j * width, axis=2), slots - j * deep, axis=1)
        result = jnp.where(turn == j, moved, result)
    return result


def experts_kernel(
    share, expert, core, gathered, gain, router, chosen, gate_up_in, down, own, other, gate_up, sems
):
    blocks, slots = own.shape[0], 2 * own.shape[1]
    step = blocks * LANES // CHUNKS
    copies = []
    for i in range(CHUNKS):
        lanes = pl.ds(i * step, step)
        copies.append(
            pltpu.make_async_copy(
                gate_up_in.at[:, :, lanes], gate_up.at[:, :, lanes], sems.at[i]
            )
        )
        copies[i].start()
    mixed = in_feature_order(gathered, share)
    scale = lax.rsqrt(jnp.sum(mixed * mixed, axis=1, keepdims=True) / (blocks * LANES) + 1e-05)
    normed = (mixed * scale * gain[...].astype(jnp.float32).reshape(1, blocks * LANES)).astype(jnp.bfloat16)
    plain = normed.astype(jnp.float32)
    weights = router[...].astype(jnp.float32)
    logits = [
        jnp.sum(plain * weights[e : e + 1], axis=1, keepdims=True) for e in range(EXPERTS)
    ]
    upright = lax.broadcasted_iota(jnp.int32, (slots, slots), 0) == lax.broadcasted_iota(
        jnp.int32, (slots, slots), 1
    )
    ids = [
        jnp.sum(
            jnp.where(upright, chosen[i : i + 1, :].astype(jnp.float32), 0.0),
            axis=1,
            keepdims=True,
        )
        for i in range(2)
    ]
    picked = [sum(jnp.where(k == e, logits[e], 0.0) for e in range(EXPERTS)) for k in ids]
    gates = [jax.nn.sigmoid(picked[i] - picked[1 - i]) for i in range(2)]
    mine = expert[0].astype(jnp.float32)
    part = sum(jnp.where(ids[i] == mine, gates[i], 0.0) for i in range(2))
    gate, up = 0.0, 0.0
    for i in range(CHUNKS):
        copies[i].wait()
        lanes = slice(i * step, (i + 1) * step)
        contract = functools.partial(
            lax.dot_general,
            normed[:, lanes],
            dimension_numbers=(((1,), (1,)), ((), ())),
            preferred_element_type=jnp.float32,
        )
        gate = gate + contract(gate_up[0, :, lanes])
        up = up + contract(gate_up[1, :, lanes])
    act = (gate * jax.nn.sigmoid(gate) * up).astype(jnp.bfloat16)
    term = part * jnp.dot(act, down[...], preferred_element_type=jnp.float32)
    tiles = [term[None, :, k * LANES : (k + 1) * LANES] for k in range(blocks)]
    even, odd = by_core(swapped(jnp.concatenate(tiles, axis=0), share), slots // share)
    own[...] = jnp.where(core[0] == 0, even, odd)
    other[...] = jnp.where(core[0] == 0, odd, even).astype(jnp.bfloat16)


def by_core(tiles, deep):
    top, bottom = tiles[:, : 2 * deep], tiles[:, 2 * deep :]
    first = lax.broadcasted_iota(jnp.int32, top.shape, 1) < deep
    even = jnp.where(first, top, pltpu.roll(bottom, deep, axis=1))
    odd = jnp.where(first, pltpu.roll(top, deep, axis=1), bottom)
    return even, odd


def add_kernel(own, other, out):
    out[...] = (own[...] + other[...].astype(jnp.float32)).astype(jnp.bfloat16)


def final_kernel(pieces, mixed, out):
    slots, columns = mixed.shape
    share = LANES // columns
    total = jnp.sum(pieces[...].astype(jnp.float32), axis=0)
    moe = jnp.concatenate(
        [total[:, b * columns : (b + 1) * columns] for b in range(share)], axis=0
    )
    out[...] = (mixed[...].astype(jnp.float32) + moe).astype(jnp.bfloat16)


def on_device(
    hidden,
    queries,
    cache_kv,
    cache_len,
    inserted_key_value,
    insert_slot,
    prefix_len,
    out_weight,
    norm_gain,
    router_weight,
    expert_ids,
    gate_up,
    down_proj,
):
    devices = lax.axis_size(BLK)
    dev_index = lax.axis_index(BLK)
    slots, columns = hidden.shape
    ctx_rows, kv_width = cache_kv.shape[2:]
    prefixes = insert_slot.shape[0]
    share = LANES // columns
    deep = slots * (GROUP + 1)
    width = devices * columns
    blocks = width // LANES
    bf16 = jnp.bfloat16

    first = (dev_index * ctx_rows).astype(jnp.int32).reshape(1)
    place = lax.axis_index(BLK[0]).astype(jnp.int32).reshape(1)
    expert = (dev_index * gate_up.shape[2] // FF).astype(jnp.int32).reshape(1)
    core = lax.axis_index(BLK[2]).astype(jnp.int32).reshape(1)
    first, place, expert, core = lax.optimization_barrier((first, place, expert, core))
    partials = pl.pallas_call(
        functools.partial(attention_kernel, devices * ctx_rows),
        out_shape=jax.ShapeDtypeStruct((KEY_VALUE_HEADS, deep + GROUP * columns, HEAD_SIZE), bf16),
        in_specs=[IN_SMEM] + [IN_HBM] * 7,
        out_specs=IN_VMEM,
        scratch_shapes=[
            pltpu.SMEM((slots,), jnp.int32),
            pltpu.SMEM((prefixes,), jnp.int32),
            pltpu.SMEM((prefixes,), jnp.int32),
            pltpu.VMEM(queries.shape, bf16),
            pltpu.VMEM(out_weight.shape[::-1], bf16),
            pltpu.VMEM((slots * QUERY_HEADS, HEAD_SIZE), jnp.float32),
            pltpu.VMEM((2, slots + prefixes, ctx_rows, kv_width), bf16),
            pltpu.VMEM((slots, QUERY_HEADS, ctx_rows), jnp.float32),
            pltpu.VMEM((slots * QUERY_HEADS, HEAD_SIZE), jnp.float32),
            pltpu.VMEM((slots * QUERY_HEADS, HEAD_SIZE), jnp.float32),
            pltpu.SemaphoreType.DMA((5 + 2 * (slots + prefixes) // BATCH,)),
        ],
        compiler_params=pltpu.CompilerParams(vmem_limit_bytes=ALL_VMEM),
        name="attention",
    )(first, cache_len, insert_slot, prefix_len, queries, out_weight.T, cache_kv, inserted_key_value)
    along, across, pair = BLK
    copies = lax.axis_size(across)
    landed = exchanged(partials, along)
    part = merging(spread_kernel, (copies, deep, HEAD_SIZE), landed)
    part = merging(part_kernel, (deep, HEAD_SIZE), exchanged(part, across))
    other = lax.ppermute(part, pair, [(0, 1), (1, 0)])
    count = lax.axis_size(along)
    parts = pl.pallas_call(
        project_kernel,
        out_shape=jax.ShapeDtypeStruct((count, slots, count * columns), bf16),
        in_specs=[IN_SMEM] + [IN_VMEM] * 4,
        out_specs=IN_VMEM,
        compiler_params=params(8),
        cost_estimate=COVER,
        name="project",
    )(place, part, other, landed, hidden)
    local_mixed, packed = pl.pallas_call(
        mixed_kernel,
        out_shape=(
            jax.ShapeDtypeStruct((slots, columns), bf16),
            jax.ShapeDtypeStruct((devices // count, slots, count * columns), bf16),
        ),
        in_specs=[IN_SMEM, IN_VMEM],
        out_specs=(IN_VMEM, IN_VMEM),
        compiler_params=params(8),
        cost_estimate=COVER,
        name="mixed",
    )(place, exchanged(parts, along))
    gathered = exchanged(packed, (across, pair))

    own, other = pl.pallas_call(
        functools.partial(experts_kernel, share),
        out_shape=(
            jax.ShapeDtypeStruct((blocks, slots // 2, LANES), jnp.float32),
            jax.ShapeDtypeStruct((blocks, slots // 2, LANES), bf16),
        ),
        in_specs=[IN_SMEM] * 2 + [IN_VMEM] * 4 + [IN_HBM, IN_VMEM],
        out_specs=(IN_VMEM, IN_VMEM),
        scratch_shapes=[
            pltpu.VMEM((2, gate_up.shape[2], width), bf16),
            pltpu.SemaphoreType.DMA((CHUNKS,)),
        ],
        compiler_params=params(50),
        name="experts",
    )(
        expert,
        core,
        gathered,
        norm_gain,
        router_weight.T,
        expert_ids.T,
        jnp.swapaxes(gate_up, 1, 2),
        down_proj,
    )
    other = lax.ppermute(other, pair, [(0, 1), (1, 0)])
    terms = merging(add_kernel, own.shape, own, other)
    moe = exchanged(terms.reshape(devices // 2, slots // share, LANES), (along, across))
    return pl.pallas_call(
        final_kernel,
        out_shape=jax.ShapeDtypeStruct((slots, columns), bf16),
        in_specs=[IN_VMEM] * 2,
        out_specs=IN_VMEM,
        compiler_params=params(4),
        name="final",
    )(moe, local_mixed)


def solution(mesh):
    split = Mesh(
        mesh.devices.reshape(mesh.shape["rep"], 8, 8, 2), ("rep", "blk_0", "blk_1", "blk_2")
    )
    return jax.shard_map(
        on_device,
        mesh=split,
        in_specs=(
            P("rep", BLK),
            P("rep", None),
            P(None, "rep", BLK, None),
            P("rep"),
            P(None, "rep", BLK, None),
            P("rep"),
            P("rep"),
            P(None, BLK),
            P(),
            P(),
            P("rep", None),
            P(None, None, BLK),
            P(BLK, None),
        ),
        out_specs=P("rep", BLK),
        check_vma=False,
    )
```

```python
import functools
import math

import jax
import jax.numpy as jnp
from jax import lax
from jax.experimental import pallas as pl
from jax.experimental.pallas import tpu as pltpu
from jax.sharding import Mesh
from jax.sharding import PartitionSpec as P

QUERY_HEADS = 32
KEY_VALUE_HEADS = 8
HEAD_SIZE = 128
EXPERTS = 4
FF = 7168
BLK = ("blk_0", "blk_1", "blk_2")
GROUP = QUERY_HEADS // KEY_VALUE_HEADS
LANES = 128
SPAN = LANES // GROUP
IN_VMEM = pl.BlockSpec(memory_space=pltpu.VMEM)
IN_SMEM = pl.BlockSpec(memory_space=pltpu.SMEM)
IN_HBM = pl.BlockSpec(memory_space=pltpu.HBM)
BATCH = 4
CHUNKS = 8
MIB = 1 << 20
COVER = pl.CostEstimate(flops=8*10**8, bytes_accessed=8 << 20, transcendentals=0)


def exchanged(pieces, axis=BLK):
    return lax.all_to_all(pieces, axis, 0, 0, tiled=True)


def merging(kernel, shape, *pieces):
    return pl.pallas_call(
        kernel,
        out_shape=jax.ShapeDtypeStruct(shape, jnp.bfloat16),
        in_specs=[IN_VMEM] * len(pieces),
        out_specs=IN_VMEM,
        compiler_params=params(8),
        cost_estimate=COVER,
        name=kernel.__name__,
    )(*pieces)


def in_hbm(array):
    return pltpu.with_memory_space_constraint(array, pltpu.HBM)


def params(mib):
    return pltpu.CompilerParams(vmem_limit_bytes=mib * MIB)


def attention_kernel(
    positions,
    first,
    lengths_in,
    insert_slot_in,
    prefix_len_in,
    queries_in,
    weight_in,
    cache,
    inserted,
    out,
    lengths,
    insert_slot,
    prefix_len,
    queries,
    weight,
    spread,
    rows,
    score_of,
    values,
    stats,
    sems,
):
    slots, prefixes, count = lengths.shape[0], insert_slot.shape[0], rows.shape[2]
    wide = QUERY_HEADS
    copies = [
        pltpu.make_async_copy(lengths_in, lengths, sems.at[0]),
        pltpu.make_async_copy(insert_slot_in, insert_slot, sems.at[1]),
        pltpu.make_async_copy(prefix_len_in, prefix_len, sems.at[2]),
        pltpu.make_async_copy(queries_in, queries, sems.at[3]),
        pltpu.make_async_copy(weight_in, weight, sems.at[4]),
    ]
    key_copies, value_copies = [], []
    for k, group in enumerate((key_copies, value_copies)):
        for start in range(0, slots, BATCH):
            here = pl.ds(start, BATCH)
            group.append((cache.at[k, here], rows.at[k, here]))
        for start in range(0, prefixes, BATCH):
            group.append(
                (inserted.at[k, pl.ds(start, BATCH)], rows.at[k, pl.ds(slots + start, BATCH)])
            )
    for at, group in ((5, key_copies), (5 + len(key_copies), value_copies)):
        for i, (source_ref, target_ref) in enumerate(group):
            group[i] = pltpu.make_async_copy(source_ref, target_ref, sems.at[at + i])
    copies = copies[:4] + key_copies + value_copies + copies[4:]
    for copy in copies:
        copy.start()
    for copy in copies[:4]:
        copy.wait()
    for g in range(KEY_VALUE_HEADS):
        for h in range(GROUP):
            at = (g * GROUP + h) * HEAD_SIZE
            one = queries[:, at : at + HEAD_SIZE].astype(jnp.float32)
            spread[pl.ds(g * GROUP + h, slots, stride=wide), :] = one
    here = first[0]
    half = positions // 2
    there = jnp.where(here < half, here + half, here - half)
    valid, source = [], []
    for s in range(slots):
        length, at, start = lengths[s], jnp.int32(s), here
        for j in range(prefixes):
            mine = insert_slot[j] == s
            length = jnp.where(mine, prefix_len[j], length)
            at = jnp.where(mine, slots + j, at)
            start = jnp.where(mine, there, start)
        valid.append(length - start)
        source.append(at)
    for copy in key_copies:
        copy.wait()
    shape = (wide, KEY_VALUE_HEADS * HEAD_SIZE)
    own = (
        lax.broadcasted_iota(jnp.int32, shape, 0) // GROUP
        == lax.broadcasted_iota(jnp.int32, shape, 1) // HEAD_SIZE
    )
    row = lax.broadcasted_iota(jnp.int32, (wide, HEAD_SIZE), 0)
    lane = lax.broadcasted_iota(jnp.int32, (wide, HEAD_SIZE), 1)
    counted = lane // SPAN == row % GROUP
    early = lax.broadcasted_iota(jnp.int32, (2 * GROUP, HEAD_SIZE), 0) < GROUP
    place = lax.broadcasted_iota(jnp.int32, (wide, count), 1)
    for s in range(slots):
        one = spread[s * wide : (s + 1) * wide, :]
        tiled = jnp.concatenate([one] * KEY_VALUE_HEADS, axis=1)
        blocks = jnp.where(own, tiled, 0.0).astype(jnp.bfloat16)
        score_of[s] = lax.dot_general(
            blocks,
            rows[0, source[s]],
            (((1,), (1,)), ((), ())),
            preferred_element_type=jnp.float32,
        ) * (1.0 / math.sqrt(HEAD_SIZE))
    for copy in value_copies:
        copy.wait()
    for batch in range(0, slots, BATCH):
        several = range(batch, batch + BATCH)
        inside = [place < valid[s] for s in several]
        scores = [jnp.where(i, score_of[s], -1e30) for i, s in zip(inside, several)]
        peaks = [jnp.max(x, axis=1, keepdims=True) for x in scores]
        peaks = [x.astype(jnp.bfloat16).astype(jnp.float32) for x in peaks]
        weights = [
            jnp.where(i, jnp.exp(x - p), 0.0) for i, x, p in zip(inside, scores, peaks)
        ]
        totals = [jnp.sum(x, axis=1, keepdims=True) for x in weights]
        every = [
            jnp.dot(
                x.astype(jnp.bfloat16), rows[1, source[s]], preferred_element_type=jnp.float32
            )
            for x, s in zip(weights, several)
        ]
        for s, full, peak, total in zip(several, every, peaks, totals):
            value = jnp.concatenate(
                [
                    jnp.where(
                        early,
                        full[g * GROUP : (g + 2) * GROUP, g * HEAD_SIZE : (g + 1) * HEAD_SIZE],
                        full[
                            g * GROUP : (g + 2) * GROUP, (g + 1) * HEAD_SIZE : (g + 2) * HEAD_SIZE
                        ],
                    )
                    for g in range(0, KEY_VALUE_HEADS, 2)
                ],
                axis=0,
            )
            values[pl.ds(s, wide, stride=slots), :] = value / jnp.where(total > 0.0, total, 1.0)
            stats[pl.ds(s, wide, stride=slots), :] = jnp.where(
                counted, packed_stats(lane, peak, total), 0.0
            )
    deep = GROUP * slots
    copies[-1].wait()
    for g in range(KEY_VALUE_HEADS):
        out[g, :deep, :] = values[g * deep : (g + 1) * deep, :].astype(jnp.bfloat16)
        one = [stats[g * deep + h * slots : g * deep + (h + 1) * slots, :] for h in range(GROUP)]
        out[g, deep : deep + slots, :] = sum(one).astype(jnp.bfloat16)
        for h in range(GROUP):
            at = deep + slots + h * weight.shape[0]
            head = (g * GROUP + h) * HEAD_SIZE
            out[g, at : at + weight.shape[0], :] = weight[:, head : head + HEAD_SIZE]


def packed_stats(lane, peak, total):
    rounded = total.astype(jnp.bfloat16).astype(jnp.float32)
    at = lane % SPAN
    return jnp.where(
        at < SPAN // 2, peak, jnp.where(at < SPAN * 3 // 4, rounded, total - rounded)
    )


def merge(pieces):
    slots = pieces[0].shape[0] // (GROUP + 1)
    found = [x[GROUP * slots :].astype(jnp.float32) for x in pieces]
    highest = functools.reduce(jnp.maximum, found)
    scales = [
        jnp.exp(x - highest)
        * (
            pltpu.roll(x, LANES - SPAN // 2, axis=1)
            + pltpu.roll(x, LANES - SPAN * 3 // 4, axis=1)
        )
        for x in found
    ]
    total = sum(scales)
    safe = jnp.where(total > 0.0, total, 1.0)
    values = []
    for h in range(GROUP):
        column = slice(h * SPAN, h * SPAN + 1)
        parts = [
            x[h * slots : (h + 1) * slots].astype(jnp.float32) * y[:, column]
            for x, y in zip(pieces, scales)
        ]
        values.append(sum(parts) / safe[:, column])
    return values, highest, total


def whole_part(pieces):
    values, highest, total = merge(pieces)
    lane = lax.broadcasted_iota(jnp.int32, highest.shape, 1)
    total = pltpu.roll(total, SPAN // 2, axis=1)
    rounded = total.astype(jnp.bfloat16).astype(jnp.float32)
    rest = pltpu.roll(total - rounded, SPAN // 4, axis=1)
    at = lane % SPAN
    stats = jnp.where(at < SPAN // 2, highest, jnp.where(at < SPAN * 3 // 4, rounded, rest))
    return jnp.concatenate(values + [stats], axis=0).astype(jnp.bfloat16)


def spread_kernel(pieces, out):
    part = whole_part([pieces[i, : out.shape[1], :] for i in range(pieces.shape[0])])
    for i in range(out.shape[0]):
        out[i] = part


def part_kernel(pieces, out):
    out[...] = whole_part([pieces[i] for i in range(pieces.shape[0])])


def project_kernel(place, mine, other, landed, hidden, out):
    slots, columns = hidden.shape
    count, deep = landed.shape[0], mine.shape[0]
    values, _, _ = merge([mine[...], other[...]])
    attn = jnp.concatenate(values, axis=1).astype(jnp.bfloat16)
    heads = []
    for h in range(GROUP):
        at = deep + h * columns
        parts = [landed[i, at : at + columns, :] for i in range(count)]
        heads.append(jnp.concatenate(parts, axis=0))
    weight = jnp.concatenate(heads, axis=1)
    total = lax.dot_general(
        attn, weight, (((1,), (1,)), ((), ())), preferred_element_type=jnp.float32
    )
    tiled = jnp.concatenate([hidden[...].astype(jnp.float32)] * count, axis=1)
    owner = lax.broadcasted_iota(jnp.int32, tiled.shape, 1) // columns
    part = (total + jnp.where(owner == place[0], tiled, 0.0)).astype(jnp.bfloat16)
    for i in range(count):
        out[i] = part


def mixed_kernel(place, pieces, own, out):
    columns = own.shape[1]
    total = pieces[0].astype(jnp.float32)
    for i in range(1, pieces.shape[0]):
        total = total + pieces[i].astype(jnp.float32)
    mixed = total.astype(jnp.bfloat16)
    for i in range(out.shape[0]):
        out[i] = mixed
    mine = [total[:, i * columns : (i + 1) * columns] for i in range(pieces.shape[0])]
    own[...] = sum(jnp.where(place[0] == i, x, 0.0) for i, x in enumerate(mine)).astype(
        jnp.bfloat16
    )


def in_feature_order(gathered, share):
    count, slots, width = gathered.shape
    columns, rows, halves = LANES // share, count // share, width // LANES
    block = lax.broadcasted_iota(jnp.int32, (slots, LANES), 1) // columns
    tiles = {}
    for m in range(rows):
        for half in range(halves):
            found = [
                gathered[share * m + j, :, half * LANES : (half + 1) * LANES].astype(jnp.float32)
                for j in range(share)
            ]
            for b in range(share):
                tile = found[b]
                for j in range(share):
                    if j != b:
                        turned = pltpu.roll(found[j], (j - b) % share * columns, axis=1)
                        tile = jnp.where(block == j, turned, tile)
                tiles[(half * share + b) * rows + m] = tile
    return jnp.concatenate([tiles[k] for k in range(len(tiles))], axis=1)


def swapped(tiles, share):
    slots = tiles.shape[1]
    deep, width = slots // share, LANES // share
    row = lax.broadcasted_iota(jnp.int32, tiles.shape, 1) // deep
    lane = lax.broadcasted_iota(jnp.int32, tiles.shape, 2) // width
    turn = (lane - row + share) % share
    result = tiles
    for j in range(1, share):
        moved = pltpu.roll(pltpu.roll(tiles, j * width, axis=2), slots - j * deep, axis=1)
        result = jnp.where(turn == j, moved, result)
    return result


def experts_kernel(
    share, expert, core, gathered, gain, router, chosen, gate_up_in, down, own, other, gate_up, sems
):
    blocks, slots = own.shape[0], 2 * own.shape[1]
    step = blocks * LANES // CHUNKS
    copies = []
    for i in range(CHUNKS):
        lanes = pl.ds(i * step, step)
        copies.append(
            pltpu.make_async_copy(
                gate_up_in.at[:, :, lanes], gate_up.at[:, :, lanes], sems.at[i]
            )
        )
        copies[i].start()
    mixed = in_feature_order(gathered, share)
    scale = lax.rsqrt(jnp.sum(mixed * mixed, axis=1, keepdims=True) / (blocks * LANES) + 1e-05)
    normed = (mixed * scale * gain[...].astype(jnp.float32).reshape(1, blocks * LANES)).astype(jnp.bfloat16)
    plain = normed.astype(jnp.float32)
    weights = router[...].astype(jnp.float32)
    logits = [
        jnp.sum(plain * weights[e : e + 1], axis=1, keepdims=True) for e in range(EXPERTS)
    ]
    upright = lax.broadcasted_iota(jnp.int32, (slots, slots), 0) == lax.broadcasted_iota(
        jnp.int32, (slots, slots), 1
    )
    ids = [
        jnp.sum(
            jnp.where(upright, chosen[i : i + 1, :].astype(jnp.float32), 0.0),
            axis=1,
            keepdims=True,
        )
        for i in range(2)
    ]
    picked = [sum(jnp.where(k == e, logits[e], 0.0) for e in range(EXPERTS)) for k in ids]
    gates = [jax.nn.sigmoid(picked[i] - picked[1 - i]) for i in range(2)]
    mine = expert[0].astype(jnp.float32)
    part = sum(jnp.where(ids[i] == mine, gates[i], 0.0) for i in range(2))
    gate, up = 0.0, 0.0
    for i in range(CHUNKS):
        copies[i].wait()
        lanes = slice(i * step, (i + 1) * step)
        contract = functools.partial(
            lax.dot_general,
            normed[:, lanes],
            dimension_numbers=(((1,), (1,)), ((), ())),
            preferred_element_type=jnp.float32,
        )
        gate = gate + contract(gate_up[0, :, lanes])
        up = up + contract(gate_up[1, :, lanes])
    act = (gate * jax.nn.sigmoid(gate) * up).astype(jnp.bfloat16)
    term = part * jnp.dot(act, down[...], preferred_element_type=jnp.float32)
    tiles = [term[None, :, k * LANES : (k + 1) * LANES] for k in range(blocks)]
    even, odd = by_core(swapped(jnp.concatenate(tiles, axis=0), share), slots // share)
    own[...] = jnp.where(core[0] == 0, even, odd)
    other[...] = jnp.where(core[0] == 0, odd, even).astype(jnp.bfloat16)


def by_core(tiles, deep):
    top, bottom = tiles[:, : 2 * deep], tiles[:, 2 * deep :]
    first = lax.broadcasted_iota(jnp.int32, top.shape, 1) < deep
    even = jnp.where(first, top, pltpu.roll(bottom, deep, axis=1))
    odd = jnp.where(first, pltpu.roll(top, deep, axis=1), bottom)
    return even, odd


def add_kernel(own, other, out):
    out[...] = (own[...] + other[...].astype(jnp.float32)).astype(jnp.bfloat16)


def final_kernel(pieces, mixed, out):
    slots, columns = mixed.shape
    share = LANES // columns
    total = jnp.sum(pieces[...].astype(jnp.float32), axis=0)
    moe = jnp.concatenate(
        [total[:, b * columns : (b + 1) * columns] for b in range(share)], axis=0
    )
    out[...] = (mixed[...].astype(jnp.float32) + moe).astype(jnp.bfloat16)


def on_device(
    hidden,
    queries,
    cache_kv,
    cache_len,
    inserted_key_value,
    insert_slot,
    prefix_len,
    out_weight,
    norm_gain,
    router_weight,
    expert_ids,
    gate_up,
    down_proj,
):
    devices = lax.axis_size(BLK)
    dev_index = lax.axis_index(BLK)
    slots, columns = hidden.shape
    ctx_rows, kv_width = cache_kv.shape[2:]
    prefixes = insert_slot.shape[0]
    share = LANES // columns
    deep = slots * (GROUP + 1)
    width = devices * columns
    blocks = width // LANES
    bf16 = jnp.bfloat16

    first = (dev_index * ctx_rows).astype(jnp.int32).reshape(1)
    place = lax.axis_index(BLK[0]).astype(jnp.int32).reshape(1)
    expert = (dev_index * gate_up.shape[2] // FF).astype(jnp.int32).reshape(1)
    core = lax.axis_index(BLK[2]).astype(jnp.int32).reshape(1)
    first, place, expert, core = lax.optimization_barrier((first, place, expert, core))
    partials = pl.pallas_call(
        functools.partial(attention_kernel, devices * ctx_rows),
        out_shape=jax.ShapeDtypeStruct((KEY_VALUE_HEADS, deep + GROUP * columns, HEAD_SIZE), bf16),
        in_specs=[IN_SMEM] + [IN_HBM] * 7,
        out_specs=IN_VMEM,
        scratch_shapes=[
            pltpu.SMEM((slots,), jnp.int32),
            pltpu.SMEM((prefixes,), jnp.int32),
            pltpu.SMEM((prefixes,), jnp.int32),
            pltpu.VMEM(queries.shape, bf16),
            pltpu.VMEM(out_weight.shape[::-1], bf16),
            pltpu.VMEM((slots * QUERY_HEADS, HEAD_SIZE), jnp.float32),
            pltpu.VMEM((2, slots + prefixes, ctx_rows, kv_width), bf16),
            pltpu.VMEM((slots, QUERY_HEADS, ctx_rows), jnp.float32),
            pltpu.VMEM((slots * QUERY_HEADS, HEAD_SIZE), jnp.float32),
            pltpu.VMEM((slots * QUERY_HEADS, HEAD_SIZE), jnp.float32),
            pltpu.SemaphoreType.DMA((5 + 2 * (slots + prefixes) // BATCH,)),
        ],
        compiler_params=params(24),
        name="attention",
    )(
        first,
        in_hbm(cache_len),
        in_hbm(insert_slot),
        in_hbm(prefix_len),
        in_hbm(queries),
        in_hbm(out_weight.T),
        in_hbm(cache_kv),
        in_hbm(inserted_key_value),
    )
    along, across, pair = BLK
    copies = lax.axis_size(across)
    landed = exchanged(partials, along)
    part = merging(spread_kernel, (copies, deep, HEAD_SIZE), landed)
    part = merging(part_kernel, (deep, HEAD_SIZE), exchanged(part, across))
    other = lax.ppermute(part, pair, [(0, 1), (1, 0)])
    count = lax.axis_size(along)
    parts = pl.pallas_call(
        project_kernel,
        out_shape=jax.ShapeDtypeStruct((count, slots, count * columns), bf16),
        in_specs=[IN_SMEM] + [IN_VMEM] * 4,
        out_specs=IN_VMEM,
        compiler_params=params(8),
        cost_estimate=COVER,
        name="project",
    )(place, part, other, landed, hidden)
    local_mixed, packed = pl.pallas_call(
        mixed_kernel,
        out_shape=(
            jax.ShapeDtypeStruct((slots, columns), bf16),
            jax.ShapeDtypeStruct((devices // count, slots, count * columns), bf16),
        ),
        in_specs=[IN_SMEM, IN_VMEM],
        out_specs=(IN_VMEM, IN_VMEM),
        compiler_params=params(8),
        cost_estimate=COVER,
        name="mixed",
    )(place, exchanged(parts, along))
    gathered = exchanged(packed, (across, pair))

    own, other = pl.pallas_call(
        functools.partial(experts_kernel, share),
        out_shape=(
            jax.ShapeDtypeStruct((blocks, slots // 2, LANES), jnp.float32),
            jax.ShapeDtypeStruct((blocks, slots // 2, LANES), bf16),
        ),
        in_specs=[IN_SMEM] * 2 + [IN_VMEM] * 4 + [IN_HBM, IN_VMEM],
        out_specs=(IN_VMEM, IN_VMEM),
        scratch_shapes=[
            pltpu.VMEM((2, gate_up.shape[2], width), bf16),
            pltpu.SemaphoreType.DMA((CHUNKS,)),
        ],
        compiler_params=params(24),
        name="experts",
    )(
        expert,
        core,
        gathered,
        norm_gain,
        router_weight.T,
        expert_ids.T,
        in_hbm(jnp.swapaxes(gate_up, 1, 2)),
        down_proj,
    )
    other = lax.ppermute(other, pair, [(0, 1), (1, 0)])
    terms = merging(add_kernel, own.shape, own, other)
    moe = exchanged(terms.reshape(devices // 2, slots // share, LANES), (along, across))
    return pl.pallas_call(
        final_kernel,
        out_shape=jax.ShapeDtypeStruct((slots, columns), bf16),
        in_specs=[IN_VMEM] * 2,
        out_specs=IN_VMEM,
        compiler_params=params(4),
        name="final",
    )(moe, local_mixed)


def solution(mesh):
    split = Mesh(
        mesh.devices.reshape(mesh.shape["rep"], 8, 8, 2), ("rep", "blk_0", "blk_1", "blk_2")
    )
    return jax.shard_map(
        on_device,
        mesh=split,
        in_specs=(
            P("rep", BLK),
            P("rep", None),
            P(None, "rep", BLK, None),
            P("rep"),
            P(None, "rep", BLK, None),
            P("rep"),
            P("rep"),
            P(None, BLK),
            P(),
            P(),
            P("rep", None),
            P(None, None, BLK),
            P(BLK, None),
        ),
        out_specs=P("rep", BLK),
        check_vma=False,
    )
```

```python
import functools
import math

import jax
import jax.numpy as jnp
from jax import lax
from jax.experimental import pallas as pl
from jax.experimental.pallas import tpu as pltpu
from jax.sharding import Mesh
from jax.sharding import PartitionSpec as P

QUERY_HEADS = 32
KEY_VALUE_HEADS = 8
HEAD_SIZE = 128
EXPERTS = 4
FF = 7168
BLK = ("blk_0", "blk_1", "blk_2")
GROUP = QUERY_HEADS // KEY_VALUE_HEADS
LANES = 128
SPAN = LANES // GROUP
IN_VMEM = pl.BlockSpec(memory_space=pltpu.VMEM)
IN_SMEM = pl.BlockSpec(memory_space=pltpu.SMEM)
IN_HBM = pl.BlockSpec(memory_space=pltpu.HBM)
BATCH = 4
MIB = 1 << 20
COVER = pl.CostEstimate(flops=8*10**8, bytes_accessed=8 << 20, transcendentals=0)


def exchanged(pieces, axis=BLK):
    return lax.all_to_all(pieces, axis, 0, 0, tiled=True)


def merging(kernel, shape, *pieces):
    return pl.pallas_call(
        kernel,
        out_shape=jax.ShapeDtypeStruct(shape, jnp.bfloat16),
        in_specs=[IN_VMEM] * len(pieces),
        out_specs=IN_VMEM,
        compiler_params=params(8),
        cost_estimate=COVER,
        name=kernel.__name__,
    )(*pieces)


def in_hbm(array):
    return pltpu.with_memory_space_constraint(array, pltpu.HBM)


def params(mib):
    return pltpu.CompilerParams(vmem_limit_bytes=mib * MIB)


def attention_kernel(
    positions,
    first,
    lengths_in,
    insert_slot_in,
    prefix_len_in,
    queries_in,
    weight_in,
    cache,
    inserted,
    out,
    lengths,
    insert_slot,
    prefix_len,
    queries,
    weight,
    spread,
    rows,
    score_of,
    values,
    stats,
    sems,
):
    slots, prefixes, count = lengths.shape[0], insert_slot.shape[0], rows.shape[2]
    wide = QUERY_HEADS
    copies = [
        pltpu.make_async_copy(lengths_in, lengths, sems.at[0]),
        pltpu.make_async_copy(insert_slot_in, insert_slot, sems.at[1]),
        pltpu.make_async_copy(prefix_len_in, prefix_len, sems.at[2]),
        pltpu.make_async_copy(queries_in, queries, sems.at[3]),
        pltpu.make_async_copy(weight_in, weight, sems.at[4]),
    ]
    key_copies, value_copies = [], []
    for k, group in enumerate((key_copies, value_copies)):
        for start in range(0, slots, BATCH):
            here = pl.ds(start, BATCH)
            group.append((cache.at[k, here], rows.at[k, here]))
        for start in range(0, prefixes, BATCH):
            group.append(
                (inserted.at[k, pl.ds(start, BATCH)], rows.at[k, pl.ds(slots + start, BATCH)])
            )
    for at, group in ((5, key_copies), (5 + len(key_copies), value_copies)):
        for i, (source_ref, target_ref) in enumerate(group):
            group[i] = pltpu.make_async_copy(source_ref, target_ref, sems.at[at + i])
    copies = copies[:4] + key_copies + value_copies + copies[4:]
    for copy in copies:
        copy.start()
    for copy in copies[:4]:
        copy.wait()
    for g in range(KEY_VALUE_HEADS):
        for h in range(GROUP):
            at = (g * GROUP + h) * HEAD_SIZE
            one = queries[:, at : at + HEAD_SIZE].astype(jnp.float32)
            spread[pl.ds(g * GROUP + h, slots, stride=wide), :] = one
    here = first[0]
    half = positions // 2
    there = jnp.where(here < half, here + half, here - half)
    valid, source = [], []
    for s in range(slots):
        length, at, start = lengths[s], jnp.int32(s), here
        for j in range(prefixes):
            mine = insert_slot[j] == s
            length = jnp.where(mine, prefix_len[j], length)
            at = jnp.where(mine, slots + j, at)
            start = jnp.where(mine, there, start)
        valid.append(length - start)
        source.append(at)
    for copy in key_copies:
        copy.wait()
    shape = (wide, KEY_VALUE_HEADS * HEAD_SIZE)
    own = (
        lax.broadcasted_iota(jnp.int32, shape, 0) // GROUP
        == lax.broadcasted_iota(jnp.int32, shape, 1) // HEAD_SIZE
    )
    row = lax.broadcasted_iota(jnp.int32, (wide, HEAD_SIZE), 0)
    lane = lax.broadcasted_iota(jnp.int32, (wide, HEAD_SIZE), 1)
    counted = lane // SPAN == row % GROUP
    early = lax.broadcasted_iota(jnp.int32, (2 * GROUP, HEAD_SIZE), 0) < GROUP
    place = lax.broadcasted_iota(jnp.int32, (wide, count), 1)
    for s in range(slots):
        one = spread[s * wide : (s + 1) * wide, :]
        tiled = jnp.concatenate([one] * KEY_VALUE_HEADS, axis=1)
        blocks = jnp.where(own, tiled, 0.0).astype(jnp.bfloat16)
        score_of[s] = lax.dot_general(
            blocks,
            rows[0, source[s]],
            (((1,), (1,)), ((), ())),
            preferred_element_type=jnp.float32,
        ) * (1.0 / math.sqrt(HEAD_SIZE))
    for copy in value_copies:
        copy.wait()
    for batch in range(0, slots, BATCH):
        several = range(batch, batch + BATCH)
        inside = [place < valid[s] for s in several]
        scores = [jnp.where(i, score_of[s], -1e30) for i, s in zip(inside, several)]
        peaks = [jnp.max(x, axis=1, keepdims=True) for x in scores]
        peaks = [x.astype(jnp.bfloat16).astype(jnp.float32) for x in peaks]
        weights = [
            jnp.where(i, jnp.exp(x - p), 0.0) for i, x, p in zip(inside, scores, peaks)
        ]
        totals = [jnp.sum(x, axis=1, keepdims=True) for x in weights]
        every = [
            jnp.dot(
                x.astype(jnp.bfloat16), rows[1, source[s]], preferred_element_type=jnp.float32
            )
            for x, s in zip(weights, several)
        ]
        for s, full, peak, total in zip(several, every, peaks, totals):
            value = jnp.concatenate(
                [
                    jnp.where(
                        early,
                        full[g * GROUP : (g + 2) * GROUP, g * HEAD_SIZE : (g + 1) * HEAD_SIZE],
                        full[
                            g * GROUP : (g + 2) * GROUP, (g + 1) * HEAD_SIZE : (g + 2) * HEAD_SIZE
                        ],
                    )
                    for g in range(0, KEY_VALUE_HEADS, 2)
                ],
                axis=0,
            )
            values[pl.ds(s, wide, stride=slots), :] = value / jnp.where(total > 0.0, total, 1.0)
            stats[pl.ds(s, wide, stride=slots), :] = jnp.where(
                counted, packed_stats(lane, peak, total), 0.0
            )
    deep = GROUP * slots
    copies[-1].wait()
    for g in range(KEY_VALUE_HEADS):
        out[g, :deep, :] = values[g * deep : (g + 1) * deep, :].astype(jnp.bfloat16)
        one = [stats[g * deep + h * slots : g * deep + (h + 1) * slots, :] for h in range(GROUP)]
        out[g, deep : deep + slots, :] = sum(one).astype(jnp.bfloat16)
        for h in range(GROUP):
            at = deep + slots + h * weight.shape[0]
            head = (g * GROUP + h) * HEAD_SIZE
            out[g, at : at + weight.shape[0], :] = weight[:, head : head + HEAD_SIZE]


def packed_stats(lane, peak, total):
    rounded = total.astype(jnp.bfloat16).astype(jnp.float32)
    at = lane % SPAN
    return jnp.where(
        at < SPAN // 2, peak, jnp.where(at < SPAN * 3 // 4, rounded, total - rounded)
    )


def merge(pieces):
    slots = pieces[0].shape[0] // (GROUP + 1)
    found = [x[GROUP * slots :].astype(jnp.float32) for x in pieces]
    highest = functools.reduce(jnp.maximum, found)
    scales = [
        jnp.exp(x - highest)
        * (
            pltpu.roll(x, LANES - SPAN // 2, axis=1)
            + pltpu.roll(x, LANES - SPAN * 3 // 4, axis=1)
        )
        for x in found
    ]
    total = sum(scales)
    safe = jnp.where(total > 0.0, total, 1.0)
    values = []
    for h in range(GROUP):
        column = slice(h * SPAN, h * SPAN + 1)
        parts = [
            x[h * slots : (h + 1) * slots].astype(jnp.float32) * y[:, column]
            for x, y in zip(pieces, scales)
        ]
        values.append(sum(parts) / safe[:, column])
    return values, highest, total


def whole_part(pieces):
    values, highest, total = merge(pieces)
    lane = lax.broadcasted_iota(jnp.int32, highest.shape, 1)
    total = pltpu.roll(total, SPAN // 2, axis=1)
    rounded = total.astype(jnp.bfloat16).astype(jnp.float32)
    rest = pltpu.roll(total - rounded, SPAN // 4, axis=1)
    at = lane % SPAN
    stats = jnp.where(at < SPAN // 2, highest, jnp.where(at < SPAN * 3 // 4, rounded, rest))
    return jnp.concatenate(values + [stats], axis=0).astype(jnp.bfloat16)


def spread_kernel(pieces, out):
    part = whole_part([pieces[i, : out.shape[1], :] for i in range(pieces.shape[0])])
    for i in range(out.shape[0]):
        out[i] = part


def part_kernel(pieces, out):
    out[...] = whole_part([pieces[i] for i in range(pieces.shape[0])])


def project_kernel(place, mine, other, landed, hidden, out):
    slots, columns = hidden.shape
    count, deep = landed.shape[0], mine.shape[0]
    values, _, _ = merge([mine[...], other[...]])
    attn = jnp.concatenate(values, axis=1).astype(jnp.bfloat16)
    heads = []
    for h in range(GROUP):
        at = deep + h * columns
        parts = [landed[i, at : at + columns, :] for i in range(count)]
        heads.append(jnp.concatenate(parts, axis=0))
    weight = jnp.concatenate(heads, axis=1)
    total = lax.dot_general(
        attn, weight, (((1,), (1,)), ((), ())), preferred_element_type=jnp.float32
    )
    tiled = jnp.concatenate([hidden[...].astype(jnp.float32)] * count, axis=1)
    owner = lax.broadcasted_iota(jnp.int32, tiled.shape, 1) // columns
    part = (total + jnp.where(owner == place[0], tiled, 0.0)).astype(jnp.bfloat16)
    for i in range(count):
        out[i] = part


def mixed_kernel(place, pieces, own, out):
    columns = own.shape[1]
    total = pieces[0].astype(jnp.float32)
    for i in range(1, pieces.shape[0]):
        total = total + pieces[i].astype(jnp.float32)
    mixed = total.astype(jnp.bfloat16)
    for i in range(out.shape[0]):
        out[i] = mixed
    mine = [total[:, i * columns : (i + 1) * columns] for i in range(pieces.shape[0])]
    own[...] = sum(jnp.where(place[0] == i, x, 0.0) for i, x in enumerate(mine)).astype(
        jnp.bfloat16
    )


def in_feature_order(gathered, share):
    count, slots, width = gathered.shape
    columns, rows, halves = LANES // share, count // share, width // LANES
    block = lax.broadcasted_iota(jnp.int32, (slots, LANES), 1) // columns
    tiles = {}
    for m in range(rows):
        for half in range(halves):
            found = [
                gathered[share * m + j, :, half * LANES : (half + 1) * LANES].astype(jnp.float32)
                for j in range(share)
            ]
            for b in range(share):
                tile = found[b]
                for j in range(share):
                    if j != b:
                        turned = pltpu.roll(found[j], (j - b) % share * columns, axis=1)
                        tile = jnp.where(block == j, turned, tile)
                tiles[(half * share + b) * rows + m] = tile
    return jnp.concatenate([tiles[k] for k in range(len(tiles))], axis=1)


def swapped(tiles, share):
    slots = tiles.shape[1]
    deep, width = slots // share, LANES // share
    row = lax.broadcasted_iota(jnp.int32, tiles.shape, 1) // deep
    lane = lax.broadcasted_iota(jnp.int32, tiles.shape, 2) // width
    turn = (lane - row + share) % share
    result = tiles
    for j in range(1, share):
        moved = pltpu.roll(pltpu.roll(tiles, j * width, axis=2), slots - j * deep, axis=1)
        result = jnp.where(turn == j, moved, result)
    return result


def experts_kernel(
    share, expert, core, gathered, gain, router, chosen, gate_up, down, own, other
):
    blocks, slots = own.shape[0], 2 * own.shape[1]
    mixed = in_feature_order(gathered, share)
    scale = lax.rsqrt(jnp.sum(mixed * mixed, axis=1, keepdims=True) / (blocks * LANES) + 1e-05)
    normed = (mixed * scale * gain[...].astype(jnp.float32).reshape(1, blocks * LANES)).astype(jnp.bfloat16)
    plain = normed.astype(jnp.float32)
    weights = router[...].astype(jnp.float32)
    logits = [
        jnp.sum(plain * weights[e : e + 1], axis=1, keepdims=True) for e in range(EXPERTS)
    ]
    upright = lax.broadcasted_iota(jnp.int32, (slots, slots), 0) == lax.broadcasted_iota(
        jnp.int32, (slots, slots), 1
    )
    ids = [
        jnp.sum(
            jnp.where(upright, chosen[i : i + 1, :].astype(jnp.float32), 0.0),
            axis=1,
            keepdims=True,
        )
        for i in range(2)
    ]
    picked = [sum(jnp.where(k == e, logits[e], 0.0) for e in range(EXPERTS)) for k in ids]
    gates = [jax.nn.sigmoid(picked[i] - picked[1 - i]) for i in range(2)]
    mine = expert[0].astype(jnp.float32)
    part = sum(jnp.where(ids[i] == mine, gates[i], 0.0) for i in range(2))
    gate, up = [
        lax.dot_general(
            normed, gate_up[i], (((1,), (1,)), ((), ())), preferred_element_type=jnp.float32
        )
        for i in range(2)
    ]
    act = (gate * jax.nn.sigmoid(gate) * up).astype(jnp.bfloat16)
    term = part * jnp.dot(act, down[...], preferred_element_type=jnp.float32)
    tiles = [term[None, :, k * LANES : (k + 1) * LANES] for k in range(blocks)]
    even, odd = by_core(swapped(jnp.concatenate(tiles, axis=0), share), slots // share)
    own[...] = jnp.where(core[0] == 0, even, odd)
    other[...] = jnp.where(core[0] == 0, odd, even).astype(jnp.bfloat16)


def by_core(tiles, deep):
    top, bottom = tiles[:, : 2 * deep], tiles[:, 2 * deep :]
    first = lax.broadcasted_iota(jnp.int32, top.shape, 1) < deep
    even = jnp.where(first, top, pltpu.roll(bottom, deep, axis=1))
    odd = jnp.where(first, pltpu.roll(top, deep, axis=1), bottom)
    return even, odd


def add_kernel(own, other, out):
    out[...] = (own[...] + other[...].astype(jnp.float32)).astype(jnp.bfloat16)


def final_kernel(pieces, mixed, out):
    slots, columns = mixed.shape
    share = LANES // columns
    total = jnp.sum(pieces[...].astype(jnp.float32), axis=0)
    moe = jnp.concatenate(
        [total[:, b * columns : (b + 1) * columns] for b in range(share)], axis=0
    )
    out[...] = (mixed[...].astype(jnp.float32) + moe).astype(jnp.bfloat16)


def on_device(
    hidden,
    queries,
    cache_kv,
    cache_len,
    inserted_key_value,
    insert_slot,
    prefix_len,
    out_weight,
    norm_gain,
    router_weight,
    expert_ids,
    gate_up,
    down_proj,
):
    devices = lax.axis_size(BLK)
    dev_index = lax.axis_index(BLK)
    slots, columns = hidden.shape
    ctx_rows, kv_width = cache_kv.shape[2:]
    prefixes = insert_slot.shape[0]
    share = LANES // columns
    deep = slots * (GROUP + 1)
    width = devices * columns
    blocks = width // LANES
    bf16 = jnp.bfloat16

    first = (dev_index * ctx_rows).astype(jnp.int32).reshape(1)
    place = lax.axis_index(BLK[0]).astype(jnp.int32).reshape(1)
    expert = (dev_index * gate_up.shape[2] // FF).astype(jnp.int32).reshape(1)
    core = lax.axis_index(BLK[2]).astype(jnp.int32).reshape(1)
    first, place, expert, core = lax.optimization_barrier((first, place, expert, core))
    partials = pl.pallas_call(
        functools.partial(attention_kernel, devices * ctx_rows),
        out_shape=jax.ShapeDtypeStruct((KEY_VALUE_HEADS, deep + GROUP * columns, HEAD_SIZE), bf16),
        in_specs=[IN_SMEM] + [IN_HBM] * 7,
        out_specs=IN_VMEM,
        scratch_shapes=[
            pltpu.SMEM((slots,), jnp.int32),
            pltpu.SMEM((prefixes,), jnp.int32),
            pltpu.SMEM((prefixes,), jnp.int32),
            pltpu.VMEM(queries.shape, bf16),
            pltpu.VMEM(out_weight.shape[::-1], bf16),
            pltpu.VMEM((slots * QUERY_HEADS, HEAD_SIZE), jnp.float32),
            pltpu.VMEM((2, slots + prefixes, ctx_rows, kv_width), bf16),
            pltpu.VMEM((slots, QUERY_HEADS, ctx_rows), jnp.float32),
            pltpu.VMEM((slots * QUERY_HEADS, HEAD_SIZE), jnp.float32),
            pltpu.VMEM((slots * QUERY_HEADS, HEAD_SIZE), jnp.float32),
            pltpu.SemaphoreType.DMA((5 + 2 * (slots + prefixes) // BATCH,)),
        ],
        compiler_params=params(24),
        name="attention",
    )(
        first,
        in_hbm(cache_len),
        in_hbm(insert_slot),
        in_hbm(prefix_len),
        in_hbm(queries),
        in_hbm(out_weight.T),
        in_hbm(cache_kv),
        in_hbm(inserted_key_value),
    )
    along, across, pair = BLK
    copies = lax.axis_size(across)
    landed = exchanged(partials, along)
    part = merging(spread_kernel, (copies, deep, HEAD_SIZE), landed)
    part = merging(part_kernel, (deep, HEAD_SIZE), exchanged(part, across))
    other = lax.ppermute(part, pair, [(0, 1), (1, 0)])
    count = lax.axis_size(along)
    parts = pl.pallas_call(
        project_kernel,
        out_shape=jax.ShapeDtypeStruct((count, slots, count * columns), bf16),
        in_specs=[IN_SMEM] + [IN_VMEM] * 4,
        out_specs=IN_VMEM,
        compiler_params=params(8),
        cost_estimate=COVER,
        name="project",
    )(place, part, other, landed, hidden)
    local_mixed, packed = pl.pallas_call(
        mixed_kernel,
        out_shape=(
            jax.ShapeDtypeStruct((slots, columns), bf16),
            jax.ShapeDtypeStruct((devices // count, slots, count * columns), bf16),
        ),
        in_specs=[IN_SMEM, IN_VMEM],
        out_specs=(IN_VMEM, IN_VMEM),
        compiler_params=params(8),
        cost_estimate=COVER,
        name="mixed",
    )(place, exchanged(parts, along))
    gathered = exchanged(packed, (across, pair))

    own, other = pl.pallas_call(
        functools.partial(experts_kernel, share),
        out_shape=(
            jax.ShapeDtypeStruct((blocks, slots // 2, LANES), jnp.float32),
            jax.ShapeDtypeStruct((blocks, slots // 2, LANES), bf16),
        ),
        in_specs=[IN_SMEM] * 2 + [IN_VMEM] * 6,
        out_specs=(IN_VMEM, IN_VMEM),
        compiler_params=params(24),
        name="experts",
    )(
        expert,
        core,
        gathered,
        norm_gain,
        router_weight.T,
        expert_ids.T,
        jnp.swapaxes(gate_up, 1, 2),
        down_proj,
    )
    other = lax.ppermute(other, pair, [(0, 1), (1, 0)])
    terms = merging(add_kernel, own.shape, own, other)
    moe = exchanged(terms.reshape(devices // 2, slots // share, LANES), (along, across))
    return pl.pallas_call(
        final_kernel,
        out_shape=jax.ShapeDtypeStruct((slots, columns), bf16),
        in_specs=[IN_VMEM] * 2,
        out_specs=IN_VMEM,
        compiler_params=params(4),
        name="final",
    )(moe, local_mixed)


def solution(mesh):
    split = Mesh(
        mesh.devices.reshape(mesh.shape["rep"], 8, 8, 2), ("rep", "blk_0", "blk_1", "blk_2")
    )
    return jax.shard_map(
        on_device,
        mesh=split,
        in_specs=(
            P("rep", BLK),
            P("rep", None),
            P(None, "rep", BLK, None),
            P("rep"),
            P(None, "rep", BLK, None),
            P("rep"),
            P("rep"),
            P(None, BLK),
            P(),
            P(),
            P("rep", None),
            P(None, None, BLK),
            P(BLK, None),
        ),
        out_specs=P("rep", BLK),
        check_vma=False,
    )
```

```python
import functools
import math

import jax
import jax.numpy as jnp
from jax import lax
from jax.experimental import pallas as pl
from jax.experimental.pallas import tpu as pltpu
from jax.sharding import Mesh
from jax.sharding import PartitionSpec as P

QUERY_HEADS = 32
KEY_VALUE_HEADS = 8
HEAD_SIZE = 128
EXPERTS = 4
FF = 7168
BLK = ("blk_0", "blk_1", "blk_2")
GROUP = QUERY_HEADS // KEY_VALUE_HEADS
LANES = 128
HEADS = 2
PARTS = QUERY_HEADS // HEADS
SPAN = LANES // HEADS
IN_VMEM = pl.BlockSpec(memory_space=pltpu.VMEM)
IN_SMEM = pl.BlockSpec(memory_space=pltpu.SMEM)
IN_HBM = pl.BlockSpec(memory_space=pltpu.HBM)
BATCH = 4
MIB = 1 << 20
COVER = pl.CostEstimate(flops=8*10**8, bytes_accessed=8 << 20, transcendentals=0)


def exchanged(pieces, axis=BLK):
    return lax.all_to_all(pieces, axis, 0, 0, tiled=True)


def merging(kernel, shape, *pieces):
    return pl.pallas_call(
        kernel,
        out_shape=jax.ShapeDtypeStruct(shape, jnp.bfloat16),
        in_specs=[IN_VMEM] * len(pieces),
        out_specs=IN_VMEM,
        compiler_params=params(8),
        cost_estimate=COVER,
        name=kernel.__name__,
    )(*pieces)


def in_hbm(array):
    return pltpu.with_memory_space_constraint(array, pltpu.HBM)


def params(mib):
    return pltpu.CompilerParams(vmem_limit_bytes=mib * MIB)


def attention_kernel(
    positions,
    first,
    lengths_in,
    insert_slot_in,
    prefix_len_in,
    queries_in,
    weight_in,
    cache,
    inserted,
    out,
    lengths,
    insert_slot,
    prefix_len,
    queries,
    weight,
    spread,
    rows,
    score_of,
    values,
    stats,
    sems,
):
    slots, prefixes, count = lengths.shape[0], insert_slot.shape[0], rows.shape[2]
    wide = QUERY_HEADS
    copies = [
        pltpu.make_async_copy(lengths_in, lengths, sems.at[0]),
        pltpu.make_async_copy(insert_slot_in, insert_slot, sems.at[1]),
        pltpu.make_async_copy(prefix_len_in, prefix_len, sems.at[2]),
        pltpu.make_async_copy(queries_in, queries, sems.at[3]),
        pltpu.make_async_copy(weight_in, weight, sems.at[4]),
    ]
    key_copies, value_copies = [], []
    for k, group in enumerate((key_copies, value_copies)):
        for start in range(0, slots, BATCH):
            here = pl.ds(start, BATCH)
            group.append((cache.at[k, here], rows.at[k, here]))
        for start in range(0, prefixes, BATCH):
            group.append(
                (inserted.at[k, pl.ds(start, BATCH)], rows.at[k, pl.ds(slots + start, BATCH)])
            )
    for at, group in ((5, key_copies), (5 + len(key_copies), value_copies)):
        for i, (source_ref, target_ref) in enumerate(group):
            group[i] = pltpu.make_async_copy(source_ref, target_ref, sems.at[at + i])
    copies = copies[:4] + key_copies + value_copies + copies[4:]
    for copy in copies:
        copy.start()
    for copy in copies[:4]:
        copy.wait()
    for g in range(KEY_VALUE_HEADS):
        for h in range(GROUP):
            at = (g * GROUP + h) * HEAD_SIZE
            one = queries[:, at : at + HEAD_SIZE].astype(jnp.float32)
            spread[pl.ds(g * GROUP + h, slots, stride=wide), :] = one
    here = first[0]
    half = positions // 2
    there = jnp.where(here < half, here + half, here - half)
    valid, source = [], []
    for s in range(slots):
        length, at, start = lengths[s], jnp.int32(s), here
        for j in range(prefixes):
            mine = insert_slot[j] == s
            length = jnp.where(mine, prefix_len[j], length)
            at = jnp.where(mine, slots + j, at)
            start = jnp.where(mine, there, start)
        valid.append(length - start)
        source.append(at)
    for copy in key_copies:
        copy.wait()
    shape = (wide, KEY_VALUE_HEADS * HEAD_SIZE)
    own = (
        lax.broadcasted_iota(jnp.int32, shape, 0) // GROUP
        == lax.broadcasted_iota(jnp.int32, shape, 1) // HEAD_SIZE
    )
    row = lax.broadcasted_iota(jnp.int32, (wide, HEAD_SIZE), 0)
    lane = lax.broadcasted_iota(jnp.int32, (wide, HEAD_SIZE), 1)
    counted = lane // SPAN == row % HEADS
    early = lax.broadcasted_iota(jnp.int32, (2 * GROUP, HEAD_SIZE), 0) < GROUP
    place = lax.broadcasted_iota(jnp.int32, (wide, count), 1)
    for s in range(slots):
        one = spread[s * wide : (s + 1) * wide, :]
        tiled = jnp.concatenate([one] * KEY_VALUE_HEADS, axis=1)
        blocks = jnp.where(own, tiled, 0.0).astype(jnp.bfloat16)
        score_of[s] = lax.dot_general(
            blocks,
            rows[0, source[s]],
            (((1,), (1,)), ((), ())),
            preferred_element_type=jnp.float32,
        ) * (1.0 / math.sqrt(HEAD_SIZE))
    for copy in value_copies:
        copy.wait()
    for batch in range(0, slots, BATCH):
        several = range(batch, batch + BATCH)
        inside = [place < valid[s] for s in several]
        scores = [jnp.where(i, score_of[s], -1e30) for i, s in zip(inside, several)]
        peaks = [jnp.max(x, axis=1, keepdims=True) for x in scores]
        peaks = [x.astype(jnp.bfloat16).astype(jnp.float32) for x in peaks]
        weights = [
            jnp.where(i, jnp.exp(x - p), 0.0) for i, x, p in zip(inside, scores, peaks)
        ]
        totals = [jnp.sum(x, axis=1, keepdims=True) for x in weights]
        every = [
            jnp.dot(
                x.astype(jnp.bfloat16), rows[1, source[s]], preferred_element_type=jnp.float32
            )
            for x, s in zip(weights, several)
        ]
        for s, full, peak, total in zip(several, every, peaks, totals):
            value = jnp.concatenate(
                [
                    jnp.where(
                        early,
                        full[g * GROUP : (g + 2) * GROUP, g * HEAD_SIZE : (g + 1) * HEAD_SIZE],
                        full[
                            g * GROUP : (g + 2) * GROUP, (g + 1) * HEAD_SIZE : (g + 2) * HEAD_SIZE
                        ],
                    )
                    for g in range(0, KEY_VALUE_HEADS, 2)
                ],
                axis=0,
            )
            values[pl.ds(s, wide, stride=slots), :] = value / jnp.where(total > 0.0, total, 1.0)
            stats[pl.ds(s, wide, stride=slots), :] = jnp.where(
                counted, packed_stats(lane, peak, total), 0.0
            )
    deep = HEADS * slots
    copies[-1].wait()
    for o in range(PARTS):
        out[o, :deep, :] = values[o * deep : (o + 1) * deep, :].astype(jnp.bfloat16)
        one = [stats[o * deep + h * slots : o * deep + (h + 1) * slots, :] for h in range(HEADS)]
        out[o, deep : deep + slots, :] = sum(one).astype(jnp.bfloat16)
        for h in range(HEADS):
            at = deep + slots + h * weight.shape[0]
            head = (o * HEADS + h) * HEAD_SIZE
            out[o, at : at + weight.shape[0], :] = weight[:, head : head + HEAD_SIZE]


def packed_stats(lane, peak, total):
    rounded = total.astype(jnp.bfloat16).astype(jnp.float32)
    at = lane % SPAN
    return jnp.where(
        at < SPAN // 2, peak, jnp.where(at < SPAN * 3 // 4, rounded, total - rounded)
    )


def merge(pieces):
    slots = pieces[0].shape[0] // (HEADS + 1)
    found = [x[HEADS * slots :].astype(jnp.float32) for x in pieces]
    highest = functools.reduce(jnp.maximum, found)
    scales = [
        jnp.exp(x - highest)
        * (
            pltpu.roll(x, LANES - SPAN // 2, axis=1)
            + pltpu.roll(x, LANES - SPAN * 3 // 4, axis=1)
        )
        for x in found
    ]
    total = sum(scales)
    safe = jnp.where(total > 0.0, total, 1.0)
    values = []
    for h in range(HEADS):
        column = slice(h * SPAN, h * SPAN + 1)
        parts = [
            x[h * slots : (h + 1) * slots].astype(jnp.float32) * y[:, column]
            for x, y in zip(pieces, scales)
        ]
        values.append(sum(parts) / safe[:, column])
    return values, highest, total


def whole_part(pieces):
    values, highest, total = merge(pieces)
    lane = lax.broadcasted_iota(jnp.int32, highest.shape, 1)
    total = pltpu.roll(total, SPAN // 2, axis=1)
    rounded = total.astype(jnp.bfloat16).astype(jnp.float32)
    rest = pltpu.roll(total - rounded, SPAN // 4, axis=1)
    at = lane % SPAN
    stats = jnp.where(at < SPAN // 2, highest, jnp.where(at < SPAN * 3 // 4, rounded, rest))
    return jnp.concatenate(values + [stats], axis=0).astype(jnp.bfloat16)


def spread_kernel(pieces, out):
    part = whole_part([pieces[i, : out.shape[1], :] for i in range(pieces.shape[0])])
    for i in range(out.shape[0]):
        out[i] = part


def project_kernel(place, pieces, landed, hidden, out):
    slots, columns = hidden.shape
    count, deep = landed.shape[0], pieces.shape[1]
    values, _, _ = merge([pieces[i] for i in range(pieces.shape[0])])
    attn = jnp.concatenate(values, axis=1).astype(jnp.bfloat16)
    order = [i for core in range(2) for i in range(core, count, 2)]
    heads = []
    for h in range(HEADS):
        at = deep + h * columns
        parts = [landed[i, at : at + columns, :] for i in order]
        heads.append(jnp.concatenate(parts, axis=0))
    weight = jnp.concatenate(heads, axis=1)
    total = lax.dot_general(
        attn, weight, (((1,), (1,)), ((), ())), preferred_element_type=jnp.float32
    )
    tiled = jnp.concatenate([hidden[...].astype(jnp.float32)] * count, axis=1)
    owner = lax.broadcasted_iota(jnp.int32, tiled.shape, 1) // columns
    part = (total + jnp.where(owner == place[0], tiled, 0.0)).astype(jnp.bfloat16)
    half = count * columns // 2
    for i in range(count):
        out[i] = part[:, i % 2 * half : (i % 2 + 1) * half]


def mixed_kernel(place, pieces, own, out):
    columns = own.shape[1]
    total = pieces[0].astype(jnp.float32)
    for i in range(1, pieces.shape[0]):
        total = total + pieces[i].astype(jnp.float32)
    mixed = total.astype(jnp.bfloat16)
    for i in range(out.shape[0]):
        out[i] = mixed
    mine = [
        total[:, i * columns : (i + 1) * columns] for i in range(total.shape[1] // columns)
    ]
    own[...] = sum(jnp.where(place[0] == i, x, 0.0) for i, x in enumerate(mine)).astype(
        jnp.bfloat16
    )


def in_feature_order(gathered, share):
    count, slots, width = gathered.shape
    columns, rows, halves = LANES // share, count // share, width // LANES
    block = lax.broadcasted_iota(jnp.int32, (slots, LANES), 1) // columns
    tiles = {}
    for m in range(rows):
        for half in range(halves):
            found = [
                gathered[share * m + j, :, half * LANES : (half + 1) * LANES].astype(jnp.float32)
                for j in range(share)
            ]
            for b in range(share):
                tile = found[b]
                for j in range(share):
                    if j != b:
                        turned = pltpu.roll(found[j], (j - b) % share * columns, axis=1)
                        tile = jnp.where(block == j, turned, tile)
                tiles[(half * share + b) * rows + m] = tile
    return jnp.concatenate([tiles[k] for k in range(len(tiles))], axis=1)


def swapped(tiles, share):
    slots = tiles.shape[1]
    deep, width = slots // share, LANES // share
    row = lax.broadcasted_iota(jnp.int32, tiles.shape, 1) // deep
    lane = lax.broadcasted_iota(jnp.int32, tiles.shape, 2) // width
    turn = (lane - row + share) % share
    result = tiles
    for j in range(1, share):
        moved = pltpu.roll(pltpu.roll(tiles, j * width, axis=2), slots - j * deep, axis=1)
        result = jnp.where(turn == j, moved, result)
    return result


def experts_kernel(
    share, expert, core, gathered, gain, router, chosen, gate_up, down, own, other
):
    blocks, slots = own.shape[0], 2 * own.shape[1]
    mixed = in_feature_order(gathered, share)
    scale = lax.rsqrt(jnp.sum(mixed * mixed, axis=1, keepdims=True) / (blocks * LANES) + 1e-05)
    normed = (mixed * scale * gain[...].astype(jnp.float32).reshape(1, blocks * LANES)).astype(jnp.bfloat16)
    plain = normed.astype(jnp.float32)
    weights = router[...].astype(jnp.float32)
    logits = [
        jnp.sum(plain * weights[e : e + 1], axis=1, keepdims=True) for e in range(EXPERTS)
    ]
    upright = lax.broadcasted_iota(jnp.int32, (slots, slots), 0) == lax.broadcasted_iota(
        jnp.int32, (slots, slots), 1
    )
    ids = [
        jnp.sum(
            jnp.where(upright, chosen[i : i + 1, :].astype(jnp.float32), 0.0),
            axis=1,
            keepdims=True,
        )
        for i in range(2)
    ]
    picked = [sum(jnp.where(k == e, logits[e], 0.0) for e in range(EXPERTS)) for k in ids]
    gates = [jax.nn.sigmoid(picked[i] - picked[1 - i]) for i in range(2)]
    mine = expert[0].astype(jnp.float32)
    part = sum(jnp.where(ids[i] == mine, gates[i], 0.0) for i in range(2))
    gate, up = [
        lax.dot_general(
            normed, gate_up[i], (((1,), (1,)), ((), ())), preferred_element_type=jnp.float32
        )
        for i in range(2)
    ]
    act = (gate * jax.nn.sigmoid(gate) * up).astype(jnp.bfloat16)
    term = part * jnp.dot(act, down[...], preferred_element_type=jnp.float32)
    tiles = [term[None, :, k * LANES : (k + 1) * LANES] for k in range(blocks)]
    even, odd = by_core(swapped(jnp.concatenate(tiles, axis=0), share), slots // share)
    own[...] = jnp.where(core[0] == 0, even, odd)
    other[...] = jnp.where(core[0] == 0, odd, even).astype(jnp.bfloat16)


def by_core(tiles, deep):
    top, bottom = tiles[:, : 2 * deep], tiles[:, 2 * deep :]
    first = lax.broadcasted_iota(jnp.int32, top.shape, 1) < deep
    even = jnp.where(first, top, pltpu.roll(bottom, deep, axis=1))
    odd = jnp.where(first, pltpu.roll(top, deep, axis=1), bottom)
    return even, odd


def add_kernel(own, other, out):
    out[...] = (own[...] + other[...].astype(jnp.float32)).astype(jnp.bfloat16)


def final_kernel(pieces, mixed, out):
    slots, columns = mixed.shape
    share = LANES // columns
    total = jnp.sum(pieces[...].astype(jnp.float32), axis=0)
    moe = jnp.concatenate(
        [total[:, b * columns : (b + 1) * columns] for b in range(share)], axis=0
    )
    out[...] = (mixed[...].astype(jnp.float32) + moe).astype(jnp.bfloat16)


def on_device(
    hidden,
    queries,
    cache_kv,
    cache_len,
    inserted_key_value,
    insert_slot,
    prefix_len,
    out_weight,
    norm_gain,
    router_weight,
    expert_ids,
    gate_up,
    down_proj,
):
    devices = lax.axis_size(BLK)
    dev_index = lax.axis_index(BLK)
    slots, columns = hidden.shape
    ctx_rows, kv_width = cache_kv.shape[2:]
    prefixes = insert_slot.shape[0]
    share = LANES // columns
    deep = slots * (HEADS + 1)
    width = devices * columns
    blocks = width // LANES
    bf16 = jnp.bfloat16

    first = (dev_index * ctx_rows).astype(jnp.int32).reshape(1)
    place = lax.axis_index(BLK[0]).astype(jnp.int32).reshape(1)
    expert = (dev_index * gate_up.shape[2] // FF).astype(jnp.int32).reshape(1)
    core = lax.axis_index(BLK[2]).astype(jnp.int32).reshape(1)
    block = core * lax.axis_size(BLK[0]) + place
    first, place, expert, core, block = lax.optimization_barrier(
        (first, place, expert, core, block)
    )
    partials = pl.pallas_call(
        functools.partial(attention_kernel, devices * ctx_rows),
        out_shape=jax.ShapeDtypeStruct((PARTS, deep + HEADS * columns, HEAD_SIZE), bf16),
        in_specs=[IN_SMEM] + [IN_HBM] * 7,
        out_specs=IN_VMEM,
        scratch_shapes=[
            pltpu.SMEM((slots,), jnp.int32),
            pltpu.SMEM((prefixes,), jnp.int32),
            pltpu.SMEM((prefixes,), jnp.int32),
            pltpu.VMEM(queries.shape, bf16),
            pltpu.VMEM(out_weight.shape[::-1], bf16),
            pltpu.VMEM((slots * QUERY_HEADS, HEAD_SIZE), jnp.float32),
            pltpu.VMEM((2, slots + prefixes, ctx_rows, kv_width), bf16),
            pltpu.VMEM((slots, QUERY_HEADS, ctx_rows), jnp.float32),
            pltpu.VMEM((slots * QUERY_HEADS, HEAD_SIZE), jnp.float32),
            pltpu.VMEM((slots * QUERY_HEADS, HEAD_SIZE), jnp.float32),
            pltpu.SemaphoreType.DMA((5 + 2 * (slots + prefixes) // BATCH,)),
        ],
        compiler_params=params(24),
        name="attention",
    )(
        first,
        in_hbm(cache_len),
        in_hbm(insert_slot),
        in_hbm(prefix_len),
        in_hbm(queries),
        in_hbm(out_weight.T),
        in_hbm(cache_kv),
        in_hbm(inserted_key_value),
    )
    along, across, pair = BLK
    copies = lax.axis_size(across)
    landed = exchanged(partials, (along, pair))
    part = merging(spread_kernel, (copies, deep, HEAD_SIZE), landed)
    count = lax.axis_size(along)
    parts = pl.pallas_call(
        project_kernel,
        out_shape=jax.ShapeDtypeStruct((2 * count, slots, count * columns), bf16),
        in_specs=[IN_SMEM] + [IN_VMEM] * 3,
        out_specs=IN_VMEM,
        compiler_params=params(8),
        cost_estimate=COVER,
        name="project",
    )(block, exchanged(part, across), landed, hidden)
    local_mixed, packed = pl.pallas_call(
        mixed_kernel,
        out_shape=(
            jax.ShapeDtypeStruct((slots, columns), bf16),
            jax.ShapeDtypeStruct((devices // count, slots, count * columns), bf16),
        ),
        in_specs=[IN_SMEM, IN_VMEM],
        out_specs=(IN_VMEM, IN_VMEM),
        compiler_params=params(8),
        cost_estimate=COVER,
        name="mixed",
    )(place, exchanged(parts, (along, pair)))
    gathered = exchanged(packed, (across, pair))

    own, other = pl.pallas_call(
        functools.partial(experts_kernel, share),
        out_shape=(
            jax.ShapeDtypeStruct((blocks, slots // 2, LANES), jnp.float32),
            jax.ShapeDtypeStruct((blocks, slots // 2, LANES), bf16),
        ),
        in_specs=[IN_SMEM] * 2 + [IN_VMEM] * 6,
        out_specs=(IN_VMEM, IN_VMEM),
        compiler_params=params(24),
        name="experts",
    )(
        expert,
        core,
        gathered,
        norm_gain,
        router_weight.T,
        expert_ids.T,
        jnp.swapaxes(gate_up, 1, 2),
        down_proj,
    )
    other = lax.ppermute(other, pair, [(0, 1), (1, 0)])
    terms = merging(add_kernel, own.shape, own, other)
    moe = exchanged(terms.reshape(devices // 2, slots // share, LANES), (along, across))
    return pl.pallas_call(
        final_kernel,
        out_shape=jax.ShapeDtypeStruct((slots, columns), bf16),
        in_specs=[IN_VMEM] * 2,
        out_specs=IN_VMEM,
        compiler_params=params(4),
        name="final",
    )(moe, local_mixed)


def solution(mesh):
    split = Mesh(
        mesh.devices.reshape(mesh.shape["rep"], 8, 8, 2), ("rep", "blk_0", "blk_1", "blk_2")
    )
    return jax.shard_map(
        on_device,
        mesh=split,
        in_specs=(
            P("rep", BLK),
            P("rep", None),
            P(None, "rep", BLK, None),
            P("rep"),
            P(None, "rep", BLK, None),
            P("rep"),
            P("rep"),
            P(None, BLK),
            P(),
            P(),
            P("rep", None),
            P(None, None, BLK),
            P(BLK, None),
        ),
        out_specs=P("rep", BLK),
        check_vma=False,
    )
```

```python
import functools
import math

import jax
import jax.numpy as jnp
from jax import lax
from jax.experimental import pallas as pl
from jax.experimental.pallas import tpu as pltpu
from jax.sharding import Mesh
from jax.sharding import PartitionSpec as P

QUERY_HEADS = 32
KEY_VALUE_HEADS = 8
HEAD_SIZE = 128
EXPERTS = 4
FF = 7168
BLK = ("blk_0", "blk_1", "blk_2")
GROUP = QUERY_HEADS // KEY_VALUE_HEADS
LANES = 128
SPAN = LANES // GROUP
IN_VMEM = pl.BlockSpec(memory_space=pltpu.VMEM)
IN_SMEM = pl.BlockSpec(memory_space=pltpu.SMEM)
IN_HBM = pl.BlockSpec(memory_space=pltpu.HBM)
BATCH = 4
SOFTMAX_BATCH = 8
MIB = 1 << 20
COVER = pl.CostEstimate(flops=8*10**8, bytes_accessed=8 << 20, transcendentals=0)


def exchanged(pieces, axis=BLK):
    return lax.all_to_all(pieces, axis, 0, 0, tiled=True)


def merging(kernel, shape, *pieces):
    return pl.pallas_call(
        kernel,
        out_shape=jax.ShapeDtypeStruct(shape, jnp.bfloat16),
        in_specs=[IN_VMEM] * len(pieces),
        out_specs=IN_VMEM,
        compiler_params=params(8),
        cost_estimate=COVER,
        name=kernel.__name__,
    )(*pieces)


def in_hbm(array):
    return pltpu.with_memory_space_constraint(array, pltpu.HBM)


def params(mib):
    return pltpu.CompilerParams(vmem_limit_bytes=mib * MIB)


def attention_kernel(
    positions,
    first,
    lengths_in,
    insert_slot_in,
    prefix_len_in,
    queries_in,
    weight_in,
    cache,
    inserted,
    out,
    lengths,
    insert_slot,
    prefix_len,
    queries,
    weight,
    spread,
    rows,
    score_of,
    values,
    stats,
    sems,
):
    slots, prefixes, count = lengths.shape[0], insert_slot.shape[0], rows.shape[2]
    wide = QUERY_HEADS
    copies = [
        pltpu.make_async_copy(lengths_in, lengths, sems.at[0]),
        pltpu.make_async_copy(insert_slot_in, insert_slot, sems.at[1]),
        pltpu.make_async_copy(prefix_len_in, prefix_len, sems.at[2]),
        pltpu.make_async_copy(queries_in, queries, sems.at[3]),
        pltpu.make_async_copy(weight_in, weight, sems.at[4]),
    ]
    key_copies, value_copies = [], []
    for k, group in enumerate((key_copies, value_copies)):
        for start in range(0, slots, BATCH):
            here = pl.ds(start, BATCH)
            group.append((cache.at[k, here], rows.at[k, here]))
        for start in range(0, prefixes, BATCH):
            group.append(
                (inserted.at[k, pl.ds(start, BATCH)], rows.at[k, pl.ds(slots + start, BATCH)])
            )
    for at, group in ((5, key_copies), (5 + len(key_copies), value_copies)):
        for i, (source_ref, target_ref) in enumerate(group):
            group[i] = pltpu.make_async_copy(source_ref, target_ref, sems.at[at + i])
    copies = copies[:4] + key_copies + value_copies + copies[4:]
    for copy in copies:
        copy.start()
    for copy in copies[:4]:
        copy.wait()
    for g in range(KEY_VALUE_HEADS):
        for h in range(GROUP):
            at = (g * GROUP + h) * HEAD_SIZE
            one = queries[:, at : at + HEAD_SIZE].astype(jnp.float32)
            spread[pl.ds(g * GROUP + h, slots, stride=wide), :] = one
    here = first[0]
    half = positions // 2
    there = jnp.where(here < half, here + half, here - half)
    valid, source = [], []
    for s in range(slots):
        length, at, start = lengths[s], jnp.int32(s), here
        for j in range(prefixes):
            mine = insert_slot[j] == s
            length = jnp.where(mine, prefix_len[j], length)
            at = jnp.where(mine, slots + j, at)
            start = jnp.where(mine, there, start)
        valid.append(length - start)
        source.append(at)
    for copy in key_copies:
        copy.wait()
    shape = (wide, KEY_VALUE_HEADS * HEAD_SIZE)
    own = (
        lax.broadcasted_iota(jnp.int32, shape, 0) // GROUP
        == lax.broadcasted_iota(jnp.int32, shape, 1) // HEAD_SIZE
    )
    row = lax.broadcasted_iota(jnp.int32, (wide, HEAD_SIZE), 0)
    lane = lax.broadcasted_iota(jnp.int32, (wide, HEAD_SIZE), 1)
    counted = lane // SPAN == row % GROUP
    early = lax.broadcasted_iota(jnp.int32, (2 * GROUP, HEAD_SIZE), 0) < GROUP
    place = lax.broadcasted_iota(jnp.int32, (wide, count), 1)
    for s in range(slots):
        one = spread[s * wide : (s + 1) * wide, :]
        tiled = jnp.concatenate([one] * KEY_VALUE_HEADS, axis=1)
        blocks = jnp.where(own, tiled, 0.0).astype(jnp.bfloat16)
        score_of[s] = lax.dot_general(
            blocks,
            rows[0, source[s]],
            (((1,), (1,)), ((), ())),
            preferred_element_type=jnp.float32,
        ) * (1.0 / math.sqrt(HEAD_SIZE))
    for copy in value_copies:
        copy.wait()
    for batch in range(0, slots, SOFTMAX_BATCH):
        several = range(batch, batch + SOFTMAX_BATCH)
        inside = [place < valid[s] for s in several]
        scores = [jnp.where(i, score_of[s], -1e30) for i, s in zip(inside, several)]
        peaks = [jnp.max(x, axis=1, keepdims=True) for x in scores]
        peaks = [x.astype(jnp.bfloat16).astype(jnp.float32) for x in peaks]
        weights = [
            jnp.where(i, jnp.exp(x - p), 0.0) for i, x, p in zip(inside, scores, peaks)
        ]
        totals = [jnp.sum(x, axis=1, keepdims=True) for x in weights]
        every = [
            jnp.dot(
                x.astype(jnp.bfloat16), rows[1, source[s]], preferred_element_type=jnp.float32
            )
            for x, s in zip(weights, several)
        ]
        for s, full, peak, total in zip(several, every, peaks, totals):
            value = jnp.concatenate(
                [
                    jnp.where(
                        early,
                        full[g * GROUP : (g + 2) * GROUP, g * HEAD_SIZE : (g + 1) * HEAD_SIZE],
                        full[
                            g * GROUP : (g + 2) * GROUP, (g + 1) * HEAD_SIZE : (g + 2) * HEAD_SIZE
                        ],
                    )
                    for g in range(0, KEY_VALUE_HEADS, 2)
                ],
                axis=0,
            )
            values[pl.ds(s, wide, stride=slots), :] = value / jnp.where(total > 0.0, total, 1.0)
            stats[pl.ds(s, wide, stride=slots), :] = jnp.where(
                counted, packed_stats(lane, peak, total), 0.0
            )
    deep = GROUP * slots
    copies[-1].wait()
    for g in range(KEY_VALUE_HEADS):
        out[g, :deep, :] = values[g * deep : (g + 1) * deep, :].astype(jnp.bfloat16)
        one = [stats[g * deep + h * slots : g * deep + (h + 1) * slots, :] for h in range(GROUP)]
        out[g, deep : deep + slots, :] = sum(one).astype(jnp.bfloat16)
        for h in range(GROUP):
            at = deep + slots + h * weight.shape[0]
            head = (g * GROUP + h) * HEAD_SIZE
            out[g, at : at + weight.shape[0], :] = weight[:, head : head + HEAD_SIZE]


def packed_stats(lane, peak, total):
    rounded = total.astype(jnp.bfloat16).astype(jnp.float32)
    at = lane % SPAN
    return jnp.where(
        at < SPAN // 2, peak, jnp.where(at < SPAN * 3 // 4, rounded, total - rounded)
    )


def merge(pieces):
    slots = pieces[0].shape[0] // (GROUP + 1)
    found = [x[GROUP * slots :].astype(jnp.float32) for x in pieces]
    highest = functools.reduce(jnp.maximum, found)
    scales = [
        jnp.exp(x - highest)
        * (
            pltpu.roll(x, LANES - SPAN // 2, axis=1)
            + pltpu.roll(x, LANES - SPAN * 3 // 4, axis=1)
        )
        for x in found
    ]
    total = sum(scales)
    safe = jnp.where(total > 0.0, total, 1.0)
    values = []
    for h in range(GROUP):
        column = slice(h * SPAN, h * SPAN + 1)
        parts = [
            x[h * slots : (h + 1) * slots].astype(jnp.float32) * y[:, column]
            for x, y in zip(pieces, scales)
        ]
        values.append(sum(parts) / safe[:, column])
    return values, highest, total


def whole_part(pieces):
    values, highest, total = merge(pieces)
    lane = lax.broadcasted_iota(jnp.int32, highest.shape, 1)
    total = pltpu.roll(total, SPAN // 2, axis=1)
    rounded = total.astype(jnp.bfloat16).astype(jnp.float32)
    rest = pltpu.roll(total - rounded, SPAN // 4, axis=1)
    at = lane % SPAN
    stats = jnp.where(at < SPAN // 2, highest, jnp.where(at < SPAN * 3 // 4, rounded, rest))
    return jnp.concatenate(values + [stats], axis=0).astype(jnp.bfloat16)


def spread_kernel(pieces, out):
    part = whole_part([pieces[i, : out.shape[1], :] for i in range(pieces.shape[0])])
    for i in range(out.shape[0]):
        out[i] = part


def part_kernel(pieces, out):
    out[...] = whole_part([pieces[i] for i in range(pieces.shape[0])])


def project_kernel(place, mine, other, landed, hidden, out):
    slots, columns = hidden.shape
    count, deep = landed.shape[0], mine.shape[0]
    values, _, _ = merge([mine[...], other[...]])
    attn = jnp.concatenate(values, axis=1).astype(jnp.bfloat16)
    heads = []
    for h in range(GROUP):
        at = deep + h * columns
        parts = [landed[i, at : at + columns, :] for i in range(count)]
        heads.append(jnp.concatenate(parts, axis=0))
    weight = jnp.concatenate(heads, axis=1)
    total = lax.dot_general(
        attn, weight, (((1,), (1,)), ((), ())), preferred_element_type=jnp.float32
    )
    tiled = jnp.concatenate([hidden[...].astype(jnp.float32)] * count, axis=1)
    owner = lax.broadcasted_iota(jnp.int32, tiled.shape, 1) // columns
    part = (total + jnp.where(owner == place[0], tiled, 0.0)).astype(jnp.bfloat16)
    for i in range(count):
        out[i] = part


def mixed_kernel(place, pieces, own, out):
    columns = own.shape[1]
    total = pieces[0].astype(jnp.float32)
    for i in range(1, pieces.shape[0]):
        total = total + pieces[i].astype(jnp.float32)
    mixed = total.astype(jnp.bfloat16)
    for i in range(out.shape[0]):
        out[i] = mixed
    mine = [total[:, i * columns : (i + 1) * columns] for i in range(pieces.shape[0])]
    own[...] = sum(jnp.where(place[0] == i, x, 0.0) for i, x in enumerate(mine)).astype(
        jnp.bfloat16
    )


def in_feature_order(gathered, share):
    count, slots, width = gathered.shape
    columns, rows, halves = LANES // share, count // share, width // LANES
    block = lax.broadcasted_iota(jnp.int32, (slots, LANES), 1) // columns
    tiles = {}
    for m in range(rows):
        for half in range(halves):
            found = [
                gathered[share * m + j, :, half * LANES : (half + 1) * LANES].astype(jnp.float32)
                for j in range(share)
            ]
            for b in range(share):
                tile = found[b]
                for j in range(share):
                    if j != b:
                        turned = pltpu.roll(found[j], (j - b) % share * columns, axis=1)
                        tile = jnp.where(block == j, turned, tile)
                tiles[(half * share + b) * rows + m] = tile
    return jnp.concatenate([tiles[k] for k in range(len(tiles))], axis=1)


def swapped(tiles, share):
    slots = tiles.shape[1]
    deep, width = slots // share, LANES // share
    row = lax.broadcasted_iota(jnp.int32, tiles.shape, 1) // deep
    lane = lax.broadcasted_iota(jnp.int32, tiles.shape, 2) // width
    turn = (lane - row + share) % share
    result = tiles
    for j in range(1, share):
        moved = pltpu.roll(pltpu.roll(tiles, j * width, axis=2), slots - j * deep, axis=1)
        result = jnp.where(turn == j, moved, result)
    return result


def experts_kernel(
    share, expert, core, gathered, gain, router, chosen, gate_up, down, own, other
):
    blocks, slots = own.shape[0], 2 * own.shape[1]
    mixed = in_feature_order(gathered, share)
    scale = lax.rsqrt(jnp.sum(mixed * mixed, axis=1, keepdims=True) / (blocks * LANES) + 1e-05)
    normed = (mixed * scale * gain[...].astype(jnp.float32).reshape(1, blocks * LANES)).astype(jnp.bfloat16)
    plain = normed.astype(jnp.float32)
    weights = router[...].astype(jnp.float32)
    logits = [
        jnp.sum(plain * weights[e : e + 1], axis=1, keepdims=True) for e in range(EXPERTS)
    ]
    upright = lax.broadcasted_iota(jnp.int32, (slots, slots), 0) == lax.broadcasted_iota(
        jnp.int32, (slots, slots), 1
    )
    ids = [
        jnp.sum(
            jnp.where(upright, chosen[i : i + 1, :].astype(jnp.float32), 0.0),
            axis=1,
            keepdims=True,
        )
        for i in range(2)
    ]
    picked = [sum(jnp.where(k == e, logits[e], 0.0) for e in range(EXPERTS)) for k in ids]
    gates = [jax.nn.sigmoid(picked[i] - picked[1 - i]) for i in range(2)]
    mine = expert[0].astype(jnp.float32)
    part = sum(jnp.where(ids[i] == mine, gates[i], 0.0) for i in range(2))
    gate, up = [
        lax.dot_general(
            normed, gate_up[i], (((1,), (1,)), ((), ())), preferred_element_type=jnp.float32
        )
        for i in range(2)
    ]
    act = (gate * jax.nn.sigmoid(gate) * up).astype(jnp.bfloat16)
    term = part * jnp.dot(act, down[...], preferred_element_type=jnp.float32)
    tiles = [term[None, :, k * LANES : (k + 1) * LANES] for k in range(blocks)]
    even, odd = by_core(swapped(jnp.concatenate(tiles, axis=0), share), slots // share)
    own[...] = jnp.where(core[0] == 0, even, odd)
    other[...] = jnp.where(core[0] == 0, odd, even).astype(jnp.bfloat16)


def by_core(tiles, deep):
    top, bottom = tiles[:, : 2 * deep], tiles[:, 2 * deep :]
    first = lax.broadcasted_iota(jnp.int32, top.shape, 1) < deep
    even = jnp.where(first, top, pltpu.roll(bottom, deep, axis=1))
    odd = jnp.where(first, pltpu.roll(top, deep, axis=1), bottom)
    return even, odd


def add_kernel(own, other, out):
    out[...] = (own[...] + other[...].astype(jnp.float32)).astype(jnp.bfloat16)


def final_kernel(pieces, mixed, out):
    slots, columns = mixed.shape
    share = LANES // columns
    total = jnp.sum(pieces[...].astype(jnp.float32), axis=0)
    moe = jnp.concatenate(
        [total[:, b * columns : (b + 1) * columns] for b in range(share)], axis=0
    )
    out[...] = (mixed[...].astype(jnp.float32) + moe).astype(jnp.bfloat16)


def on_device(
    hidden,
    queries,
    cache_kv,
    cache_len,
    inserted_key_value,
    insert_slot,
    prefix_len,
    out_weight,
    norm_gain,
    router_weight,
    expert_ids,
    gate_up,
    down_proj,
):
    devices = lax.axis_size(BLK)
    dev_index = lax.axis_index(BLK)
    slots, columns = hidden.shape
    ctx_rows, kv_width = cache_kv.shape[2:]
    prefixes = insert_slot.shape[0]
    share = LANES // columns
    deep = slots * (GROUP + 1)
    width = devices * columns
    blocks = width // LANES
    bf16 = jnp.bfloat16

    first = (dev_index * ctx_rows).astype(jnp.int32).reshape(1)
    place = lax.axis_index(BLK[0]).astype(jnp.int32).reshape(1)
    expert = (dev_index * gate_up.shape[2] // FF).astype(jnp.int32).reshape(1)
    core = lax.axis_index(BLK[2]).astype(jnp.int32).reshape(1)
    first, place, expert, core = lax.optimization_barrier((first, place, expert, core))
    partials = pl.pallas_call(
        functools.partial(attention_kernel, devices * ctx_rows),
        out_shape=jax.ShapeDtypeStruct((KEY_VALUE_HEADS, deep + GROUP * columns, HEAD_SIZE), bf16),
        in_specs=[IN_SMEM] + [IN_HBM] * 7,
        out_specs=IN_VMEM,
        scratch_shapes=[
            pltpu.SMEM((slots,), jnp.int32),
            pltpu.SMEM((prefixes,), jnp.int32),
            pltpu.SMEM((prefixes,), jnp.int32),
            pltpu.VMEM(queries.shape, bf16),
            pltpu.VMEM(out_weight.shape[::-1], bf16),
            pltpu.VMEM((slots * QUERY_HEADS, HEAD_SIZE), jnp.float32),
            pltpu.VMEM((2, slots + prefixes, ctx_rows, kv_width), bf16),
            pltpu.VMEM((slots, QUERY_HEADS, ctx_rows), jnp.float32),
            pltpu.VMEM((slots * QUERY_HEADS, HEAD_SIZE), jnp.float32),
            pltpu.VMEM((slots * QUERY_HEADS, HEAD_SIZE), jnp.float32),
            pltpu.SemaphoreType.DMA((5 + 2 * (slots + prefixes) // BATCH,)),
        ],
        compiler_params=params(24),
        name="attention",
    )(
        first,
        in_hbm(cache_len),
        in_hbm(insert_slot),
        in_hbm(prefix_len),
        in_hbm(queries),
        in_hbm(out_weight.T),
        in_hbm(cache_kv),
        in_hbm(inserted_key_value),
    )
    along, across, pair = BLK
    copies = lax.axis_size(across)
    landed = exchanged(partials, along)
    part = merging(spread_kernel, (copies, deep, HEAD_SIZE), landed)
    part = merging(part_kernel, (deep, HEAD_SIZE), exchanged(part, across))
    other = lax.ppermute(part, pair, [(0, 1), (1, 0)])
    count = lax.axis_size(along)
    parts = pl.pallas_call(
        project_kernel,
        out_shape=jax.ShapeDtypeStruct((count, slots, count * columns), bf16),
        in_specs=[IN_SMEM] + [IN_VMEM] * 4,
        out_specs=IN_VMEM,
        compiler_params=params(8),
        cost_estimate=COVER,
        name="project",
    )(place, part, other, landed, hidden)
    local_mixed, packed = pl.pallas_call(
        mixed_kernel,
        out_shape=(
            jax.ShapeDtypeStruct((slots, columns), bf16),
            jax.ShapeDtypeStruct((devices // count, slots, count * columns), bf16),
        ),
        in_specs=[IN_SMEM, IN_VMEM],
        out_specs=(IN_VMEM, IN_VMEM),
        compiler_params=params(8),
        cost_estimate=COVER,
        name="mixed",
    )(place, exchanged(parts, along))
    gathered = exchanged(packed, (across, pair))

    own, other = pl.pallas_call(
        functools.partial(experts_kernel, share),
        out_shape=(
            jax.ShapeDtypeStruct((blocks, slots // 2, LANES), jnp.float32),
            jax.ShapeDtypeStruct((blocks, slots // 2, LANES), bf16),
        ),
        in_specs=[IN_SMEM] * 2 + [IN_VMEM] * 6,
        out_specs=(IN_VMEM, IN_VMEM),
        compiler_params=params(24),
        name="experts",
    )(
        expert,
        core,
        gathered,
        norm_gain,
        router_weight.T,
        expert_ids.T,
        jnp.swapaxes(gate_up, 1, 2),
        down_proj,
    )
    other = lax.ppermute(other, pair, [(0, 1), (1, 0)])
    terms = merging(add_kernel, own.shape, own, other)
    moe = exchanged(terms.reshape(devices // 2, slots // share, LANES), (along, across))
    return pl.pallas_call(
        final_kernel,
        out_shape=jax.ShapeDtypeStruct((slots, columns), bf16),
        in_specs=[IN_VMEM] * 2,
        out_specs=IN_VMEM,
        compiler_params=params(4),
        name="final",
    )(moe, local_mixed)


def solution(mesh):
    split = Mesh(
        mesh.devices.reshape(mesh.shape["rep"], 8, 8, 2), ("rep", "blk_0", "blk_1", "blk_2")
    )
    return jax.shard_map(
        on_device,
        mesh=split,
        in_specs=(
            P("rep", BLK),
            P("rep", None),
            P(None, "rep", BLK, None),
            P("rep"),
            P(None, "rep", BLK, None),
            P("rep"),
            P("rep"),
            P(None, BLK),
            P(),
            P(),
            P("rep", None),
            P(None, None, BLK),
            P(BLK, None),
        ),
        out_specs=P("rep", BLK),
        check_vma=False,
    )
```

```python
import functools
import math

import jax
import jax.numpy as jnp
from jax import lax
from jax.experimental import pallas as pl
from jax.experimental.pallas import tpu as pltpu
from jax.sharding import Mesh
from jax.sharding import PartitionSpec as P

QUERY_HEADS = 32
KEY_VALUE_HEADS = 8
HEAD_SIZE = 128
EXPERTS = 4
FF = 7168
BLK = ("blk_0", "blk_1", "blk_2")
GROUP = QUERY_HEADS // KEY_VALUE_HEADS
LANES = 128
SPAN = LANES // GROUP
IN_VMEM = pl.BlockSpec(memory_space=pltpu.VMEM)
IN_SMEM = pl.BlockSpec(memory_space=pltpu.SMEM)
IN_HBM = pl.BlockSpec(memory_space=pltpu.HBM)
BATCH = 8
MIB = 1 << 20
COVER = pl.CostEstimate(flops=8*10**8, bytes_accessed=8 << 20, transcendentals=0)


def exchanged(pieces, axis=BLK):
    return lax.all_to_all(pieces, axis, 0, 0, tiled=True)


def merging(kernel, shape, *pieces):
    return pl.pallas_call(
        kernel,
        out_shape=jax.ShapeDtypeStruct(shape, jnp.bfloat16),
        in_specs=[IN_VMEM] * len(pieces),
        out_specs=IN_VMEM,
        compiler_params=params(8),
        cost_estimate=COVER,
        name=kernel.__name__,
    )(*pieces)


def in_hbm(array):
    return pltpu.with_memory_space_constraint(array, pltpu.HBM)


def params(mib):
    return pltpu.CompilerParams(vmem_limit_bytes=mib * MIB)


def attention_kernel(
    positions,
    first,
    lengths_in,
    insert_slot_in,
    prefix_len_in,
    queries_in,
    weight_in,
    cache,
    inserted,
    out,
    lengths,
    insert_slot,
    prefix_len,
    queries,
    weight,
    spread,
    rows,
    score_of,
    values,
    stats,
    sems,
):
    slots, prefixes, count = lengths.shape[0], insert_slot.shape[0], rows.shape[2]
    wide = QUERY_HEADS
    copies = [
        pltpu.make_async_copy(lengths_in, lengths, sems.at[0]),
        pltpu.make_async_copy(insert_slot_in, insert_slot, sems.at[1]),
        pltpu.make_async_copy(prefix_len_in, prefix_len, sems.at[2]),
        pltpu.make_async_copy(queries_in, queries, sems.at[3]),
        pltpu.make_async_copy(weight_in, weight, sems.at[4]),
    ]
    key_copies, value_copies = [], []
    for k, group in enumerate((key_copies, value_copies)):
        for start in range(0, slots, BATCH):
            here = pl.ds(start, BATCH)
            group.append((cache.at[k, here], rows.at[k, here]))
        for start in range(0, prefixes, BATCH):
            group.append(
                (inserted.at[k, pl.ds(start, BATCH)], rows.at[k, pl.ds(slots + start, BATCH)])
            )
    for at, group in ((5, key_copies), (5 + len(key_copies), value_copies)):
        for i, (source_ref, target_ref) in enumerate(group):
            group[i] = pltpu.make_async_copy(source_ref, target_ref, sems.at[at + i])
    copies = copies[:4] + key_copies + value_copies + copies[4:]
    for copy in copies:
        copy.start()
    for copy in copies[:4]:
        copy.wait()
    for g in range(KEY_VALUE_HEADS):
        for h in range(GROUP):
            at = (g * GROUP + h) * HEAD_SIZE
            one = queries[:, at : at + HEAD_SIZE].astype(jnp.float32)
            spread[pl.ds(g * GROUP + h, slots, stride=wide), :] = one
    here = first[0]
    half = positions // 2
    there = jnp.where(here < half, here + half, here - half)
    valid, source = [], []
    for s in range(slots):
        length, at, start = lengths[s], jnp.int32(s), here
        for j in range(prefixes):
            mine = insert_slot[j] == s
            length = jnp.where(mine, prefix_len[j], length)
            at = jnp.where(mine, slots + j, at)
            start = jnp.where(mine, there, start)
        valid.append(length - start)
        source.append(at)
    for copy in key_copies:
        copy.wait()
    shape = (wide, KEY_VALUE_HEADS * HEAD_SIZE)
    own = (
        lax.broadcasted_iota(jnp.int32, shape, 0) // GROUP
        == lax.broadcasted_iota(jnp.int32, shape, 1) // HEAD_SIZE
    )
    row = lax.broadcasted_iota(jnp.int32, (wide, HEAD_SIZE), 0)
    lane = lax.broadcasted_iota(jnp.int32, (wide, HEAD_SIZE), 1)
    counted = lane // SPAN == row % GROUP
    early = lax.broadcasted_iota(jnp.int32, (2 * GROUP, HEAD_SIZE), 0) < GROUP
    place = lax.broadcasted_iota(jnp.int32, (wide, count), 1)
    for s in range(slots):
        one = spread[s * wide : (s + 1) * wide, :]
        tiled = jnp.concatenate([one] * KEY_VALUE_HEADS, axis=1)
        blocks = jnp.where(own, tiled, 0.0).astype(jnp.bfloat16)
        score_of[s] = lax.dot_general(
            blocks,
            rows[0, source[s]],
            (((1,), (1,)), ((), ())),
            preferred_element_type=jnp.float32,
        ) * (1.0 / math.sqrt(HEAD_SIZE))
    for copy in value_copies:
        copy.wait()
    for batch in range(0, slots, BATCH):
        several = range(batch, batch + BATCH)
        inside = [place < valid[s] for s in several]
        scores = [jnp.where(i, score_of[s], -1e30) for i, s in zip(inside, several)]
        peaks = [jnp.max(x, axis=1, keepdims=True) for x in scores]
        peaks = [x.astype(jnp.bfloat16).astype(jnp.float32) for x in peaks]
        weights = [
            jnp.where(i, jnp.exp(x - p), 0.0) for i, x, p in zip(inside, scores, peaks)
        ]
        totals = [jnp.sum(x, axis=1, keepdims=True) for x in weights]
        every = [
            jnp.dot(
                x.astype(jnp.bfloat16), rows[1, source[s]], preferred_element_type=jnp.float32
            )
            for x, s in zip(weights, several)
        ]
        for s, full, peak, total in zip(several, every, peaks, totals):
            value = jnp.concatenate(
                [
                    jnp.where(
                        early,
                        full[g * GROUP : (g + 2) * GROUP, g * HEAD_SIZE : (g + 1) * HEAD_SIZE],
                        full[
                            g * GROUP : (g + 2) * GROUP, (g + 1) * HEAD_SIZE : (g + 2) * HEAD_SIZE
                        ],
                    )
                    for g in range(0, KEY_VALUE_HEADS, 2)
                ],
                axis=0,
            )
            values[pl.ds(s, wide, stride=slots), :] = value / jnp.where(total > 0.0, total, 1.0)
            stats[pl.ds(s, wide, stride=slots), :] = jnp.where(
                counted, packed_stats(lane, peak, total), 0.0
            )
    deep = GROUP * slots
    copies[-1].wait()
    for g in range(KEY_VALUE_HEADS):
        out[g, :deep, :] = values[g * deep : (g + 1) * deep, :].astype(jnp.bfloat16)
        one = [stats[g * deep + h * slots : g * deep + (h + 1) * slots, :] for h in range(GROUP)]
        out[g, deep : deep + slots, :] = sum(one).astype(jnp.bfloat16)
        for h in range(GROUP):
            at = deep + slots + h * weight.shape[0]
            head = (g * GROUP + h) * HEAD_SIZE
            out[g, at : at + weight.shape[0], :] = weight[:, head : head + HEAD_SIZE]


def packed_stats(lane, peak, total):
    rounded = total.astype(jnp.bfloat16).astype(jnp.float32)
    at = lane % SPAN
    return jnp.where(
        at < SPAN // 2, peak, jnp.where(at < SPAN * 3 // 4, rounded, total - rounded)
    )


def merge(pieces):
    slots = pieces[0].shape[0] // (GROUP + 1)
    found = [x[GROUP * slots :].astype(jnp.float32) for x in pieces]
    highest = functools.reduce(jnp.maximum, found)
    scales = [
        jnp.exp(x - highest)
        * (
            pltpu.roll(x, LANES - SPAN // 2, axis=1)
            + pltpu.roll(x, LANES - SPAN * 3 // 4, axis=1)
        )
        for x in found
    ]
    total = sum(scales)
    safe = jnp.where(total > 0.0, total, 1.0)
    values = []
    for h in range(GROUP):
        column = slice(h * SPAN, h * SPAN + 1)
        parts = [
            x[h * slots : (h + 1) * slots].astype(jnp.float32) * y[:, column]
            for x, y in zip(pieces, scales)
        ]
        values.append(sum(parts) / safe[:, column])
    return values, highest, total


def whole_part(pieces):
    values, highest, total = merge(pieces)
    lane = lax.broadcasted_iota(jnp.int32, highest.shape, 1)
    total = pltpu.roll(total, SPAN // 2, axis=1)
    rounded = total.astype(jnp.bfloat16).astype(jnp.float32)
    rest = pltpu.roll(total - rounded, SPAN // 4, axis=1)
    at = lane % SPAN
    stats = jnp.where(at < SPAN // 2, highest, jnp.where(at < SPAN * 3 // 4, rounded, rest))
    return jnp.concatenate(values + [stats], axis=0).astype(jnp.bfloat16)


def spread_kernel(pieces, out):
    part = whole_part([pieces[i, : out.shape[1], :] for i in range(pieces.shape[0])])
    for i in range(out.shape[0]):
        out[i] = part


def part_kernel(pieces, out):
    out[...] = whole_part([pieces[i] for i in range(pieces.shape[0])])


def project_kernel(place, mine, other, landed, hidden, out):
    slots, columns = hidden.shape
    count, deep = landed.shape[0], mine.shape[0]
    values, _, _ = merge([mine[...], other[...]])
    attn = jnp.concatenate(values, axis=1).astype(jnp.bfloat16)
    heads = []
    for h in range(GROUP):
        at = deep + h * columns
        parts = [landed[i, at : at + columns, :] for i in range(count)]
        heads.append(jnp.concatenate(parts, axis=0))
    weight = jnp.concatenate(heads, axis=1)
    total = lax.dot_general(
        attn, weight, (((1,), (1,)), ((), ())), preferred_element_type=jnp.float32
    )
    tiled = jnp.concatenate([hidden[...].astype(jnp.float32)] * count, axis=1)
    owner = lax.broadcasted_iota(jnp.int32, tiled.shape, 1) // columns
    part = (total + jnp.where(owner == place[0], tiled, 0.0)).astype(jnp.bfloat16)
    for i in range(count):
        out[i] = part


def mixed_kernel(place, pieces, own, out):
    columns = own.shape[1]
    total = pieces[0].astype(jnp.float32)
    for i in range(1, pieces.shape[0]):
        total = total + pieces[i].astype(jnp.float32)
    mixed = total.astype(jnp.bfloat16)
    for i in range(out.shape[0]):
        out[i] = mixed
    mine = [total[:, i * columns : (i + 1) * columns] for i in range(pieces.shape[0])]
    own[...] = sum(jnp.where(place[0] == i, x, 0.0) for i, x in enumerate(mine)).astype(
        jnp.bfloat16
    )


def in_feature_order(gathered, share):
    count, slots, width = gathered.shape
    columns, rows, halves = LANES // share, count // share, width // LANES
    block = lax.broadcasted_iota(jnp.int32, (slots, LANES), 1) // columns
    tiles = {}
    for m in range(rows):
        for half in range(halves):
            found = [
                gathered[share * m + j, :, half * LANES : (half + 1) * LANES].astype(jnp.float32)
                for j in range(share)
            ]
            for b in range(share):
                tile = found[b]
                for j in range(share):
                    if j != b:
                        turned = pltpu.roll(found[j], (j - b) % share * columns, axis=1)
                        tile = jnp.where(block == j, turned, tile)
                tiles[(half * share + b) * rows + m] = tile
    return jnp.concatenate([tiles[k] for k in range(len(tiles))], axis=1)


def swapped(tiles, share):
    slots = tiles.shape[1]
    deep, width = slots // share, LANES // share
    row = lax.broadcasted_iota(jnp.int32, tiles.shape, 1) // deep
    lane = lax.broadcasted_iota(jnp.int32, tiles.shape, 2) // width
    turn = (lane - row + share) % share
    result = tiles
    for j in range(1, share):
        moved = pltpu.roll(pltpu.roll(tiles, j * width, axis=2), slots - j * deep, axis=1)
        result = jnp.where(turn == j, moved, result)
    return result


def experts_kernel(
    share, expert, core, gathered, gain, router, chosen, gate_up, down, own, other
):
    blocks, slots = own.shape[0], 2 * own.shape[1]
    mixed = in_feature_order(gathered, share)
    scale = lax.rsqrt(jnp.sum(mixed * mixed, axis=1, keepdims=True) / (blocks * LANES) + 1e-05)
    normed = (mixed * scale * gain[...].astype(jnp.float32).reshape(1, blocks * LANES)).astype(jnp.bfloat16)
    plain = normed.astype(jnp.float32)
    weights = router[...].astype(jnp.float32)
    logits = [
        jnp.sum(plain * weights[e : e + 1], axis=1, keepdims=True) for e in range(EXPERTS)
    ]
    upright = lax.broadcasted_iota(jnp.int32, (slots, slots), 0) == lax.broadcasted_iota(
        jnp.int32, (slots, slots), 1
    )
    ids = [
        jnp.sum(
            jnp.where(upright, chosen[i : i + 1, :].astype(jnp.float32), 0.0),
            axis=1,
            keepdims=True,
        )
        for i in range(2)
    ]
    picked = [sum(jnp.where(k == e, logits[e], 0.0) for e in range(EXPERTS)) for k in ids]
    gates = [jax.nn.sigmoid(picked[i] - picked[1 - i]) for i in range(2)]
    mine = expert[0].astype(jnp.float32)
    part = sum(jnp.where(ids[i] == mine, gates[i], 0.0) for i in range(2))
    gate, up = [
        lax.dot_general(
            normed, gate_up[i], (((1,), (1,)), ((), ())), preferred_element_type=jnp.float32
        )
        for i in range(2)
    ]
    act = (gate * jax.nn.sigmoid(gate) * up).astype(jnp.bfloat16)
    term = part * jnp.dot(act, down[...], preferred_element_type=jnp.float32)
    tiles = [term[None, :, k * LANES : (k + 1) * LANES] for k in range(blocks)]
    even, odd = by_core(swapped(jnp.concatenate(tiles, axis=0), share), slots // share)
    own[...] = jnp.where(core[0] == 0, even, odd)
    other[...] = jnp.where(core[0] == 0, odd, even).astype(jnp.bfloat16)


def by_core(tiles, deep):
    top, bottom = tiles[:, : 2 * deep], tiles[:, 2 * deep :]
    first = lax.broadcasted_iota(jnp.int32, top.shape, 1) < deep
    even = jnp.where(first, top, pltpu.roll(bottom, deep, axis=1))
    odd = jnp.where(first, pltpu.roll(top, deep, axis=1), bottom)
    return even, odd


def add_kernel(own, other, out):
    out[...] = (own[...] + other[...].astype(jnp.float32)).astype(jnp.bfloat16)


def final_kernel(pieces, mixed, out):
    slots, columns = mixed.shape
    share = LANES // columns
    total = jnp.sum(pieces[...].astype(jnp.float32), axis=0)
    moe = jnp.concatenate(
        [total[:, b * columns : (b + 1) * columns] for b in range(share)], axis=0
    )
    out[...] = (mixed[...].astype(jnp.float32) + moe).astype(jnp.bfloat16)


def on_device(
    hidden,
    queries,
    cache_kv,
    cache_len,
    inserted_key_value,
    insert_slot,
    prefix_len,
    out_weight,
    norm_gain,
    router_weight,
    expert_ids,
    gate_up,
    down_proj,
):
    devices = lax.axis_size(BLK)
    dev_index = lax.axis_index(BLK)
    slots, columns = hidden.shape
    ctx_rows, kv_width = cache_kv.shape[2:]
    prefixes = insert_slot.shape[0]
    share = LANES // columns
    deep = slots * (GROUP + 1)
    width = devices * columns
    blocks = width // LANES
    bf16 = jnp.bfloat16

    first = (dev_index * ctx_rows).astype(jnp.int32).reshape(1)
    place = lax.axis_index(BLK[0]).astype(jnp.int32).reshape(1)
    expert = (dev_index * gate_up.shape[2] // FF).astype(jnp.int32).reshape(1)
    core = lax.axis_index(BLK[2]).astype(jnp.int32).reshape(1)
    first, place, expert, core = lax.optimization_barrier((first, place, expert, core))
    partials = pl.pallas_call(
        functools.partial(attention_kernel, devices * ctx_rows),
        out_shape=jax.ShapeDtypeStruct((KEY_VALUE_HEADS, deep + GROUP * columns, HEAD_SIZE), bf16),
        in_specs=[IN_SMEM] + [IN_HBM] * 7,
        out_specs=IN_VMEM,
        scratch_shapes=[
            pltpu.SMEM((slots,), jnp.int32),
            pltpu.SMEM((prefixes,), jnp.int32),
            pltpu.SMEM((prefixes,), jnp.int32),
            pltpu.VMEM(queries.shape, bf16),
            pltpu.VMEM(out_weight.shape[::-1], bf16),
            pltpu.VMEM((slots * QUERY_HEADS, HEAD_SIZE), jnp.float32),
            pltpu.VMEM((2, slots + prefixes, ctx_rows, kv_width), bf16),
            pltpu.VMEM((slots, QUERY_HEADS, ctx_rows), jnp.float32),
            pltpu.VMEM((slots * QUERY_HEADS, HEAD_SIZE), jnp.float32),
            pltpu.VMEM((slots * QUERY_HEADS, HEAD_SIZE), jnp.float32),
            pltpu.SemaphoreType.DMA((5 + 2 * (slots + prefixes) // BATCH,)),
        ],
        compiler_params=params(24),
        name="attention",
    )(
        first,
        in_hbm(cache_len),
        in_hbm(insert_slot),
        in_hbm(prefix_len),
        in_hbm(queries),
        in_hbm(out_weight.T),
        in_hbm(cache_kv),
        in_hbm(inserted_key_value),
    )
    along, across, pair = BLK
    copies = lax.axis_size(across)
    landed = exchanged(partials, along)
    part = merging(spread_kernel, (copies, deep, HEAD_SIZE), landed)
    part = merging(part_kernel, (deep, HEAD_SIZE), exchanged(part, across))
    other = lax.ppermute(part, pair, [(0, 1), (1, 0)])
    count = lax.axis_size(along)
    parts = pl.pallas_call(
        project_kernel,
        out_shape=jax.ShapeDtypeStruct((count, slots, count * columns), bf16),
        in_specs=[IN_SMEM] + [IN_VMEM] * 4,
        out_specs=IN_VMEM,
        compiler_params=params(8),
        cost_estimate=COVER,
        name="project",
    )(place, part, other, landed, hidden)
    local_mixed, packed = pl.pallas_call(
        mixed_kernel,
        out_shape=(
            jax.ShapeDtypeStruct((slots, columns), bf16),
            jax.ShapeDtypeStruct((devices // count, slots, count * columns), bf16),
        ),
        in_specs=[IN_SMEM, IN_VMEM],
        out_specs=(IN_VMEM, IN_VMEM),
        compiler_params=params(8),
        cost_estimate=COVER,
        name="mixed",
    )(place, exchanged(parts, along))
    gathered = exchanged(packed, (across, pair))

    own, other = pl.pallas_call(
        functools.partial(experts_kernel, share),
        out_shape=(
            jax.ShapeDtypeStruct((blocks, slots // 2, LANES), jnp.float32),
            jax.ShapeDtypeStruct((blocks, slots // 2, LANES), bf16),
        ),
        in_specs=[IN_SMEM] * 2 + [IN_VMEM] * 6,
        out_specs=(IN_VMEM, IN_VMEM),
        compiler_params=params(24),
        name="experts",
    )(
        expert,
        core,
        gathered,
        norm_gain,
        router_weight.T,
        expert_ids.T,
        jnp.swapaxes(gate_up, 1, 2),
        down_proj,
    )
    other = lax.ppermute(other, pair, [(0, 1), (1, 0)])
    terms = merging(add_kernel, own.shape, own, other)
    moe = exchanged(terms.reshape(devices // 2, slots // share, LANES), (along, across))
    return pl.pallas_call(
        final_kernel,
        out_shape=jax.ShapeDtypeStruct((slots, columns), bf16),
        in_specs=[IN_VMEM] * 2,
        out_specs=IN_VMEM,
        compiler_params=params(4),
        name="final",
    )(moe, local_mixed)


def solution(mesh):
    split = Mesh(
        mesh.devices.reshape(mesh.shape["rep"], 8, 8, 2), ("rep", "blk_0", "blk_1", "blk_2")
    )
    return jax.shard_map(
        on_device,
        mesh=split,
        in_specs=(
            P("rep", BLK),
            P("rep", None),
            P(None, "rep", BLK, None),
            P("rep"),
            P(None, "rep", BLK, None),
            P("rep"),
            P("rep"),
            P(None, BLK),
            P(),
            P(),
            P("rep", None),
            P(None, None, BLK),
            P(BLK, None),
        ),
        out_specs=P("rep", BLK),
        check_vma=False,
    )
```
